256 devices in a mesh: dp: 16 (over y, x_hi, core), space: 16 (over x_lo, z).
Axes of the slice: x: 4 (x_hi: 2, x_lo: 2; x = x_hi * 2 + x_lo), y: 4, z: 8, core: 2. Of those that a mesh axis runs over, the one named last changes fastest.
Arguments:
- act_in: bfloat16 [16, 32, 64, 2048], P('dp', 'space'), may hold values from -6 to 6
- weight_one: bfloat16 [3, 3, 3, 32, 64], replicated, may hold values from -0.21875 to 0.21875
- bias_one: float32 [64], replicated, may hold values from -3 to 3
- weight_two: bfloat16 [3, 3, 3, 64, 128], replicated, may hold values from -0.15625 to 0.15625
- bias_two: float32 [128], replicated, may hold values from -3 to 3
- cotangent: bfloat16 [16, 16, 32, 4096], P('dp', 'space'), may hold values from -24 to 24
Outputs:
- grad_input: bfloat16 [16, 32, 64, 2048], P('dp', 'space')
- grad_w_one: float32 [3, 3, 3, 32, 64], replicated
- grad_b_one: float32 [64], replicated
- grad_w_two: float32 [3, 3, 3, 64, 128], replicated
- grad_b_two: float32 [128], replicated
The draws below stay inside these ranges and needn't reach their ends.
All inputs are finite; a program needn't handle non-finite values.
Results may differ from the reference program's by a relative error of at most 0.01.
Values may be sent and summed in bfloat16 or wider, within the bound.
No kernel may reach another device: no remote copies, remote signals or barrier semaphores. Data moves between devices by JAX's collectives and lax.ppermute only.
A program may use at most 128 MiB of HBM per device.

```python
import math
import jax
import jax.numpy as jnp
from jax import lax

C0 = 32
C1 = 64
C2 = 128
SIDE = 64
BATCH = 16
DEPTH = 32
DEPTH2 = 16
HALF = 32


def levels(rng, shape, shards, smallest, high):
    gain = 1.0
    for dim, blocks in shards:
        draws = jax.random.uniform(jax.random.fold_in(jax.random.fold_in(rng, 6), dim), (blocks,), jnp.float32, smallest / len(shards), high / len(shards))
        gain = gain * jnp.repeat(jnp.exp(draws), shape[dim] // blocks).reshape((-1,) + (1,) * (len(shape) - 1 - dim))
    return gain


def centred(stream_key, dims, deviation, reach, cuts=(), kind=jnp.bfloat16):
    gain = levels(stream_key, dims, cuts, -0.22, 0.18) if cuts else 1.0
    drawn = jax.random.normal(stream_key, dims, jnp.float32) * deviation * gain
    return jnp.minimum(jnp.maximum(drawn, -reach), reach).astype(kind)


def setup_inputs(seed: int = 0) -> dict:
    splits = jax.random.split(jax.random.key(seed), 7)
    return {
        "act_in": centred(splits[0], (BATCH, DEPTH, SIDE, SIDE * C0), 1.0, 6.0, ((0, 16), (1, 16))),
        "weight_one": centred(splits[1], (3, 3, 3, C0, C1), (27 * C0) ** -0.5, 0.21875),
        "bias_one": centred(splits[2], (C1,), 0.5, 3.0, (), jnp.float32),
        "weight_two": centred(splits[3], (3, 3, 3, C1, C2), (27 * C1) ** -0.5, 0.15625),
        "bias_two": centred(splits[4], (C2,), 0.5, 3.0, (), jnp.float32),
        "cotangent": centred(splits[5], (BATCH, DEPTH2, HALF, HALF * C2), 4.0, 24.0, ((0, 16), (1, 16))),
    }


def forward_conv(padded, kernel):
    return lax.conv_general_dilated(padded, kernel, (1, 1, 1), ((0, 0), (1, 1), (1, 1)), dimension_numbers=('NDHWC', 'DHWIO', 'NDHWC'), preferred_element_type=jnp.float32)

def weight_grad(padded, delta):
    return lax.conv_general_dilated(padded, delta, (1, 1, 1), ((0, 0), (1, 1), (1, 1)), dimension_numbers=('CDHWN', 'IDHWO', 'DHWNC'), preferred_element_type=jnp.float32)

def input_grad(delta, kernel, depth_pad):
    return lax.conv_general_dilated(delta, kernel[::-1, ::-1, ::-1], (1, 1, 1), (depth_pad, (1, 1), (1, 1)), dimension_numbers=('NDHWC', 'DHWOI', 'NDHWC'), preferred_element_type=jnp.float32)

def silu_slope(value):
    sig = jax.nn.sigmoid(value)
    return sig * (1.0 + value * (1.0 - sig))

def reference(act_in, weight_one, bias_one, weight_two, bias_two, cotangent):

    def single(pair):
        sample, cot = pair
        x_five = sample.reshape(1, DEPTH, SIDE, SIDE, C0)
        x_pad = jnp.pad(x_five, ((0, 0), (1, 1), (0, 0), (0, 0), (0, 0)))
        pre_one = forward_conv(x_pad, weight_one) + bias_one
        act_one = pre_one * jax.nn.sigmoid(pre_one)
        pooled = act_one.reshape(1, DEPTH2, 2, HALF, 2, HALF, 2, C1).mean(axis=(2, 4, 6)).astype(jnp.bfloat16)
        pool_pad = jnp.pad(pooled, ((0, 0), (1, 1), (0, 0), (0, 0), (0, 0)))
        pre_two = forward_conv(pool_pad, weight_two) + bias_two
        cot_five = cot.reshape(1, DEPTH2, HALF, HALF, C2).astype(jnp.float32)
        delta_two = (cot_five * silu_slope(pre_two)).astype(jnp.bfloat16)
        gw_two = weight_grad(pool_pad, delta_two)
        gb_two = lax.optimization_barrier(jnp.sum(delta_two, axis=(0, 1, 2, 3), dtype=jnp.float32))
        grad_pooled = input_grad(delta_two, weight_two, (1, 1))
        spread = jnp.broadcast_to(grad_pooled[:, :, None, :, None, :, None, :], (1, DEPTH2, 2, HALF, 2, HALF, 2, C1)).reshape(1, DEPTH, SIDE, SIDE, C1)
        delta_one = (spread / 8.0 * silu_slope(pre_one)).astype(jnp.bfloat16)
        gw_one = weight_grad(x_pad, delta_one)
        gb_one = lax.optimization_barrier(jnp.sum(delta_one, axis=(0, 1, 2, 3), dtype=jnp.float32))
        grad_x = input_grad(delta_one, weight_one, (1, 1)).astype(jnp.bfloat16).reshape(DEPTH, SIDE, SIDE * C0)
        return (grad_x, gw_one, gb_one, gw_two, gb_two)
    grad_x, gw_one, gb_one, gw_two, gb_two = lax.map(single, (act_in, cotangent))
    scale_one = 16.0 / math.sqrt(BATCH * DEPTH * SIDE * SIDE)
    scale_two = 1.0 / math.sqrt(BATCH * DEPTH2 * HALF * HALF)
    return (grad_x, lax.optimization_barrier(jnp.sum(gw_one, axis=0)) * scale_one, lax.optimization_barrier(jnp.sum(gb_one, axis=0)) * scale_one, lax.optimization_barrier(jnp.sum(gw_two, axis=0)) * scale_two, lax.optimization_barrier(jnp.sum(gb_two, axis=0)) * scale_two)
```

```python
import functools
import math

import jax
import jax.numpy as jnp
from jax import lax
from jax.experimental import pallas as pl
from jax.experimental.pallas import tpu as pltpu
from jax.sharding import PartitionSpec as P

F32 = jnp.float32
BF16 = jnp.bfloat16
LANES = 128
MIB = 1024 * 1024


def _params(mib):
    return pltpu.CompilerParams(vmem_limit_bytes=mib * MIB)


def _cost(flops, moved):
    return pl.CostEstimate(flops=int(flops), bytes_accessed=int(moved), transcendentals=0)


def _dot(a, b):
    return lax.dot_general(a, b, (((1,), (0,)), ((), ())), preferred_element_type=F32)


def _dot_t(a, b):
    return lax.dot_general(a, b, (((1,), (1,)), ((), ())), preferred_element_type=F32)


def _sigmoid(v):
    return 1.0 / (1.0 + jnp.exp(-v))


def _zero_edges(buf, rows):
    tiles = buf.shape[0]
    buf[:, 0:8, :] = jnp.zeros((tiles, 8, LANES), F32)
    buf[:, 8 + rows : 16 + rows, :] = jnp.zeros((tiles, 8, LANES), F32)


def _spread(load, tiles, rows, shift, buf, out):
    lane = lax.broadcasted_iota(jnp.int32, (rows, LANES), 1)
    before = jnp.zeros((rows, LANES), F32)
    for t in range(tiles + 1):
        now = pltpu.roll(load(t).astype(F32), shift, 1) if t < tiles else jnp.zeros((rows, LANES), F32)
        tile = jnp.where(lane < shift, before, now)
        buf[t, 8 : 8 + rows, :] = tile
        out[1, t] = tile.astype(BF16)
        before = now
    for t in range(tiles + 1):
        out[0, t] = buf[t, 7 : 7 + rows, :].astype(BF16)
        out[2, t] = buf[t, 9 : 9 + rows, :].astype(BF16)


def _cols(ref, first, groups):
    rows = ref.shape[1]
    a = ref[pl.ds(first, groups)].reshape(groups * rows, LANES)
    b = ref[pl.ds(first + 1, groups)].reshape(groups * rows, LANES)
    return jnp.concatenate([a, b], axis=1)


def _first_kernel(x_ref, w_ref, pre_ref, xs_ref, band_ref, buf):
    rows, groups = x_ref.shape[1], pre_ref.shape[1]
    band_ref[...] = jnp.zeros(band_ref.shape, BF16)
    for kk in range(9):
        for kw in range(3):
            tap = w_ref[3 * kk + kw]
            for j in range(4):
                r = 256 * kk + 32 * (j + kw)
                band_ref[r : r + 32, 64 * j : 64 * j + 64] = tap
    _zero_edges(buf, rows)
    for p in range(2):
        _spread(
            lambda t, p=p: x_ref[p, :, LANES * t : LANES * (t + 1)], groups, rows, 32, buf, xs_ref.at[p]
        )
    step = 8

    def chunk(c, carry):
        g = c * step
        sides = [[_cols(xs_ref.at[p, kh], g, step) for kh in range(3)] for p in range(2)]
        lhs = jnp.concatenate(sides[0] + sides[1], axis=1)
        pre_ref[0, pl.ds(g, step)] = _dot(lhs, band_ref[768:2304, :]).reshape(step, rows, 256)
        pre_ref[1, pl.ds(g, step)] = _dot(lhs, band_ref[0:1536, :]).reshape(step, rows, 256)
        return carry

    lax.fori_loop(0, groups // step, chunk, 0)


def _second_kernel(left_ref, right_ref, pre_ref, band_ref, bias_ref, slope_ref, pool_ref, xs_ref, buf, low, high):
    rows, groups = left_ref.shape[0], pre_ref.shape[1]
    half = rows // 2
    _zero_edges(buf, rows)
    for s, ref in enumerate((left_ref, right_ref)):
        _spread(lambda t, ref=ref: ref[:, LANES * t : LANES * (t + 1)], groups, rows, 32, buf, xs_ref.at[s])
    step = 4
    lane = lax.broadcasted_iota(jnp.int32, (step * half, LANES), 1)

    def chunk(c, carry):
        g = c * step
        total = None
        for p in range(2):
            lhs = jnp.concatenate([_cols(xs_ref.at[p, kh], g, step) for kh in range(3)], axis=1)
            more = _dot(lhs, band_ref[1536 * p : 1536 * p + 768, :])
            pre = pre_ref[p, pl.ds(g, step)].reshape(step * rows, 256) + more + bias_ref[...]
            sig = _sigmoid(pre)
            slope_ref[p, pl.ds(g, step)] = (sig * (1.0 + pre * (1.0 - sig))).reshape(step, rows, 256)
            act = pre * sig
            total = act if total is None else total + act
        for part, lanes in ((low, 0), (high, LANES)):
            v = total[:, lanes : lanes + LANES]
            part[...] = v + pltpu.roll(v, 64, 1)
        a = low[pl.ds(0, step * half, stride=2), :] + low[pl.ds(1, step * half, stride=2), :]
        b = high[pl.ds(0, step * half, stride=2), :] + high[pl.ds(1, step * half, stride=2), :]
        mean = jnp.where(lane < 64, a, b) * 0.125
        pool_ref[pl.ds(g, step)] = mean.astype(BF16).reshape(step, half, LANES)
        return carry

    lax.fori_loop(0, groups // step, chunk, 0)


def _third_kernel(
    own_ref, left_ref, right_ref, w_ref, bias_ref, cot_ref, delta_ref, ps_ref, gl_ref, gm_ref, gr_ref, band, back, buf, ds
):
    groups, rows = own_ref.shape[0], own_ref.shape[1]
    band[...] = jnp.zeros(band.shape, BF16)
    back[...] = jnp.zeros(back.shape, BF16)
    for kk in range(9):
        kd, kh = kk // 3, kk % 3
        for kw in range(3):
            tap = w_ref[3 * kk + kw]
            for j in range(2):
                r = 256 * kk + 64 * (j + kw)
                band[r : r + 64, LANES * j : LANES * (j + 1)] = tap
            for j in range(4):
                c = 768 * kh + LANES * (j - kw + 2)
                back[kd, 64 * j : 64 * j + 64, c : c + LANES] = tap
    _zero_edges(buf, rows)
    for s, ref in enumerate((left_ref, own_ref, right_ref)):
        _spread(lambda t, ref=ref: ref[t], groups, rows, 64, buf, ps_ref.at[s])
    lhs = jnp.concatenate([_cols(ps_ref.at[kk // 3, kk % 3], 0, groups) for kk in range(9)], axis=1)
    pre = _dot(lhs, band[...]) + bias_ref[...]
    sig = _sigmoid(pre)
    cot = jnp.concatenate([cot_ref[:, 256 * g : 256 * (g + 1)] for g in range(groups)], axis=0)
    delta = (cot.astype(F32) * (sig * (1.0 + pre * (1.0 - sig)))).astype(BF16)
    delta_ref[...] = delta
    again = delta.astype(F32)
    cells = 2 * groups
    zero = jnp.zeros((rows, LANES), BF16)
    for kh in range(3):
        ds[kh, 0] = zero
        ds[kh, cells + 1] = zero
    for t in range(cells):
        g, j = t // 2, t % 2
        tile = again[g * rows : (g + 1) * rows, LANES * j : LANES * (j + 1)]
        spot = buf.at[t % buf.shape[0]]
        spot[8 : 8 + rows, :] = tile
        ds[0, t + 1] = spot[9 : 9 + rows, :].astype(BF16)
        ds[1, t + 1] = tile.astype(BF16)
        ds[2, t + 1] = spot[7 : 7 + rows, :].astype(BF16)
    wide = cells // 4
    parts = []
    for kh in range(3):
        for i in range(6):
            parts.append(jnp.concatenate([ds[kh, 4 * g + i] for g in range(wide)], axis=0))
    lhs = jnp.concatenate(parts, axis=1)
    for kd, ref in enumerate((gl_ref, gm_ref, gr_ref)):
        out = _dot_t(lhs, back[kd])
        for g in range(wide):
            for j in range(2):
                ref[2 * g + j] = out[g * rows : (g + 1) * rows, LANES * j : LANES * (j + 1)].astype(ref.dtype)


def _grad_two_kernel(delta_ref, ps_ref, out_ref):
    groups = ps_ref.shape[2] - 1
    out_ref[...] = jnp.zeros(out_ref.shape, BF16)
    delta = delta_ref[...]
    flip = delta.astype(F32).T.astype(BF16)
    for kk in range(9):
        full = _dot(flip, _cols(ps_ref.at[kk // 3, kk % 3], 0, groups))
        band = full[0:LANES, :] + pltpu.roll(full[LANES:256, :], 192, 1)
        out_ref[192 * kk : 192 * (kk + 1), :] = band.T[0:192, :].astype(BF16)
    total = jnp.sum(delta.astype(F32), axis=0, keepdims=True)
    line = total[:, 0:LANES] + total[:, LANES:256]
    out_ref[1728:1744, :] = jnp.broadcast_to(line, (16, LANES)).astype(BF16)


def _delta_one_kernel(
    gm_ref, fl_ref, fr_ref, slope_ref, w_ref, delta_ref, ds_ref, back_ref, gl_ref, gr_ref, sum_ref, buf, up0, up1
):
    groups, rows = slope_ref.shape[1], slope_ref.shape[2]
    half = rows // 2
    cells = 2 * groups
    back_ref[...] = jnp.zeros(back_ref.shape, BF16)
    for kk in range(9):
        kd, kh = kk // 3, kk % 3
        for kw in range(3):
            tap = w_ref[3 * kk + kw]
            for j in range(8):
                c = 768 * kh + 64 * (j - kw + 3)
                back_ref[kd, 32 * j : 32 * j + 32, c : c + 64] = tap
    _zero_edges(buf, rows)
    zero = jnp.zeros((rows, LANES), BF16)
    for p in range(2):
        for kh in range(3):
            ds_ref[p, kh, 0] = zero
            ds_ref[p, kh, cells + 1] = zero
    lane = lax.broadcasted_iota(jnp.int32, (half, LANES), 1)
    sum_ref[...] = jnp.zeros(sum_ref.shape, F32)

    def group(g, carry):
        v = (gm_ref[g] + fl_ref[g].astype(F32) + fr_ref[g].astype(F32)) * 0.125
        turned = pltpu.roll(v, 64, 1)
        a = jnp.where(lane < 64, v, turned)
        b = jnp.where(lane < 64, turned, v)
        for ref, val in ((up0, a), (up1, b)):
            ref[pl.ds(0, half, stride=2), :] = val
            ref[pl.ds(1, half, stride=2), :] = val
        for p in range(2):
            for j, ref in enumerate((up0, up1)):
                low = (ref[...] * slope_ref[p, g, :, LANES * j : LANES * (j + 1)]).astype(BF16)
                delta_ref[p, g, :, LANES * j : LANES * (j + 1)] = low
                tile = low.astype(F32)
                sum_ref[:, LANES * j : LANES * (j + 1)] += jnp.sum(tile.reshape(rows // 8, 8, LANES), axis=0)
                spot = buf.at[2 * p + j]
                spot[8 : 8 + rows, :] = tile
                t = 2 * g + j + 1
                ds_ref[p, 0, t] = spot[9 : 9 + rows, :].astype(BF16)
                ds_ref[p, 1, t] = low
                ds_ref[p, 2, t] = spot[7 : 7 + rows, :].astype(BF16)
        return carry

    lax.fori_loop(0, groups, group, 0)
    wide = cells // 4
    step = wide // 2

    def chunk(c, carry):
        for p, kd, ref in ((0, 0, gl_ref), (1, 2, gr_ref)):
            out = _dot_t(_window(ds_ref.at[p], c * step, step), back_ref[kd])
            ref[pl.ds(c * step, step)] = out.astype(BF16).reshape(step, rows, 256)
        return carry

    lax.fori_loop(0, 2, chunk, 0)


def _window(ref, first, count):
    parts = []
    for kh in range(3):
        for i in range(6):
            parts.append(jnp.concatenate([ref[kh, 4 * (first + g) + i] for g in range(count)], axis=0))
    return jnp.concatenate(parts, axis=1)


def _grad_one_kernel(delta_ref, own_ref, halo_ref, sum_ref, out_ref, flip):
    groups, rows = delta_ref.shape[1], delta_ref.shape[2]
    size = groups * rows
    out_ref[...] = jnp.zeros(out_ref.shape, BF16)
    for p in range(2):
        for g in range(0, groups, 2):
            block = delta_ref[p, g : g + 2].reshape(2 * rows, 256).astype(F32)
            flip[:, p * size + g * rows : p * size + (g + 2) * rows] = block.T.astype(BF16)
    planes = (halo_ref.at[0], own_ref.at[0], own_ref.at[1], halo_ref.at[1])
    for kd in range(3):
        for kh in range(3):
            kk = 3 * kd + kh
            cols = jnp.concatenate([_cols(planes[p + kd].at[kh], 0, groups) for p in range(2)], axis=0)
            full = _dot(flip[...], cols)
            band = full[0:64, 0:LANES]
            for j in range(1, 4):
                band = band + pltpu.roll(full[64 * j : 64 * j + 64, :], 256 - 32 * j, 1)[:, 0:LANES]
            tall = band.T[0:96, :].astype(BF16)
            for r in range(0, 96, 48):
                at = 96 * kk + r
                side = at // 432
                out_ref[at - 432 * side : at - 432 * side + 48, 64 * side : 64 * side + 64] = tall[r : r + 48, :]
    total = jnp.sum(sum_ref[...], axis=0, keepdims=True)
    line = total[:, 0:LANES] + total[:, LANES:256]
    line = line + pltpu.roll(line, 64, 1)
    out_ref[432:448, :] = jnp.broadcast_to(line, (16, LANES)).astype(BF16)


def _grad_input_kernel(ds_ref, back_ref, fl_ref, fr_ref, out_ref):
    wide, rows = fl_ref.shape[0], fl_ref.shape[1]
    for g in range(0, wide, 2):
        near = _window(ds_ref.at[0], g, 2)
        far = _window(ds_ref.at[1], g, 2)
        first = _dot_t(near, back_ref[1]) + _dot_t(far, back_ref[0])
        second = _dot_t(near, back_ref[2]) + _dot_t(far, back_ref[1])
        for s in range(2):
            for p, val, ref in ((0, first, fl_ref), (1, second, fr_ref)):
                whole = val[s * rows : (s + 1) * rows] + ref[g + s].astype(F32)
                out_ref[p, :, 256 * (g + s) : 256 * (g + s + 1)] = whole.astype(BF16)


def _merge_kernel(a_ref, b_ref, out_ref):
    rows = a_ref.shape[1]
    a = jnp.sum(a_ref[...].astype(F32), axis=0).astype(BF16)
    b = jnp.sum(b_ref[...].astype(F32), axis=0).astype(BF16)
    for i in range(out_ref.shape[0]):
        out_ref[i, 0:rows, :] = a
        out_ref[i, rows:, :] = b


def _total_kernel(scale_two, scale_one, rows, in_ref, out_ref):
    whole = jnp.sum(in_ref[...].astype(F32), axis=0)
    a = (whole[0:rows] * scale_two).astype(BF16)
    b = (whole[rows:] * scale_one).astype(BF16)
    for i in range(out_ref.shape[0]):
        out_ref[i, 0:rows, :] = a
        out_ref[i, rows:, :] = b


def _unpack_kernel(rows_two, rows_one, in_ref, w_two_ref, b_two_ref, w_one_ref, b_one_ref):
    two, one = w_two_ref.shape[0], w_one_ref.shape[0] // 2
    for i in range(in_ref.shape[0]):
        at = i * rows_two
        take = min(rows_two, max(two - at, 0))
        if take:
            w_two_ref[at : at + take, :] = in_ref[i, 0:take, :].astype(F32)
        if at <= two < at + rows_two:
            b_two_ref[...] = in_ref[i, two - at : two - at + 16, :].astype(F32)[0:1]
        at = i * rows_one
        take = min(rows_one, max(one - at, 0))
        if take:
            block = in_ref[i, rows_two : rows_two + take, :].astype(F32)
            w_one_ref[at : at + take, :] = block[:, 0:64]
            w_one_ref[one + at : one + at + take, :] = block[:, 64:128]
        if at <= one < at + rows_one:
            spot = rows_two + one - at
            b_one_ref[...] = in_ref[i, spot : spot + 16, :].astype(F32)[0:1, 0:64]


def _shape(shape, dtype):
    return jax.ShapeDtypeStruct(shape, dtype)


def _call(kernel, name, out, scratch, flops, moved, mib, args):
    return pl.pallas_call(
        kernel,
        out_shape=out,
        scratch_shapes=scratch,
        compiler_params=_params(mib),
        cost_estimate=_cost(flops, moved),
        name=name,
    )(*args)


def _round_up(value, unit):
    return -(-value // unit) * unit


def local(act_in, weight_one, bias_one, weight_two, bias_two, cotangent):
    _, slab, side, merged = act_in.shape
    half = side // 2
    c0, c1 = weight_one.shape[3:]
    c2 = weight_two.shape[4]
    dp, space = lax.axis_size("dp"), lax.axis_size("space")
    depth_all = slab * space
    scale_one = 16.0 / math.sqrt(dp * depth_all * side * side)
    scale_two = 1.0 / math.sqrt(dp * (depth_all // 2) * half * half)
    up = [(i, i + 1) for i in range(space - 1)]
    down = [(i + 1, i) for i in range(space - 1)]

    x = act_in.reshape(slab, side, merged)
    from_left = lax.ppermute(x[slab - 1], "space", up)
    from_right = lax.ppermute(x[0], "space", down)
    w_one = weight_one.reshape(27, c0, c1)
    w_two = weight_two.reshape(27, c1, c2)
    bias_a = jnp.tile(bias_one.reshape(1, c1), (1, 4))
    bias_b = jnp.tile(bias_two.reshape(1, c2), (1, 2))
    groups = merged // LANES
    xs_shape = (2, 3, groups + 1, side, LANES)
    work = 2 * side * groups * 256
    pre, xs_own, band = _call(
        _first_kernel,
        "first",
        (_shape((2, groups, side, 256), F32), _shape(xs_shape, BF16), _shape((2304, 256), BF16)),
        [pltpu.VMEM((groups + 1, side + 16, LANES), F32)],
        2 * work * 1536,
        8 * MIB,
        24,
        (x, w_one),
    )
    slope, pooled, xs_halo = _call(
        _second_kernel,
        "second",
        (_shape((2, groups, side, 256), F32), _shape((groups, half, LANES), BF16), _shape(xs_shape, BF16)),
        [pltpu.VMEM((groups + 1, side + 16, LANES), F32)] + [pltpu.VMEM((4 * side, LANES), F32)] * 2,
        2 * work * 768,
        8 * MIB,
        24,
        (from_left, from_right, pre, band, bias_a),
    )
    pool_left = lax.ppermute(pooled, "space", up)
    pool_right = lax.ppermute(pooled, "space", down)
    rows_mid = groups * half
    delta_two, ps, gp_left, gp_own, gp_right = _call(
        _third_kernel,
        "third",
        (
            _shape((rows_mid, 256), BF16),
            _shape((3, 3, groups + 1, half, LANES), BF16),
            _shape((groups, half, LANES), BF16),
            _shape((groups, half, LANES), F32),
            _shape((groups, half, LANES), BF16),
        ),
        [
            pltpu.VMEM((2304, 256), BF16),
            pltpu.VMEM((3, 256, 2304), BF16),
            pltpu.VMEM((groups + 1, half + 16, LANES), F32),
            pltpu.VMEM((3, 2 * groups + 2, half, LANES), BF16),
        ],
        4 * rows_mid * 256 * 2304,
        4 * MIB,
        32,
        (pooled, pool_left, pool_right, w_two, bias_b, cotangent.reshape(half, -1)),
    )
    gp_from_right = lax.ppermute(gp_left, "space", down)
    gp_from_left = lax.ppermute(gp_right, "space", up)
    rows_two = _round_up(1744, 16 * dp)
    rows_one = _round_up(448, 16 * dp)
    part_two = _call(
        _grad_two_kernel,
        "grad_two",
        _shape((rows_two, LANES), BF16),
        [],
        2 * rows_mid * 256 * 2304,
        2 * MIB,
        24,
        (delta_two, ps),
    )
    met_two = lax.all_to_all(part_two.reshape(dp, rows_two // dp, LANES), "dp", 0, 0)
    delta_one, ds, back, gx_left, gx_right, sums = _call(
        _delta_one_kernel,
        "delta_one",
        (
            _shape((2, groups, side, 256), BF16),
            _shape((2, 3, 2 * groups + 2, side, LANES), BF16),
            _shape((3, 256, 2304), BF16),
            _shape((groups // 2, side, 256), BF16),
            _shape((groups // 2, side, 256), BF16),
            _shape((8, 256), F32),
        ),
        [pltpu.VMEM((4, side + 16, LANES), F32)] + [pltpu.VMEM((side, LANES), F32)] * 2,
        2 * work * 2304 // 2,
        8 * MIB,
        32,
        (gp_own, gp_from_left, gp_from_right, slope, w_one),
    )
    gx_from_right = lax.ppermute(gx_left, "space", down)
    gx_from_left = lax.ppermute(gx_right, "space", up)
    part_one = _call(
        _grad_one_kernel,
        "grad_one",
        _shape((rows_one, LANES), BF16),
        [pltpu.VMEM((256, 2 * groups * side), BF16)],
        2 * work * 2304,
        4 * MIB,
        24,
        (delta_one, xs_own, xs_halo, sums),
    )
    met_one = lax.all_to_all(part_one.reshape(dp, rows_one // dp, LANES), "dp", 0, 0)
    grad_x = _call(
        _grad_input_kernel,
        "grad_input",
        _shape((2, side, merged), BF16),
        [],
        2 * work * 2304,
        8 * MIB,
        24,
        (ds, back, gx_from_left, gx_from_right),
    )
    rows_two //= dp
    rows_one //= dp
    both = _shape((space, rows_two + rows_one, LANES), BF16)
    merged_parts = _call(_merge_kernel, "merge", both, [], 0, MIB, 16, (met_two, met_one))
    met = lax.all_to_all(merged_parts, "space", 0, 0)
    both = _shape((dp, rows_two + rows_one, LANES), BF16)
    total = _call(
        functools.partial(_total_kernel, scale_two, scale_one, rows_two), "total", both, [], 0, MIB, 16, (met,)
    )
    done = lax.all_to_all(total, "dp", 0, 0)
    gw_two, gb_two, gw_one, gb_one = _call(
        functools.partial(_unpack_kernel, rows_two, rows_one),
        "unpack",
        (
            _shape((27 * c1, c2), F32),
            _shape((1, c2), F32),
            _shape((27 * c0, c1), F32),
            _shape((1, c1), F32),
        ),
        [],
        0,
        MIB,
        16,
        (done,),
    )
    return (
        grad_x.reshape(act_in.shape),
        gw_one.reshape(weight_one.shape),
        gb_one.reshape(bias_one.shape),
        gw_two.reshape(weight_two.shape),
        gb_two.reshape(bias_two.shape),
    )


def solution(mesh):
    placed = (P("dp", "space", None, None), P(), P(), P(), P(), P("dp", "space", None, None))
    return jax.shard_map(
        local,
        mesh=mesh,
        in_specs=placed,
        out_specs=(P("dp", "space", None, None), P(), P(), P(), P()),
        check_vma=False,
    )
```

```python
import functools
import math

import jax
import jax.numpy as jnp
from jax import lax
from jax.experimental import pallas as pl
from jax.experimental.pallas import tpu as pltpu
from jax.sharding import PartitionSpec as P


F32 = jnp.float32
BF16 = jnp.bfloat16
LANES = 128
MIB = 1024 * 1024


def _params(mib):
    return pltpu.CompilerParams(vmem_limit_bytes=mib * MIB)


def _cost(flops, moved):
    return pl.CostEstimate(flops=int(flops), bytes_accessed=int(moved), transcendentals=0)


def _dot(a, b):
    return lax.dot_general(a, b, (((1,), (0,)), ((), ())), preferred_element_type=F32)


def _dot_t(a, b):
    return lax.dot_general(a, b, (((1,), (1,)), ((), ())), preferred_element_type=F32)


def _sigmoid(v):
    return 1.0 / (1.0 + jnp.exp(-v))


def _zero_edges(buf, rows):
    tiles = buf.shape[0]
    buf[:, 0:8, :] = jnp.zeros((tiles, 8, LANES), F32)
    buf[:, 8 + rows : 16 + rows, :] = jnp.zeros((tiles, 8, LANES), F32)


def _spread(load, tiles, rows, shift, buf, out):
    lane = lax.broadcasted_iota(jnp.int32, (rows, LANES), 1)
    before = jnp.zeros((rows, LANES), F32)
    for t in range(tiles + 1):
        now = pltpu.roll(load(t).astype(F32), shift, 1) if t < tiles else jnp.zeros((rows, LANES), F32)
        tile = jnp.where(lane < shift, before, now)
        buf[t, 8 : 8 + rows, :] = tile
        out[1, t] = tile.astype(BF16)
        before = now
    for t in range(tiles + 1):
        out[0, t] = buf[t, 7 : 7 + rows, :].astype(BF16)
        out[2, t] = buf[t, 9 : 9 + rows, :].astype(BF16)


def _cols(ref, first, groups):
    rows = ref.shape[1]
    a = ref[pl.ds(first, groups)].reshape(groups * rows, LANES)
    b = ref[pl.ds(first + 1, groups)].reshape(groups * rows, LANES)
    return jnp.concatenate([a, b], axis=1)


def _prep_kernel(w_one_ref, w_two_ref, back_one, band_two, back_two):
    for ref in (back_one, band_two, back_two):
        ref[...] = jnp.zeros(ref.shape, BF16)
    for kk in range(9):
        kd, kh = kk // 3, kk % 3
        for kw in range(3):
            tap = w_one_ref[3 * kk + kw]
            for j in range(8):
                c = 768 * kh + 64 * (j - kw + 3)
                back_one[kd, 32 * j : 32 * j + 32, c : c + 64] = tap
            tap = w_two_ref[3 * kk + kw]
            for j in range(2):
                r = 256 * kk + 64 * (j + kw)
                band_two[r : r + 64, LANES * j : LANES * (j + 1)] = tap
            for j in range(4):
                c = 768 * kh + LANES * (j - kw + 2)
                back_two[kd, 64 * j : 64 * j + 64, c : c + LANES] = tap


def _first_kernel(x0_ref, x1_ref, w_ref, pre_ref, xs_ref, band_ref, buf):
    rows, groups = x0_ref.shape[0], pre_ref.shape[1]
    band_ref[...] = jnp.zeros(band_ref.shape, BF16)
    for kk in range(9):
        for kw in range(3):
            tap = w_ref[3 * kk + kw]
            for j in range(4):
                r = 256 * kk + 32 * (j + kw)
                band_ref[r : r + 32, 64 * j : 64 * j + 64] = tap
    _zero_edges(buf, rows)
    for p, ref in enumerate((x0_ref, x1_ref)):
        _spread(lambda t, ref=ref: ref[:, LANES * t : LANES * (t + 1)], groups, rows, 32, buf, xs_ref.at[p])
    step = 8

    def chunk(c, carry):
        g = c * step
        sides = [[_cols(xs_ref.at[p, kh], g, step) for kh in range(3)] for p in range(2)]
        lhs = jnp.concatenate(sides[0] + sides[1], axis=1)
        pre_ref[0, pl.ds(g, step)] = _dot(lhs, band_ref[768:2304, :]).reshape(step, rows, 256)
        pre_ref[1, pl.ds(g, step)] = _dot(lhs, band_ref[0:1536, :]).reshape(step, rows, 256)
        return carry

    lax.fori_loop(0, groups // step, chunk, 0)


def _second_kernel(left_ref, right_ref, pre_ref, band_ref, bias_ref, slope_ref, pool_ref, xs_ref, buf, low, high):
    rows, groups = left_ref.shape[0], pre_ref.shape[1]
    half = rows // 2
    bias = jnp.concatenate([bias_ref[...]] * 4, axis=1)
    _zero_edges(buf, rows)
    for s, ref in enumerate((left_ref, right_ref)):
        _spread(lambda t, ref=ref: ref[:, LANES * t : LANES * (t + 1)], groups, rows, 32, buf, xs_ref.at[s])
    step = 4
    lane = lax.broadcasted_iota(jnp.int32, (step * half, LANES), 1)

    def chunk(c, carry):
        g = c * step
        total = None
        for p in range(2):
            lhs = jnp.concatenate([_cols(xs_ref.at[p, kh], g, step) for kh in range(3)], axis=1)
            more = _dot(lhs, band_ref[1536 * p : 1536 * p + 768, :])
            pre = pre_ref[p, pl.ds(g, step)].reshape(step * rows, 256) + more + bias
            sig = _sigmoid(pre)
            slope_ref[p, pl.ds(g, step)] = (sig * (1.0 + pre * (1.0 - sig))).reshape(step, rows, 256)
            act = pre * sig
            total = act if total is None else total + act
        for part, lanes in ((low, 0), (high, LANES)):
            v = total[:, lanes : lanes + LANES]
            part[...] = v + pltpu.roll(v, 64, 1)
        a = low[pl.ds(0, step * half, stride=2), :] + low[pl.ds(1, step * half, stride=2), :]
        b = high[pl.ds(0, step * half, stride=2), :] + high[pl.ds(1, step * half, stride=2), :]
        mean = jnp.where(lane < 64, a, b) * 0.125
        pool_ref[pl.ds(g, step)] = mean.astype(BF16).reshape(step, half, LANES)
        return carry

    lax.fori_loop(0, groups // step, chunk, 0)


def _mid_kernel(own_ref, band_ref, bias_ref, ps_ref, pre_ref, buf):
    groups, rows = own_ref.shape[0], own_ref.shape[1]
    _zero_edges(buf, rows)
    _spread(lambda t: own_ref[t], groups, rows, 64, buf, ps_ref)
    lhs = jnp.concatenate([_cols(ps_ref.at[kh], 0, groups) for kh in range(3)], axis=1)
    bias = jnp.concatenate([bias_ref[...]] * 2, axis=1)
    pre_ref[...] = _dot(lhs, band_ref[768:1536, :]) + bias


def _third_kernel(
    left_ref, right_ref, pre_ref, band_ref, back_ref, cot_ref, delta_ref, ps_ref, ds_ref, gl_ref, gr_ref, buf
):
    groups, rows = left_ref.shape[0], left_ref.shape[1]
    _zero_edges(buf, rows)
    for s, ref in enumerate((left_ref, right_ref)):
        _spread(lambda t, ref=ref: ref[t], groups, rows, 64, buf, ps_ref.at[s])
    near = jnp.concatenate([_cols(ps_ref.at[0, kh], 0, groups) for kh in range(3)], axis=1)
    far = jnp.concatenate([_cols(ps_ref.at[1, kh], 0, groups) for kh in range(3)], axis=1)
    pre = pre_ref[...] + _dot(near, band_ref[0:768, :]) + _dot(far, band_ref[1536:2304, :])
    sig = _sigmoid(pre)
    cot = jnp.concatenate([cot_ref[:, 256 * g : 256 * (g + 1)] for g in range(groups)], axis=0)
    delta = (cot.astype(F32) * (sig * (1.0 + pre * (1.0 - sig)))).astype(BF16)
    delta_ref[...] = delta
    again = delta.astype(F32)
    cells = 2 * groups
    zero = jnp.zeros((rows, LANES), BF16)
    for kh in range(3):
        ds_ref[kh, 0] = zero
        ds_ref[kh, cells + 1] = zero
    for t in range(cells):
        g, j = t // 2, t % 2
        tile = again[g * rows : (g + 1) * rows, LANES * j : LANES * (j + 1)]
        spot = buf.at[t % buf.shape[0]]
        spot[8 : 8 + rows, :] = tile
        ds_ref[0, t + 1] = spot[9 : 9 + rows, :].astype(BF16)
        ds_ref[1, t + 1] = tile.astype(BF16)
        ds_ref[2, t + 1] = spot[7 : 7 + rows, :].astype(BF16)
    wide = cells // 4
    lhs = _window(ds_ref, 0, wide)
    for kd, ref in ((0, gl_ref), (2, gr_ref)):
        _put_cells(ref, _dot_t(lhs, back_ref[kd]), wide, rows)


def _put_cells(ref, out, wide, rows):
    for g in range(wide):
        for j in range(2):
            ref[2 * g + j] = out[g * rows : (g + 1) * rows, LANES * j : LANES * (j + 1)].astype(ref.dtype)


def _own_two_kernel(delta_ref, own_ref, halo_ref, ds_ref, back_ref, gm_ref, out_ref):
    groups, rows = own_ref.shape[1] - 1, own_ref.shape[2]
    out_ref[1728:, :] = jnp.zeros((out_ref.shape[0] - 1728, LANES), BF16)
    _put_cells(gm_ref, _dot_t(_window(ds_ref, 0, groups // 2), back_ref[1]), groups // 2, rows)
    delta = delta_ref[...]
    flip = delta.astype(F32).T.astype(BF16)
    planes = (halo_ref.at[0], own_ref, halo_ref.at[1])
    for kk in range(9):
        full = _dot(flip, _cols(planes[kk // 3].at[kk % 3], 0, groups))
        band = full[0:LANES, :] + pltpu.roll(full[LANES:256, :], 192, 1)
        out_ref[192 * kk : 192 * (kk + 1), :] = band.T[0:192, :].astype(BF16)
    total = jnp.sum(delta.astype(F32), axis=0, keepdims=True)
    line = total[:, 0:LANES] + total[:, LANES:256]
    out_ref[1728:1744, :] = jnp.broadcast_to(line, (16, LANES)).astype(BF16)


def _grad_one_kernel(
    gm_ref, fl_ref, fr_ref, slope_ref, own_ref, halo_ref, two_ref, delta_ref, out_ref, sums, up0, up1, flip, one
):
    groups, rows = slope_ref.shape[1], slope_ref.shape[2]
    half = rows // 2
    lane = lax.broadcasted_iota(jnp.int32, (half, LANES), 1)
    sums[...] = jnp.zeros(sums.shape, F32)
    for g in range(groups):
        v = (gm_ref[g] + fl_ref[g].astype(F32) + fr_ref[g].astype(F32)) * 0.125
        turned = pltpu.roll(v, 64, 1)
        a = jnp.where(lane < 64, v, turned)
        b = jnp.where(lane < 64, turned, v)
        for j, (ref, val) in enumerate(((up0, a), (up1, b))):
            spot = ref.at[g % 2]
            spot[pl.ds(0, half, stride=2), :] = val
            spot[pl.ds(1, half, stride=2), :] = val
            lanes = slice(LANES * j, LANES * (j + 1))
            both = []
            for p in range(2):
                low = (spot[...] * slope_ref[p, g, :, lanes]).astype(BF16)
                delta_ref[p, g, :, lanes] = low
                both.append(low.astype(F32))
            sums[:, lanes] += jnp.sum(both[0].reshape(rows // 8, 8, LANES) + both[1].reshape(rows // 8, 8, LANES), axis=0)
            turn = jnp.concatenate(both, axis=0).T.astype(BF16)
            flip[lanes, 2 * rows * g : 2 * rows * (g + 1)] = turn
    one[...] = jnp.zeros(one.shape, BF16)
    planes = (halo_ref.at[0], own_ref.at[0], own_ref.at[1], halo_ref.at[1])
    for kd in range(3):
        for kh in range(3):
            kk = 3 * kd + kh
            a = planes[kd].at[kh]
            b = planes[kd + 1].at[kh]
            left = jnp.concatenate([r[g] for g in range(groups) for r in (a, b)], axis=0)
            right = jnp.concatenate([r[g + 1] for g in range(groups) for r in (a, b)], axis=0)
            full = _dot(flip[...], jnp.concatenate([left, right], axis=1))
            band = full[0:64, 0:LANES]
            for j in range(1, 4):
                band = band + pltpu.roll(full[64 * j : 64 * j + 64, :], 256 - 32 * j, 1)[:, 0:LANES]
            tall = band.T[0:96, :].astype(BF16)
            for r in range(0, 96, 48):
                at = 96 * kk + r
                side = at // 432
                one[at - 432 * side : at - 432 * side + 48, 64 * side : 64 * side + 64] = tall[r : r + 48, :]
    total = jnp.sum(sums[...], axis=0, keepdims=True)
    line = total[:, 0:LANES] + total[:, LANES:256]
    line = line + pltpu.roll(line, 64, 1)
    one[432:448, :] = jnp.broadcast_to(line, (16, LANES)).astype(BF16)
    count = out_ref.shape[0]
    rows_two, rows_one = two_ref.shape[0] // count, one.shape[0] // count
    for i in range(count):
        out_ref[i, 0:rows_two, :] = two_ref[i * rows_two : (i + 1) * rows_two, :]
        out_ref[i, rows_two:, :] = one[i * rows_one : (i + 1) * rows_one, :]


def _sides_kernel(delta_ref, back_ref, ds_ref, gl_ref, gr_ref, buf):
    groups, rows = delta_ref.shape[1], delta_ref.shape[2]
    cells = 2 * groups
    _zero_edges(buf, rows)
    zero = jnp.zeros((rows, LANES), BF16)
    for p in range(2):
        for kh in range(3):
            ds_ref[p, kh, 0] = zero
            ds_ref[p, kh, cells + 1] = zero

    def group(g, carry):
        for p in range(2):
            for j in range(2):
                low = delta_ref[p, g, :, LANES * j : LANES * (j + 1)]
                spot = buf.at[2 * p + j]
                spot[8 : 8 + rows, :] = low.astype(F32)
                t = 2 * g + j + 1
                ds_ref[p, 0, t] = spot[9 : 9 + rows, :].astype(BF16)
                ds_ref[p, 1, t] = low
                ds_ref[p, 2, t] = spot[7 : 7 + rows, :].astype(BF16)
        return carry

    lax.fori_loop(0, groups, group, 0)
    step = cells // 8

    def chunk(c, carry):
        for p, kd, ref in ((0, 0, gl_ref), (1, 2, gr_ref)):
            out = _dot_t(_window(ds_ref.at[p], c * step, step), back_ref[kd])
            ref[pl.ds(c * step, step)] = out.astype(BF16).reshape(step, rows, 256)
        return carry

    lax.fori_loop(0, 2, chunk, 0)


def _window(ref, first, count):
    parts = []
    for kh in range(3):
        for i in range(6):
            parts.append(jnp.concatenate([ref[kh, 4 * (first + g) + i] for g in range(count)], axis=0))
    return jnp.concatenate(parts, axis=1)


def _grad_input_kernel(ds_ref, back_ref, fl_ref, fr_ref, out_ref):
    wide, rows = fl_ref.shape[0], fl_ref.shape[1]
    for g in range(0, wide, 2):
        near = _window(ds_ref.at[0], g, 2)
        far = _window(ds_ref.at[1], g, 2)
        first = _dot_t(near, back_ref[1]) + _dot_t(far, back_ref[0])
        second = _dot_t(near, back_ref[2]) + _dot_t(far, back_ref[1])
        for s in range(2):
            for p, val, ref in ((0, first, fl_ref), (1, second, fr_ref)):
                whole = val[s * rows : (s + 1) * rows] + ref[g + s].astype(F32)
                out_ref[p, :, 256 * (g + s) : 256 * (g + s + 1)] = whole.astype(BF16)


def _split_kernel(scale_two, scale_one, rows_two, in_ref, out_ref, buf):
    count, rows = out_ref.shape[0], in_ref.shape[1]
    whole = jnp.sum(in_ref[...].astype(F32), axis=0)
    buf[0:rows_two, :] = whole[0:rows_two] * scale_two
    buf[rows_two:rows, :] = whole[rows_two:] * scale_one
    buf[rows:, :] = jnp.zeros((buf.shape[0] - rows, LANES), F32)
    part, tall = rows // count, out_ref.shape[1]
    for i in range(count):
        out_ref[i] = buf[i * part : i * part + tall, :].astype(BF16)


def _sum_kernel(in_ref, out_ref):
    whole = jnp.sum(in_ref[...].astype(F32), axis=0).astype(BF16)
    for i in range(out_ref.shape[0]):
        out_ref[i] = whole


def _join_kernel(in_ref, out_ref, buf):
    count, tall = in_ref.shape[0], in_ref.shape[1]
    rows = out_ref.shape[1]
    part = rows // count
    for i in range(count):
        buf[i * part : i * part + tall, :] = in_ref[i].astype(F32)
    whole = buf[0:rows, :].astype(BF16)
    for i in range(out_ref.shape[0]):
        out_ref[i] = whole


def _unpack_kernel(rows_two, rows_one, in_ref, w_two_ref, b_two_ref, w_one_ref, b_one_ref):
    two, one = w_two_ref.shape[0], w_one_ref.shape[0] // 2
    for i in range(in_ref.shape[0]):
        at = i * rows_two
        take = min(rows_two, max(two - at, 0))
        if take:
            w_two_ref[at : at + take, :] = in_ref[i, 0:take, :].astype(F32)
        if at <= two < at + rows_two:
            b_two_ref[...] = in_ref[i, two - at : two - at + 16, :].astype(F32)[0:1]
        at = i * rows_one
        take = min(rows_one, max(one - at, 0))
        if take:
            block = in_ref[i, rows_two : rows_two + take, :].astype(F32)
            w_one_ref[at : at + take, :] = block[:, 0:64]
            w_one_ref[one + at : one + at + take, :] = block[:, 64:128]
        if at <= one < at + rows_one:
            spot = rows_two + one - at
            b_one_ref[...] = in_ref[i, spot : spot + 16, :].astype(F32)[0:1, 0:64]


def _shape(shape, dtype):
    return jax.ShapeDtypeStruct(shape, dtype)


def _call(kernel, out, scratch, flops, moved, mib, args):
    return pl.pallas_call(
        kernel, out_shape=out, scratch_shapes=scratch, compiler_params=_params(mib), cost_estimate=_cost(flops, moved)
    )(*args)


def _round_up(value, unit):
    return -(-value // unit) * unit


def local(act_in, weight_one, bias_one, weight_two, bias_two, cotangent):
    _, slab, side, merged = act_in.shape
    half = side // 2
    c0, c1 = weight_one.shape[3:]
    c2 = weight_two.shape[4]
    dp, space = lax.axis_size("dp"), lax.axis_size("space")
    depth_all = slab * space
    scale_one = 16.0 / math.sqrt(dp * depth_all * side * side)
    scale_two = 1.0 / math.sqrt(dp * (depth_all // 2) * half * half)
    up = [(i, i + 1) for i in range(space - 1)]
    down = [(i + 1, i) for i in range(space - 1)]

    x = act_in.reshape(slab, side, merged)
    x0, x1 = x[0], x[slab - 1]
    from_left = lax.ppermute(x1, "space", up)
    from_right = lax.ppermute(x0, "space", down)
    w_one = weight_one.reshape(27, c0, c1)
    w_two = weight_two.reshape(27, c1, c2)
    groups = merged // LANES
    xs_shape = (2, 3, groups + 1, side, LANES)
    work = 2 * side * groups * 256
    rows_mid = groups * half
    work_two = rows_mid * 256 * 768
    tile = _shape((groups, half, LANES), BF16)
    tall = pltpu.VMEM((groups + 1, side + 16, LANES), F32)
    short = pltpu.VMEM((groups + 1, half + 16, LANES), F32)
    pre, xs_own, band_one = _call(
        _first_kernel,
        (_shape((2, groups, side, 256), F32), _shape(xs_shape, BF16), _shape((2304, 256), BF16)),
        [tall],
        2 * work * 1536,
        8 * MIB,
        16,
        (x0, x1, w_one),
    )
    back_one, band_two, back_two = _call(
        _prep_kernel,
        (_shape((3, 256, 2304), BF16), _shape((2304, 256), BF16), _shape((3, 256, 2304), BF16)),
        [],
        work * 768,
        8 * MIB,
        16,
        (w_one, w_two),
    )
    slope, pooled, xs_halo = _call(
        _second_kernel,
        (_shape((2, groups, side, 256), F32), tile, _shape(xs_shape, BF16)),
        [tall] + [pltpu.VMEM((4 * side, LANES), F32)] * 2,
        2 * work * 768,
        8 * MIB,
        16,
        (from_left, from_right, pre, band_one, bias_one.reshape(1, c1)),
    )
    pool_left = lax.ppermute(pooled, "space", up)
    pool_right = lax.ppermute(pooled, "space", down)
    ps_own, pre_two = _call(
        _mid_kernel,
        (_shape((3, groups + 1, half, LANES), BF16), _shape((rows_mid, 256), F32)),
        [short],
        2 * work_two,
        2 * MIB,
        12,
        (pooled, band_two, bias_two.reshape(1, c2)),
    )
    delta_two, ps_halo, ds_two, gp_left, gp_right = _call(
        _third_kernel,
        (
            _shape((rows_mid, 256), BF16),
            _shape((2, 3, groups + 1, half, LANES), BF16),
            _shape((3, 2 * groups + 2, half, LANES), BF16),
            tile,
            tile,
        ),
        [short],
        8 * work_two,
        4 * MIB,
        16,
        (pool_left, pool_right, pre_two, band_two, back_two, cotangent.reshape(half, -1)),
    )
    gp_from_right = lax.ppermute(gp_left, "space", down)
    gp_from_left = lax.ppermute(gp_right, "space", up)
    rows_two = _round_up(1744, 16 * dp)
    rows_one = _round_up(448, 16 * dp)
    gp_own, part_two = _call(
        _own_two_kernel,
        (_shape((groups, half, LANES), F32), _shape((rows_two, LANES), BF16)),
        [],
        8 * work_two,
        2 * MIB,
        16,
        (delta_two, ps_own, ps_halo, ds_two, back_two),
    )
    rows_all = (rows_two + rows_one) // dp
    delta_one, parts = _call(
        _grad_one_kernel,
        (_shape((2, groups, side, 256), BF16), _shape((dp, rows_all, LANES), BF16)),
        [pltpu.VMEM((8, 256), F32)]
        + [pltpu.VMEM((2, side, LANES), F32)] * 2
        + [pltpu.VMEM((256, 2 * groups * side), BF16), pltpu.VMEM((rows_one, LANES), BF16)],
        2 * work * 2304,
        4 * MIB,
        16,
        (gp_own, gp_from_left, gp_from_right, slope, xs_own, xs_halo, part_two),
    )
    rows_two //= dp
    rows_one //= dp
    met = lax.all_to_all(parts, "dp", 0, 0)
    ds, gx_left, gx_right = _call(
        _sides_kernel,
        (
            _shape((2, 3, 2 * groups + 2, side, LANES), BF16),
            _shape((groups // 2, side, 256), BF16),
            _shape((groups // 2, side, 256), BF16),
        ),
        [pltpu.VMEM((4, side + 16, LANES), F32)],
        2 * work * 2304 // 2,
        8 * MIB,
        16,
        (delta_one, back_one),
    )
    gx_from_right = lax.ppermute(gx_left, "space", down)
    gx_from_left = lax.ppermute(gx_right, "space", up)
    grad_x = _call(
        _grad_input_kernel,
        _shape((2, side, merged), BF16),
        [],
        2 * work * 2304,
        8 * MIB,
        16,
        (ds, back_one, gx_from_left, gx_from_right),
    )
    small = _shape((space, _round_up(rows_all // space, 16), LANES), BF16)
    pieces = _call(
        functools.partial(_split_kernel, scale_two, scale_one, rows_two),
        small,
        [pltpu.VMEM((rows_all + 16, LANES), F32)],
        0,
        MIB,
        8,
        (met,),
    )
    met = lax.all_to_all(pieces, "space", 0, 0)
    total = _call(_sum_kernel, small, [], 0, MIB, 8, (met,))
    met = lax.all_to_all(total, "space", 0, 0)
    joined = _call(
        _join_kernel, _shape((dp, rows_all, LANES), BF16), [pltpu.VMEM((rows_all + 16, LANES), F32)], 0, MIB, 8, (met,)
    )
    done = lax.all_to_all(joined, "dp", 0, 0)
    gw_two, gb_two, gw_one, gb_one = _call(
        functools.partial(_unpack_kernel, rows_two, rows_one),
        (
            _shape((27 * c1, c2), F32),
            _shape((1, c2), F32),
            _shape((27 * c0, c1), F32),
            _shape((1, c1), F32),
        ),
        [],
        0,
        MIB,
        8,
        (done,),
    )
    return (
        grad_x.reshape(act_in.shape),
        gw_one.reshape(weight_one.shape),
        gb_one.reshape(bias_one.shape),
        gw_two.reshape(weight_two.shape),
        gb_two.reshape(bias_two.shape),
    )


def solution(mesh):
    placed = (P("dp", "space", None, None), P(), P(), P(), P(), P("dp", "space", None, None))
    return jax.shard_map(
        local,
        mesh=mesh,
        in_specs=placed,
        out_specs=(P("dp", "space", None, None), P(), P(), P(), P()),
        check_vma=False,
    )
```

```python
import functools
import math

import jax
import jax.numpy as jnp
from jax import lax
from jax.experimental import pallas as pl
from jax.experimental.pallas import tpu as pltpu
from jax.sharding import PartitionSpec as P


F32 = jnp.float32
BF16 = jnp.bfloat16
LANES = 128
MIB = 1024 * 1024


def _params(mib):
    return pltpu.CompilerParams(vmem_limit_bytes=mib * MIB)


def _cost(flops, moved):
    return pl.CostEstimate(flops=int(flops), bytes_accessed=int(moved), transcendentals=0)


def _dot(a, b):
    return lax.dot_general(a, b, (((1,), (0,)), ((), ())), preferred_element_type=F32)


def _sigmoid(v):
    return 1.0 / (1.0 + jnp.exp(-v))


def _zero_edges(buf, rows):
    tiles = buf.shape[0]
    buf[:, 0:8, :] = jnp.zeros((tiles, 8, LANES), F32)
    buf[:, 8 + rows : 16 + rows, :] = jnp.zeros((tiles, 8, LANES), F32)


def _spread(load, tiles, rows, shift, buf, out):
    lane = lax.broadcasted_iota(jnp.int32, (rows, LANES), 1)
    before = jnp.zeros((rows, LANES), F32)
    for t in range(tiles + 1):
        now = pltpu.roll(load(t).astype(F32), shift, 1) if t < tiles else jnp.zeros((rows, LANES), F32)
        tile = jnp.where(lane < shift, before, now)
        buf[t, 8 : 8 + rows, :] = tile
        out[1, t] = tile.astype(BF16)
        before = now
    for t in range(tiles + 1):
        out[0, t] = buf[t, 7 : 7 + rows, :].astype(BF16)
        out[2, t] = buf[t, 9 : 9 + rows, :].astype(BF16)


def _cols(ref, first, groups):
    rows = ref.shape[1]
    a = ref[pl.ds(first, groups)].reshape(groups * rows, LANES)
    b = ref[pl.ds(first + 1, groups)].reshape(groups * rows, LANES)
    return jnp.concatenate([a, b], axis=1)


def _back_bands(w_ref, kk, out, size, first):
    chan_in, chan_out = w_ref.shape[1] // 3, w_ref.shape[2]
    flip = w_ref[kk].astype(F32).T.astype(BF16)
    for i in range(size // chan_out):
        start = chan_in * (i - first)
        low, high = max(start, 0), min(start + 3 * chan_in, 256)
        if low < high:
            r = size * (kk % 3) + chan_out * i
            out[r : r + chan_out, low:high] = flip[:, low - start : high - start]


def _prep_kernel(w_ref, band_two, back_two):
    band_two[...] = jnp.zeros(band_two.shape, BF16)
    back_two[...] = jnp.zeros(back_two.shape, BF16)
    for kk in range(9):
        for j in range(2):
            r = 256 * kk + 64 * j
            band_two[r : r + 192, LANES * j : LANES * (j + 1)] = w_ref[kk]
        _back_bands(w_ref, kk, back_two.at[kk // 3], 768, 2)


def _first_kernel(x0_ref, x1_ref, w_ref, pre_ref, xs_ref, band_ref, buf):
    rows, groups = x0_ref.shape[0], pre_ref.shape[1]
    band_ref[...] = jnp.zeros(band_ref.shape, BF16)
    for kk in range(9):
        for j in range(4):
            r = 256 * kk + 32 * j
            band_ref[r : r + 96, 64 * j : 64 * j + 64] = w_ref[kk]
    _zero_edges(buf, rows)
    for p, ref in enumerate((x0_ref, x1_ref)):
        _spread(lambda t, ref=ref: ref[:, LANES * t : LANES * (t + 1)], groups, rows, 32, buf, xs_ref.at[p])
    step = 8

    def chunk(c, carry):
        g = c * step
        sides = [[_cols(xs_ref.at[p, kh], g, step) for kh in range(3)] for p in range(2)]
        lhs = jnp.concatenate(sides[0] + sides[1], axis=1)
        pre_ref[0, pl.ds(g, step)] = _dot(lhs, band_ref[768:2304, :]).reshape(step, rows, 256)
        pre_ref[1, pl.ds(g, step)] = _dot(lhs, band_ref[0:1536, :]).reshape(step, rows, 256)
        return carry

    lax.fori_loop(0, groups // step, chunk, 0)


def _second_kernel(left_ref, right_ref, pre_ref, band_ref, bias_ref, slope_ref, pool_ref, xs_ref, buf, low, high):
    rows, groups = left_ref.shape[0], pre_ref.shape[1]
    half = rows // 2
    bias = jnp.concatenate([bias_ref[...]] * 4, axis=1)
    _zero_edges(buf, rows)
    for s, ref in enumerate((left_ref, right_ref)):
        _spread(lambda t, ref=ref: ref[:, LANES * t : LANES * (t + 1)], groups, rows, 32, buf, xs_ref.at[s])
    step = 4
    lane = lax.broadcasted_iota(jnp.int32, (step * half, LANES), 1)

    def chunk(c, carry):
        g = c * step
        total = None
        for p in range(2):
            lhs = jnp.concatenate([_cols(xs_ref.at[p, kh], g, step) for kh in range(3)], axis=1)
            more = _dot(lhs, band_ref[1536 * p : 1536 * p + 768, :])
            pre = pre_ref[p, pl.ds(g, step)].reshape(step * rows, 256) + more + bias
            sig = _sigmoid(pre)
            slope_ref[p, pl.ds(g, step)] = (sig * (1.0 + pre * (1.0 - sig))).reshape(step, rows, 256)
            act = pre * sig
            total = act if total is None else total + act
        for part, lanes in ((low, 0), (high, LANES)):
            v = total[:, lanes : lanes + LANES]
            part[...] = v + pltpu.roll(v, 64, 1)
        a = low[pl.ds(0, step * half, stride=2), :] + low[pl.ds(1, step * half, stride=2), :]
        b = high[pl.ds(0, step * half, stride=2), :] + high[pl.ds(1, step * half, stride=2), :]
        mean = jnp.where(lane < 64, a, b) * 0.125
        pool_ref[pl.ds(g, step)] = mean.astype(BF16).reshape(step, half, LANES)
        return carry

    lax.fori_loop(0, groups // step, chunk, 0)


def _mid_kernel(own_ref, band_ref, bias_ref, ps_ref, pre_ref, buf):
    groups, rows = own_ref.shape[0], own_ref.shape[1]
    _zero_edges(buf, rows)
    _spread(lambda t: own_ref[t], groups, rows, 64, buf, ps_ref)
    lhs = jnp.concatenate([_cols(ps_ref.at[kh], 0, groups) for kh in range(3)], axis=1)
    bias = jnp.concatenate([bias_ref[...]] * 2, axis=1)
    pre_ref[...] = _dot(lhs, band_ref[768:1536, :]) + bias


def _third_kernel(
    left_ref, right_ref, pre_ref, band_ref, back_ref, cot_ref, delta_ref, ps_ref, ds_ref, gl_ref, gr_ref, buf
):
    groups, rows = left_ref.shape[0], left_ref.shape[1]
    _zero_edges(buf, rows)
    for s, ref in enumerate((left_ref, right_ref)):
        _spread(lambda t, ref=ref: ref[t], groups, rows, 64, buf, ps_ref.at[s])
    near = jnp.concatenate([_cols(ps_ref.at[0, kh], 0, groups) for kh in range(3)], axis=1)
    far = jnp.concatenate([_cols(ps_ref.at[1, kh], 0, groups) for kh in range(3)], axis=1)
    pre = pre_ref[...] + _dot(near, band_ref[0:768, :]) + _dot(far, band_ref[1536:2304, :])
    sig = _sigmoid(pre)
    cot = jnp.concatenate([cot_ref[:, 256 * g : 256 * (g + 1)] for g in range(groups)], axis=0)
    delta = (cot.astype(F32) * (sig * (1.0 + pre * (1.0 - sig)))).astype(BF16)
    delta_ref[...] = delta
    again = delta.astype(F32)
    cells = 2 * groups
    zero = jnp.zeros((rows, LANES), BF16)
    for kh in range(3):
        ds_ref[kh, 0] = zero
        ds_ref[kh, cells + 1] = zero
    for t in range(cells):
        g, j = t // 2, t % 2
        tile = again[g * rows : (g + 1) * rows, LANES * j : LANES * (j + 1)]
        spot = buf.at[t % buf.shape[0]]
        spot[8 : 8 + rows, :] = tile
        ds_ref[0, t + 1] = spot[9 : 9 + rows, :].astype(BF16)
        ds_ref[1, t + 1] = tile.astype(BF16)
        ds_ref[2, t + 1] = spot[7 : 7 + rows, :].astype(BF16)
    wide = cells // 4
    lhs = _window(ds_ref, 0, wide)
    for kd, ref in ((0, gl_ref), (2, gr_ref)):
        _put_cells(ref, _dot(lhs, back_ref[kd]), wide, rows)


def _put_cells(ref, out, wide, rows):
    for g in range(wide):
        for j in range(2):
            ref[2 * g + j] = out[g * rows : (g + 1) * rows, LANES * j : LANES * (j + 1)].astype(ref.dtype)


def _own_two_kernel(delta_ref, own_ref, halo_ref, ds_ref, back_ref, gm_ref, out_ref):
    groups, rows = own_ref.shape[1] - 1, own_ref.shape[2]
    out_ref[1728:, :] = jnp.zeros((out_ref.shape[0] - 1728, LANES), BF16)
    _put_cells(gm_ref, _dot(_window(ds_ref, 0, groups // 2), back_ref[1]), groups // 2, rows)
    delta = delta_ref[...]
    flip = delta.astype(F32).T.astype(BF16)
    planes = (halo_ref.at[0], own_ref, halo_ref.at[1])
    for kk in range(9):
        full = _dot(flip, _cols(planes[kk // 3].at[kk % 3], 0, groups))
        band = full[0:LANES, :] + pltpu.roll(full[LANES:256, :], 192, 1)
        out_ref[192 * kk : 192 * (kk + 1), :] = band.T[0:192, :].astype(BF16)
    total = jnp.sum(delta.astype(F32), axis=0, keepdims=True)
    line = total[:, 0:LANES] + total[:, LANES:256]
    out_ref[1728:1744, :] = jnp.broadcast_to(line, (16, LANES)).astype(BF16)


def _grad_one_kernel(
    gm_ref, fl_ref, fr_ref, slope_ref, own_ref, halo_ref, two_ref, delta_ref, out_ref, sums, up0, up1, flip, one
):
    groups, rows = slope_ref.shape[1], slope_ref.shape[2]
    half = rows // 2
    lane = lax.broadcasted_iota(jnp.int32, (half, LANES), 1)
    sums[...] = jnp.zeros(sums.shape, F32)
    for g in range(groups):
        v = (gm_ref[g] + fl_ref[g].astype(F32) + fr_ref[g].astype(F32)) * 0.125
        turned = pltpu.roll(v, 64, 1)
        a = jnp.where(lane < 64, v, turned)
        b = jnp.where(lane < 64, turned, v)
        for j, (ref, val) in enumerate(((up0, a), (up1, b))):
            spot = ref.at[g % 2]
            spot[pl.ds(0, half, stride=2), :] = val
            spot[pl.ds(1, half, stride=2), :] = val
            lanes = slice(LANES * j, LANES * (j + 1))
            both = []
            for p in range(2):
                low = (spot[...] * slope_ref[p, g, :, lanes]).astype(BF16)
                delta_ref[p, g, :, lanes] = low
                both.append(low.astype(F32))
            sums[:, lanes] += jnp.sum(both[0].reshape(rows // 8, 8, LANES) + both[1].reshape(rows // 8, 8, LANES), axis=0)
            turn = jnp.concatenate(both, axis=0).T.astype(BF16)
            flip[lanes, 2 * rows * g : 2 * rows * (g + 1)] = turn
    one[...] = jnp.zeros(one.shape, BF16)
    planes = (halo_ref.at[0], own_ref.at[0], own_ref.at[1], halo_ref.at[1])
    for kd in range(3):
        for kh in range(3):
            kk = 3 * kd + kh
            a = planes[kd].at[kh]
            b = planes[kd + 1].at[kh]
            left = jnp.concatenate([r[g] for g in range(groups) for r in (a, b)], axis=0)
            right = jnp.concatenate([r[g + 1] for g in range(groups) for r in (a, b)], axis=0)
            full = _dot(flip[...], jnp.concatenate([left, right], axis=1))
            band = full[0:64, 0:LANES]
            for j in range(1, 4):
                band = band + pltpu.roll(full[64 * j : 64 * j + 64, :], 256 - 32 * j, 1)[:, 0:LANES]
            tall = band.T[0:96, :].astype(BF16)
            for r in range(0, 96, 48):
                at = 96 * kk + r
                side = at // 432
                one[at - 432 * side : at - 432 * side + 48, 64 * side : 64 * side + 64] = tall[r : r + 48, :]
    total = jnp.sum(sums[...], axis=0, keepdims=True)
    line = total[:, 0:LANES] + total[:, LANES:256]
    line = line + pltpu.roll(line, 64, 1)
    one[432:448, :] = jnp.broadcast_to(line, (16, LANES)).astype(BF16)
    count = out_ref.shape[0]
    rows_two, rows_one = two_ref.shape[0] // count, one.shape[0] // count
    for i in range(count):
        out_ref[i, 0:rows_two, :] = two_ref[i * rows_two : (i + 1) * rows_two, :]
        out_ref[i, rows_two:, :] = one[i * rows_one : (i + 1) * rows_one, :]


def _input_kernel(delta_ref, w_ref, gl_ref, own_ref, gr_ref, ds, back, buf):
    groups, rows = delta_ref.shape[1], delta_ref.shape[2]
    cells = 2 * groups
    back[...] = jnp.zeros(back.shape, BF16)
    for kk in range(9):
        _back_bands(w_ref, kk, back.at[kk // 3], 768, 3)
    _zero_edges(buf, rows)
    zero = jnp.zeros((rows, LANES), BF16)
    for p in range(2):
        for kh in range(3):
            ds[p, kh, 0] = zero
            ds[p, kh, cells + 1] = zero

    def group(g, carry):
        for p in range(2):
            for j in range(2):
                low = delta_ref[p, g, :, LANES * j : LANES * (j + 1)]
                spot = buf.at[2 * p + j]
                spot[8 : 8 + rows, :] = low.astype(F32)
                t = 2 * g + j + 1
                ds[p, 0, t] = spot[9 : 9 + rows, :].astype(BF16)
                ds[p, 1, t] = low
                ds[p, 2, t] = spot[7 : 7 + rows, :].astype(BF16)
        return carry

    lax.fori_loop(0, groups, group, 0)
    step = 4

    def chunk(c, carry):
        g = c * step
        spot = pl.ds(g, step)
        near = _window(ds.at[0], g, step)
        far = _window(ds.at[1], g, step)
        gl_ref[spot] = _dot(near, back[0]).astype(BF16).reshape(step, rows, 256)
        gr_ref[spot] = _dot(far, back[2]).astype(BF16).reshape(step, rows, 256)
        own_ref[0, spot] = (_dot(near, back[1]) + _dot(far, back[0])).reshape(step, rows, 256)
        own_ref[1, spot] = (_dot(near, back[2]) + _dot(far, back[1])).reshape(step, rows, 256)
        return carry

    lax.fori_loop(0, groups // 2 // step, chunk, 0)


def _window(ref, first, count):
    parts = []
    for kh in range(3):
        for i in range(6):
            parts.append(jnp.concatenate([ref[kh, 4 * (first + g) + i] for g in range(count)], axis=0))
    return jnp.concatenate(parts, axis=1)


def _edges_kernel(own_ref, fl_ref, fr_ref, out_ref):
    for g in range(fl_ref.shape[0]):
        for p, ref in ((0, fl_ref), (1, fr_ref)):
            whole = own_ref[p, g] + ref[g].astype(F32)
            out_ref[p, :, 256 * g : 256 * (g + 1)] = whole.astype(BF16)


def _split_kernel(scale_two, scale_one, rows_two, in_ref, out_ref, buf):
    count, rows = out_ref.shape[0], in_ref.shape[1]
    whole = jnp.sum(in_ref[...].astype(F32), axis=0)
    buf[0:rows_two, :] = whole[0:rows_two] * scale_two
    buf[rows_two:rows, :] = whole[rows_two:] * scale_one
    buf[rows:, :] = jnp.zeros((buf.shape[0] - rows, LANES), F32)
    part, tall = rows // count, out_ref.shape[1]
    for i in range(count):
        out_ref[i] = buf[i * part : i * part + tall, :].astype(BF16)


def _sum_kernel(in_ref, out_ref):
    whole = jnp.sum(in_ref[...].astype(F32), axis=0).astype(BF16)
    for i in range(out_ref.shape[0]):
        out_ref[i] = whole


def _join_kernel(in_ref, out_ref, buf):
    count, tall = in_ref.shape[0], in_ref.shape[1]
    rows = out_ref.shape[1]
    part = rows // count
    for i in range(count):
        buf[i * part : i * part + tall, :] = in_ref[i].astype(F32)
    whole = buf[0:rows, :].astype(BF16)
    for i in range(out_ref.shape[0]):
        out_ref[i] = whole


def _unpack_kernel(rows_two, rows_one, in_ref, w_two_ref, b_two_ref, w_one_ref, b_one_ref):
    two, one = w_two_ref.shape[0], w_one_ref.shape[0] // 2
    for i in range(in_ref.shape[0]):
        at = i * rows_two
        take = min(rows_two, max(two - at, 0))
        if take:
            w_two_ref[at : at + take, :] = in_ref[i, 0:take, :].astype(F32)
        if at <= two < at + rows_two:
            b_two_ref[...] = in_ref[i, two - at : two - at + 16, :].astype(F32)[0:1]
        at = i * rows_one
        take = min(rows_one, max(one - at, 0))
        if take:
            block = in_ref[i, rows_two : rows_two + take, :].astype(F32)
            w_one_ref[at : at + take, :] = block[:, 0:64]
            w_one_ref[one + at : one + at + take, :] = block[:, 64:128]
        if at <= one < at + rows_one:
            spot = rows_two + one - at
            b_one_ref[...] = in_ref[i, spot : spot + 16, :].astype(F32)[0:1, 0:64]


def _shape(shape, dtype):
    return jax.ShapeDtypeStruct(shape, dtype)


def _call(kernel, out, scratch, flops, moved, mib, args):
    return pl.pallas_call(
        kernel, out_shape=out, scratch_shapes=scratch, compiler_params=_params(mib), cost_estimate=_cost(flops, moved)
    )(*args)


def _round_up(value, unit):
    return -(-value // unit) * unit


def local(act_in, weight_one, bias_one, weight_two, bias_two, cotangent):
    _, slab, side, merged = act_in.shape
    half = side // 2
    c0, c1 = weight_one.shape[3:]
    c2 = weight_two.shape[4]
    dp, space = lax.axis_size("dp"), lax.axis_size("space")
    depth_all = slab * space
    scale_one = 16.0 / math.sqrt(dp * depth_all * side * side)
    scale_two = 1.0 / math.sqrt(dp * (depth_all // 2) * half * half)
    up = [(i, i + 1) for i in range(space - 1)]
    down = [(i + 1, i) for i in range(space - 1)]

    x = act_in.reshape(slab, side, merged)
    x0, x1 = x[0], x[slab - 1]
    from_left = lax.ppermute(x1, "space", up)
    from_right = lax.ppermute(x0, "space", down)
    w_one = weight_one.reshape(9, 3 * c0, c1)
    w_two = weight_two.reshape(9, 3 * c1, c2)
    groups = merged // LANES
    xs_shape = (2, 3, groups + 1, side, LANES)
    work = 2 * side * groups * 256
    rows_mid = groups * half
    work_two = rows_mid * 256 * 768
    tile = _shape((groups, half, LANES), BF16)
    tall = pltpu.VMEM((groups + 1, side + 16, LANES), F32)
    short = pltpu.VMEM((groups + 1, half + 16, LANES), F32)
    pre, xs_own, band_one = _call(
        _first_kernel,
        (_shape((2, groups, side, 256), F32), _shape(xs_shape, BF16), _shape((2304, 256), BF16)),
        [tall],
        2 * work * 1536,
        8 * MIB,
        16,
        (x0, x1, w_one),
    )
    band_two, back_two = _call(
        _prep_kernel, (_shape((2304, 256), BF16), _shape((3, 2304, 256), BF16)), [], work * 768, 8 * MIB, 12, (w_two,)
    )
    slope, pooled, xs_halo = _call(
        _second_kernel,
        (_shape((2, groups, side, 256), F32), tile, _shape(xs_shape, BF16)),
        [tall] + [pltpu.VMEM((4 * side, LANES), F32)] * 2,
        2 * work * 768,
        8 * MIB,
        16,
        (from_left, from_right, pre, band_one, bias_one.reshape(1, c1)),
    )
    pool_left = lax.ppermute(pooled, "space", up)
    pool_right = lax.ppermute(pooled, "space", down)
    ps_own, pre_two = _call(
        _mid_kernel,
        (_shape((3, groups + 1, half, LANES), BF16), _shape((rows_mid, 256), F32)),
        [short],
        2 * work_two,
        2 * MIB,
        12,
        (pooled, band_two, bias_two.reshape(1, c2)),
    )
    delta_two, ps_halo, ds_two, gp_left, gp_right = _call(
        _third_kernel,
        (
            _shape((rows_mid, 256), BF16),
            _shape((2, 3, groups + 1, half, LANES), BF16),
            _shape((3, 2 * groups + 2, half, LANES), BF16),
            tile,
            tile,
        ),
        [short],
        8 * work_two,
        4 * MIB,
        16,
        (pool_left, pool_right, pre_two, band_two, back_two, cotangent.reshape(half, -1)),
    )
    gp_from_right = lax.ppermute(gp_left, "space", down)
    gp_from_left = lax.ppermute(gp_right, "space", up)
    rows_two = _round_up(1744, 16 * dp)
    rows_one = _round_up(448, 16 * dp)
    gp_own, part_two = _call(
        _own_two_kernel,
        (_shape((groups, half, LANES), F32), _shape((rows_two, LANES), BF16)),
        [],
        8 * work_two,
        2 * MIB,
        16,
        (delta_two, ps_own, ps_halo, ds_two, back_two),
    )
    rows_all = (rows_two + rows_one) // dp
    delta_one, parts = _call(
        _grad_one_kernel,
        (_shape((2, groups, side, 256), BF16), _shape((dp, rows_all, LANES), BF16)),
        [pltpu.VMEM((8, 256), F32)]
        + [pltpu.VMEM((2, side, LANES), F32)] * 2
        + [pltpu.VMEM((256, 2 * groups * side), BF16), pltpu.VMEM((rows_one, LANES), BF16)],
        2 * work * 2304,
        4 * MIB,
        16,
        (gp_own, gp_from_left, gp_from_right, slope, xs_own, xs_halo, part_two),
    )
    rows_two //= dp
    rows_one //= dp
    met = lax.all_to_all(parts, "dp", 0, 0)
    block = _shape((groups // 2, side, 256), BF16)
    gx_left, gx_own, gx_right = _call(
        _input_kernel,
        (block, _shape((2, groups // 2, side, 256), F32), block),
        [
            pltpu.VMEM((2, 3, 2 * groups + 2, side, LANES), BF16),
            pltpu.VMEM((3, 2304, 256), BF16),
            pltpu.VMEM((4, side + 16, LANES), F32),
        ],
        2 * work * 2304 // 2,
        8 * MIB,
        20,
        (delta_one, w_one),
    )
    gx_from_right = lax.ppermute(gx_left, "space", down)
    gx_from_left = lax.ppermute(gx_right, "space", up)
    grad_x = _call(
        _edges_kernel,
        _shape((2, side, merged), BF16),
        [],
        2 * work * 128,
        4 * MIB,
        12,
        (gx_own, gx_from_left, gx_from_right),
    )
    small = _shape((space, _round_up(rows_all // space, 16), LANES), BF16)
    pieces = _call(
        functools.partial(_split_kernel, scale_two, scale_one, rows_two),
        small,
        [pltpu.VMEM((rows_all + 16, LANES), F32)],
        0,
        MIB,
        8,
        (met,),
    )
    met = lax.all_to_all(pieces, "space", 0, 0)
    total = _call(_sum_kernel, small, [], 0, MIB, 8, (met,))
    met = lax.all_to_all(total, "space", 0, 0)
    joined = _call(
        _join_kernel, _shape((dp, rows_all, LANES), BF16), [pltpu.VMEM((rows_all + 16, LANES), F32)], 0, MIB, 8, (met,)
    )
    done = lax.all_to_all(joined, "dp", 0, 0)
    gw_two, gb_two, gw_one, gb_one = _call(
        functools.partial(_unpack_kernel, rows_two, rows_one),
        (
            _shape((27 * c1, c2), F32),
            _shape((1, c2), F32),
            _shape((27 * c0, c1), F32),
            _shape((1, c1), F32),
        ),
        [],
        0,
        MIB,
        8,
        (done,),
    )
    return (
        grad_x.reshape(act_in.shape),
        gw_one.reshape(weight_one.shape),
        gb_one.reshape(bias_one.shape),
        gw_two.reshape(weight_two.shape),
        gb_two.reshape(bias_two.shape),
    )


def solution(mesh):
    placed = (P("dp", "space", None, None), P(), P(), P(), P(), P("dp", "space", None, None))
    return jax.shard_map(
        local,
        mesh=mesh,
        in_specs=placed,
        out_specs=(P("dp", "space", None, None), P(), P(), P(), P()),
        check_vma=False,
    )
```

```python
import functools
import math

import jax
import jax.numpy as jnp
from jax import lax
from jax.experimental import pallas as pl
from jax.experimental.pallas import tpu as pltpu
from jax.sharding import PartitionSpec as P


F32 = jnp.float32
BF16 = jnp.bfloat16
LANES = 128
MIB = 1024 * 1024


def _params(mib):
    return pltpu.CompilerParams(vmem_limit_bytes=mib * MIB)


def _cost(flops, moved):
    return pl.CostEstimate(flops=int(flops), bytes_accessed=int(moved), transcendentals=0)


def _dot(a, b):
    return lax.dot_general(a, b, (((1,), (0,)), ((), ())), preferred_element_type=F32)


def _sigmoid(v):
    return 1.0 / (1.0 + jnp.exp(-v))


def _zero_edges(buf, rows):
    tiles = buf.shape[0]
    buf[:, 0:8, :] = jnp.zeros((tiles, 8, LANES), F32)
    buf[:, 8 + rows : 16 + rows, :] = jnp.zeros((tiles, 8, LANES), F32)


def _spread(load, tiles, rows, shift, buf, out):
    lane = lax.broadcasted_iota(jnp.int32, (rows, LANES), 1)
    before = jnp.zeros((rows, LANES), F32)
    for t in range(tiles + 1):
        now = pltpu.roll(load(t).astype(F32), shift, 1) if t < tiles else jnp.zeros((rows, LANES), F32)
        tile = jnp.where(lane < shift, before, now)
        buf[t, 8 : 8 + rows, :] = tile
        out[1, t] = tile.astype(BF16)
        before = now
    for t in range(tiles + 1):
        out[0, t] = buf[t, 7 : 7 + rows, :].astype(BF16)
        out[2, t] = buf[t, 9 : 9 + rows, :].astype(BF16)


def _cols(ref, first, groups):
    rows = ref.shape[1]
    a = ref[pl.ds(first, groups)].reshape(groups * rows, LANES)
    b = ref[pl.ds(first + 1, groups)].reshape(groups * rows, LANES)
    return jnp.concatenate([a, b], axis=1)


def _back_bands(w_ref, kk, out, size, first):
    chan_in, chan_out = w_ref.shape[1] // 3, w_ref.shape[2]
    flip = w_ref[kk].astype(F32).T.astype(BF16)
    for i in range(size // chan_out):
        start = chan_in * (i - first)
        low, high = max(start, 0), min(start + 3 * chan_in, 256)
        if low < high:
            r = size * (kk % 3) + chan_out * i
            out[r : r + chan_out, low:high] = flip[:, low - start : high - start]


def _prep_kernel(w_ref, band_two, back_two):
    band_two[...] = jnp.zeros(band_two.shape, BF16)
    back_two[...] = jnp.zeros(back_two.shape, BF16)
    for kk in range(9):
        for j in range(2):
            r = 256 * kk + 64 * j
            band_two[r : r + 192, LANES * j : LANES * (j + 1)] = w_ref[kk]
        _back_bands(w_ref, kk, back_two.at[kk // 3], 768, 2)


def _first_kernel(x0_ref, x1_ref, w_ref, pre_ref, xs_ref, band_ref, buf):
    rows, groups = x0_ref.shape[0], pre_ref.shape[1]
    band_ref[...] = jnp.zeros(band_ref.shape, BF16)
    for kk in range(9):
        for j in range(4):
            r = 256 * kk + 32 * j
            band_ref[r : r + 96, 64 * j : 64 * j + 64] = w_ref[kk]
    _zero_edges(buf, rows)
    for p, ref in enumerate((x0_ref, x1_ref)):
        _spread(lambda t, ref=ref: ref[:, LANES * t : LANES * (t + 1)], groups, rows, 32, buf, xs_ref.at[p])
    step = 8

    def chunk(c, carry):
        g = c * step
        sides = [[_cols(xs_ref.at[p, kh], g, step) for kh in range(3)] for p in range(2)]
        lhs = jnp.concatenate(sides[0] + sides[1], axis=1)
        pre_ref[0, pl.ds(g, step)] = _dot(lhs, band_ref[768:2304, :]).reshape(step, rows, 256)
        pre_ref[1, pl.ds(g, step)] = _dot(lhs, band_ref[0:1536, :]).reshape(step, rows, 256)
        return carry

    lax.fori_loop(0, groups // step, chunk, 0)


def _second_kernel(left_ref, right_ref, pre_ref, band_ref, bias_ref, slope_ref, pool_ref, xs_ref, buf, low, high):
    rows, groups = left_ref.shape[0], pre_ref.shape[1]
    half = rows // 2
    bias = jnp.concatenate([bias_ref[...]] * 4, axis=1)
    _zero_edges(buf, rows)
    for s, ref in enumerate((left_ref, right_ref)):
        _spread(lambda t, ref=ref: ref[:, LANES * t : LANES * (t + 1)], groups, rows, 32, buf, xs_ref.at[s])
    step = 4
    lane = lax.broadcasted_iota(jnp.int32, (step * half, LANES), 1)

    def chunk(c, carry):
        g = c * step
        total = None
        for p in range(2):
            lhs = jnp.concatenate([_cols(xs_ref.at[p, kh], g, step) for kh in range(3)], axis=1)
            more = _dot(lhs, band_ref[1536 * p : 1536 * p + 768, :])
            pre = pre_ref[p, pl.ds(g, step)].reshape(step * rows, 256) + more + bias
            sig = _sigmoid(pre)
            slope_ref[p, pl.ds(g, step)] = (sig * (1.0 + pre * (1.0 - sig))).reshape(step, rows, 256)
            act = pre * sig
            total = act if total is None else total + act
        for part, lanes in ((low, 0), (high, LANES)):
            v = total[:, lanes : lanes + LANES]
            part[...] = v + pltpu.roll(v, 64, 1)
        a = low[pl.ds(0, step * half, stride=2), :] + low[pl.ds(1, step * half, stride=2), :]
        b = high[pl.ds(0, step * half, stride=2), :] + high[pl.ds(1, step * half, stride=2), :]
        mean = jnp.where(lane < 64, a, b) * 0.125
        pool_ref[pl.ds(g, step)] = mean.astype(BF16).reshape(step, half, LANES)
        return carry

    lax.fori_loop(0, groups // step, chunk, 0)


def _mid_kernel(own_ref, band_ref, bias_ref, ps_ref, pre_ref, buf):
    groups, rows = own_ref.shape[0], own_ref.shape[1]
    _zero_edges(buf, rows)
    _spread(lambda t: own_ref[t], groups, rows, 64, buf, ps_ref)
    lhs = jnp.concatenate([_cols(ps_ref.at[kh], 0, groups) for kh in range(3)], axis=1)
    bias = jnp.concatenate([bias_ref[...]] * 2, axis=1)
    pre_ref[...] = _dot(lhs, band_ref[768:1536, :]) + bias


def _third_kernel(
    left_ref, right_ref, pre_ref, band_ref, back_ref, cot_ref, delta_ref, ps_ref, ds_ref, gl_ref, gr_ref, buf
):
    groups, rows = left_ref.shape[0], left_ref.shape[1]
    _zero_edges(buf, rows)
    for s, ref in enumerate((left_ref, right_ref)):
        _spread(lambda t, ref=ref: ref[t], groups, rows, 64, buf, ps_ref.at[s])
    near = jnp.concatenate([_cols(ps_ref.at[0, kh], 0, groups) for kh in range(3)], axis=1)
    far = jnp.concatenate([_cols(ps_ref.at[1, kh], 0, groups) for kh in range(3)], axis=1)
    pre = pre_ref[...] + _dot(near, band_ref[0:768, :]) + _dot(far, band_ref[1536:2304, :])
    sig = _sigmoid(pre)
    cot = jnp.concatenate([cot_ref[:, 256 * g : 256 * (g + 1)] for g in range(groups)], axis=0)
    delta = (cot.astype(F32) * (sig * (1.0 + pre * (1.0 - sig)))).astype(BF16)
    delta_ref[...] = delta
    again = delta.astype(F32)
    cells = 2 * groups
    zero = jnp.zeros((rows, LANES), BF16)
    for kh in range(3):
        ds_ref[kh, 0] = zero
        ds_ref[kh, cells + 1] = zero
    for t in range(cells):
        g, j = t // 2, t % 2
        tile = again[g * rows : (g + 1) * rows, LANES * j : LANES * (j + 1)]
        spot = buf.at[t % buf.shape[0]]
        spot[8 : 8 + rows, :] = tile
        ds_ref[0, t + 1] = spot[9 : 9 + rows, :].astype(BF16)
        ds_ref[1, t + 1] = tile.astype(BF16)
        ds_ref[2, t + 1] = spot[7 : 7 + rows, :].astype(BF16)
    wide = cells // 4
    lhs = _window(ds_ref, 0, wide)
    for kd, ref in ((0, gl_ref), (2, gr_ref)):
        _put_cells(ref, _dot(lhs, back_ref[kd]), wide, rows)


def _put_cells(ref, out, wide, rows):
    for g in range(wide):
        for j in range(2):
            ref[2 * g + j] = out[g * rows : (g + 1) * rows, LANES * j : LANES * (j + 1)].astype(ref.dtype)


def _own_two_kernel(delta_ref, own_ref, halo_ref, ds_ref, back_ref, gm_ref, out_ref):
    groups, rows = own_ref.shape[1] - 1, own_ref.shape[2]
    out_ref[1728:, :] = jnp.zeros((out_ref.shape[0] - 1728, LANES), BF16)
    _put_cells(gm_ref, _dot(_window(ds_ref, 0, groups // 2), back_ref[1]), groups // 2, rows)
    delta = delta_ref[...]
    flip = delta.astype(F32).T.astype(BF16)
    planes = (halo_ref.at[0], own_ref, halo_ref.at[1])
    for kk in range(9):
        full = _dot(flip, _cols(planes[kk // 3].at[kk % 3], 0, groups))
        band = full[0:LANES, :] + pltpu.roll(full[LANES:256, :], 192, 1)
        out_ref[192 * kk : 192 * (kk + 1), :] = band.T[0:192, :].astype(BF16)
    total = jnp.sum(delta.astype(F32), axis=0, keepdims=True)
    line = total[:, 0:LANES] + total[:, LANES:256]
    out_ref[1728:1744, :] = jnp.broadcast_to(line, (16, LANES)).astype(BF16)


def _grad_one_kernel(
    gm_ref, fl_ref, fr_ref, slope_ref, own_ref, halo_ref, two_ref, delta_ref, out_ref, sums, up0, up1, flip, one
):
    groups, rows = slope_ref.shape[1], slope_ref.shape[2]
    half = rows // 2
    lane = lax.broadcasted_iota(jnp.int32, (half, LANES), 1)
    sums[...] = jnp.zeros(sums.shape, F32)
    for g in range(groups):
        v = (gm_ref[g] + fl_ref[g].astype(F32) + fr_ref[g].astype(F32)) * 0.125
        turned = pltpu.roll(v, 64, 1)
        a = jnp.where(lane < 64, v, turned)
        b = jnp.where(lane < 64, turned, v)
        for j, (ref, val) in enumerate(((up0, a), (up1, b))):
            spot = ref.at[g % 2]
            spot[pl.ds(0, half, stride=2), :] = val
            spot[pl.ds(1, half, stride=2), :] = val
            lanes = slice(LANES * j, LANES * (j + 1))
            both = []
            for p in range(2):
                low = (spot[...] * slope_ref[p, g, :, lanes]).astype(BF16)
                delta_ref[p, g, :, lanes] = low
                both.append(low.astype(F32))
            sums[:, lanes] += jnp.sum(both[0].reshape(rows // 8, 8, LANES) + both[1].reshape(rows // 8, 8, LANES), axis=0)
            turn = jnp.concatenate(both, axis=0).T.astype(BF16)
            flip[lanes, 2 * rows * g : 2 * rows * (g + 1)] = turn
    one[...] = jnp.zeros(one.shape, BF16)
    planes = (halo_ref.at[0], own_ref.at[0], own_ref.at[1], halo_ref.at[1])
    for kd in range(3):
        for kh in range(3):
            kk = 3 * kd + kh
            a = planes[kd].at[kh]
            b = planes[kd + 1].at[kh]
            left = jnp.concatenate([r[g] for g in range(groups) for r in (a, b)], axis=0)
            right = jnp.concatenate([r[g + 1] for g in range(groups) for r in (a, b)], axis=0)
            full = _dot(flip[...], jnp.concatenate([left, right], axis=1))
            band = full[0:64, 0:LANES]
            for j in range(1, 4):
                band = band + pltpu.roll(full[64 * j : 64 * j + 64, :], 256 - 32 * j, 1)[:, 0:LANES]
            tall = band.T[0:96, :].astype(BF16)
            for r in range(0, 96, 48):
                at = 96 * kk + r
                side = at // 432
                one[at - 432 * side : at - 432 * side + 48, 64 * side : 64 * side + 64] = tall[r : r + 48, :]
    total = jnp.sum(sums[...], axis=0, keepdims=True)
    line = total[:, 0:LANES] + total[:, LANES:256]
    line = line + pltpu.roll(line, 64, 1)
    one[432:448, :] = jnp.broadcast_to(line, (16, LANES)).astype(BF16)
    count = out_ref.shape[0]
    rows_two, rows_one = two_ref.shape[0] // count, one.shape[0] // count
    for i in range(count):
        out_ref[i, 0:rows_two, :] = two_ref[i * rows_two : (i + 1) * rows_two, :]
        out_ref[i, rows_two:, :] = one[i * rows_one : (i + 1) * rows_one, :]


def _input_kernel(delta_ref, w_ref, gl_ref, own_ref, gr_ref, ds, back, buf):
    groups, rows = delta_ref.shape[1], delta_ref.shape[2]
    cells = 2 * groups
    back[...] = jnp.zeros(back.shape, BF16)
    for kk in range(9):
        _back_bands(w_ref, kk, back.at[kk // 3], 768, 3)
    _zero_edges(buf, rows)
    zero = jnp.zeros((rows, LANES), BF16)
    for p in range(2):
        for kh in range(3):
            ds[p, kh, 0] = zero
            ds[p, kh, cells + 1] = zero

    def group(g, carry):
        for p in range(2):
            for j in range(2):
                low = delta_ref[p, g, :, LANES * j : LANES * (j + 1)]
                spot = buf.at[2 * p + j]
                spot[8 : 8 + rows, :] = low.astype(F32)
                t = 2 * g + j + 1
                ds[p, 0, t] = spot[9 : 9 + rows, :].astype(BF16)
                ds[p, 1, t] = low
                ds[p, 2, t] = spot[7 : 7 + rows, :].astype(BF16)
        return carry

    lax.fori_loop(0, groups, group, 0)
    step = 4

    def chunk(c, carry):
        g = c * step
        spot = pl.ds(g, step)
        near = _window(ds.at[0], g, step)
        far = _window(ds.at[1], g, step)
        gl_ref[spot] = _dot(near, back[0]).astype(BF16).reshape(step, rows, 256)
        gr_ref[spot] = _dot(far, back[2]).astype(BF16).reshape(step, rows, 256)
        for p in range(2):
            own = _dot(near, back[1 + p]) + _dot(far, back[p])
            own_ref[p, spot] = own.astype(BF16).reshape(step, rows, 256)
        return carry

    lax.fori_loop(0, groups // 2 // step, chunk, 0)


def _window(ref, first, count):
    parts = []
    for kh in range(3):
        for i in range(6):
            parts.append(jnp.concatenate([ref[kh, 4 * (first + g) + i] for g in range(count)], axis=0))
    return jnp.concatenate(parts, axis=1)


def _edges_kernel(own_ref, fl_ref, fr_ref, out_ref):
    for g in range(fl_ref.shape[0]):
        for p, ref in ((0, fl_ref), (1, fr_ref)):
            whole = own_ref[p, g].astype(F32) + ref[g].astype(F32)
            out_ref[p, :, 256 * g : 256 * (g + 1)] = whole.astype(BF16)


def _split_kernel(scale_two, scale_one, rows_two, in_ref, out_ref):
    whole = jnp.sum(in_ref[...].astype(F32), axis=0)
    out_ref[0:rows_two, :] = (whole[0:rows_two] * scale_two).astype(BF16)
    out_ref[rows_two:, :] = (whole[rows_two:] * scale_one).astype(BF16)


def _add_kernel(a_ref, b_ref, out_ref):
    out_ref[...] = (a_ref[...].astype(F32) + b_ref[...].astype(F32)).astype(BF16)


def _join_kernel(a_ref, b_ref, out_ref):
    whole = (a_ref[...].astype(F32) + b_ref[...].astype(F32)).astype(BF16)
    for i in range(out_ref.shape[0]):
        out_ref[i] = whole


def _unpack_kernel(rows_two, rows_one, in_ref, w_two_ref, b_two_ref, w_one_ref, b_one_ref):
    two, one = w_two_ref.shape[0], w_one_ref.shape[0] // 2
    for i in range(in_ref.shape[0]):
        at = i * rows_two
        take = min(rows_two, max(two - at, 0))
        if take:
            w_two_ref[at : at + take, :] = in_ref[i, 0:take, :].astype(F32)
        if at <= two < at + rows_two:
            b_two_ref[...] = in_ref[i, two - at : two - at + 16, :].astype(F32)[0:1]
        at = i * rows_one
        take = min(rows_one, max(one - at, 0))
        if take:
            block = in_ref[i, rows_two : rows_two + take, :].astype(F32)
            w_one_ref[at : at + take, :] = block[:, 0:64]
            w_one_ref[one + at : one + at + take, :] = block[:, 64:128]
        if at <= one < at + rows_one:
            spot = rows_two + one - at
            b_one_ref[...] = in_ref[i, spot : spot + 16, :].astype(F32)[0:1, 0:64]


def _shape(shape, dtype):
    return jax.ShapeDtypeStruct(shape, dtype)


def _call(kernel, out, scratch, flops, moved, mib, args):
    return pl.pallas_call(
        kernel, out_shape=out, scratch_shapes=scratch, compiler_params=_params(mib), cost_estimate=_cost(flops, moved)
    )(*args)


def _round_up(value, unit):
    return -(-value // unit) * unit


def local(act_in, weight_one, bias_one, weight_two, bias_two, cotangent):
    _, slab, side, merged = act_in.shape
    half = side // 2
    c0, c1 = weight_one.shape[3:]
    c2 = weight_two.shape[4]
    dp, space = lax.axis_size("dp"), lax.axis_size("space")
    depth_all = slab * space
    scale_one = 16.0 / math.sqrt(dp * depth_all * side * side)
    scale_two = 1.0 / math.sqrt(dp * (depth_all // 2) * half * half)
    up = [(i, i + 1) for i in range(space - 1)]
    down = [(i + 1, i) for i in range(space - 1)]

    x = act_in.reshape(slab, side, merged)
    x0, x1 = x[0], x[slab - 1]
    from_left = lax.ppermute(x1, "space", up)
    from_right = lax.ppermute(x0, "space", down)
    w_one = weight_one.reshape(9, 3 * c0, c1)
    w_two = weight_two.reshape(9, 3 * c1, c2)
    groups = merged // LANES
    xs_shape = (2, 3, groups + 1, side, LANES)
    work = 2 * side * groups * 256
    rows_mid = groups * half
    work_two = rows_mid * 256 * 768
    tile = _shape((groups, half, LANES), BF16)
    tall = pltpu.VMEM((groups + 1, side + 16, LANES), F32)
    short = pltpu.VMEM((groups + 1, half + 16, LANES), F32)
    pre, xs_own, band_one = _call(
        _first_kernel,
        (_shape((2, groups, side, 256), F32), _shape(xs_shape, BF16), _shape((2304, 256), BF16)),
        [tall],
        2 * work * 1536,
        8 * MIB,
        16,
        (x0, x1, w_one),
    )
    band_two, back_two = _call(
        _prep_kernel, (_shape((2304, 256), BF16), _shape((3, 2304, 256), BF16)), [], work * 768, 8 * MIB, 12, (w_two,)
    )
    slope, pooled, xs_halo = _call(
        _second_kernel,
        (_shape((2, groups, side, 256), F32), tile, _shape(xs_shape, BF16)),
        [tall] + [pltpu.VMEM((4 * side, LANES), F32)] * 2,
        2 * work * 768,
        8 * MIB,
        16,
        (from_left, from_right, pre, band_one, bias_one.reshape(1, c1)),
    )
    pool_left = lax.ppermute(pooled, "space", up)
    pool_right = lax.ppermute(pooled, "space", down)
    ps_own, pre_two = _call(
        _mid_kernel,
        (_shape((3, groups + 1, half, LANES), BF16), _shape((rows_mid, 256), F32)),
        [short],
        2 * work_two,
        2 * MIB,
        12,
        (pooled, band_two, bias_two.reshape(1, c2)),
    )
    delta_two, ps_halo, ds_two, gp_left, gp_right = _call(
        _third_kernel,
        (
            _shape((rows_mid, 256), BF16),
            _shape((2, 3, groups + 1, half, LANES), BF16),
            _shape((3, 2 * groups + 2, half, LANES), BF16),
            tile,
            tile,
        ),
        [short],
        8 * work_two,
        4 * MIB,
        16,
        (pool_left, pool_right, pre_two, band_two, back_two, cotangent.reshape(half, -1)),
    )
    gp_from_right = lax.ppermute(gp_left, "space", down)
    gp_from_left = lax.ppermute(gp_right, "space", up)
    rows_two = _round_up(1744, 16 * dp)
    rows_one = _round_up(448, 16 * dp)
    gp_own, part_two = _call(
        _own_two_kernel,
        (_shape((groups, half, LANES), F32), _shape((rows_two, LANES), BF16)),
        [],
        8 * work_two,
        2 * MIB,
        16,
        (delta_two, ps_own, ps_halo, ds_two, back_two),
    )
    rows_all = (rows_two + rows_one) // dp
    delta_one, parts = _call(
        _grad_one_kernel,
        (_shape((2, groups, side, 256), BF16), _shape((dp, rows_all, LANES), BF16)),
        [pltpu.VMEM((8, 256), F32)]
        + [pltpu.VMEM((2, side, LANES), F32)] * 2
        + [pltpu.VMEM((256, 2 * groups * side), BF16), pltpu.VMEM((rows_one, LANES), BF16)],
        2 * work * 2304,
        4 * MIB,
        16,
        (gp_own, gp_from_left, gp_from_right, slope, xs_own, xs_halo, part_two),
    )
    rows_two //= dp
    rows_one //= dp
    met = lax.all_to_all(parts, "dp", 0, 0)
    block = _shape((groups // 2, side, 256), BF16)
    gx_left, gx_own, gx_right = _call(
        _input_kernel,
        (block, _shape((2, groups // 2, side, 256), BF16), block),
        [
            pltpu.VMEM((2, 3, 2 * groups + 2, side, LANES), BF16),
            pltpu.VMEM((3, 2304, 256), BF16),
            pltpu.VMEM((4, side + 16, LANES), F32),
        ],
        2 * work * 2304 // 2,
        8 * MIB,
        20,
        (delta_one, w_one),
    )
    gx_from_right = lax.ppermute(gx_left, "space", down)
    gx_from_left = lax.ppermute(gx_right, "space", up)
    grad_x = _call(
        _edges_kernel,
        _shape((2, side, merged), BF16),
        [],
        2 * work * 128,
        4 * MIB,
        12,
        (gx_own, gx_from_left, gx_from_right),
    )
    flat = _shape((rows_all, LANES), BF16)
    mine = _call(functools.partial(_split_kernel, scale_two, scale_one, rows_two), flat, [], 0, MIB, 8, (met,))
    far = [space // 2] + [2**k for k in range(space.bit_length() - 2)]
    for k, gap in enumerate(far):
        other = lax.ppermute(mine, "space", [(i, i ^ gap) for i in range(space)])
        if k < len(far) - 1:
            mine = _call(_add_kernel, flat, [], 0, MIB, 8, (mine, other))
    joined = _call(_join_kernel, _shape((dp, rows_all, LANES), BF16), [], 0, MIB, 8, (mine, other))
    done = lax.all_to_all(joined, "dp", 0, 0)
    gw_two, gb_two, gw_one, gb_one = _call(
        functools.partial(_unpack_kernel, rows_two, rows_one),
        (
            _shape((27 * c1, c2), F32),
            _shape((1, c2), F32),
            _shape((27 * c0, c1), F32),
            _shape((1, c1), F32),
        ),
        [],
        0,
        MIB,
        8,
        (done,),
    )
    return (
        grad_x.reshape(act_in.shape),
        gw_one.reshape(weight_one.shape),
        gb_one.reshape(bias_one.shape),
        gw_two.reshape(weight_two.shape),
        gb_two.reshape(bias_two.shape),
    )


def solution(mesh):
    placed = (P("dp", "space", None, None), P(), P(), P(), P(), P("dp", "space", None, None))
    return jax.shard_map(
        local,
        mesh=mesh,
        in_specs=placed,
        out_specs=(P("dp", "space", None, None), P(), P(), P(), P()),
        check_vma=False,
    )
```

```python
import functools
import math

import jax
import jax.numpy as jnp
from jax import lax
from jax.experimental import pallas as pl
from jax.experimental.pallas import tpu as pltpu
from jax.sharding import PartitionSpec as P


F32 = jnp.float32
BF16 = jnp.bfloat16
LANES = 128
MIB = 1024 * 1024


def _params(mib):
    return pltpu.CompilerParams(vmem_limit_bytes=mib * MIB)


def _cost(flops, moved):
    return pl.CostEstimate(flops=int(flops), bytes_accessed=int(moved), transcendentals=0)


def _dot(a, b):
    return lax.dot_general(a, b, (((1,), (0,)), ((), ())), preferred_element_type=F32)


def _sigmoid(v):
    return 1.0 / (1.0 + jnp.exp(-v))


def _zero_edges(buf, rows):
    tiles = buf.shape[0]
    buf[:, 0:8, :] = jnp.zeros((tiles, 8, LANES), F32)
    buf[:, 8 + rows : 16 + rows, :] = jnp.zeros((tiles, 8, LANES), F32)


def _spread(load, tiles, rows, shift, buf, out):
    lane = lax.broadcasted_iota(jnp.int32, (rows, LANES), 1)
    before = jnp.zeros((rows, LANES), F32)
    for t in range(tiles + 1):
        now = pltpu.roll(load(t).astype(F32), shift, 1) if t < tiles else jnp.zeros((rows, LANES), F32)
        tile = jnp.where(lane < shift, before, now)
        buf[t, 8 : 8 + rows, :] = tile
        out[1, t] = tile.astype(BF16)
        before = now
    for t in range(tiles + 1):
        out[0, t] = buf[t, 7 : 7 + rows, :].astype(BF16)
        out[2, t] = buf[t, 9 : 9 + rows, :].astype(BF16)


def _cols(ref, first, groups):
    rows = ref.shape[1]
    a = ref[pl.ds(first, groups)].reshape(groups * rows, LANES)
    b = ref[pl.ds(first + 1, groups)].reshape(groups * rows, LANES)
    return jnp.concatenate([a, b], axis=1)


def _back_bands(w_ref, kk, out, size, first):
    chan_in, chan_out = w_ref.shape[1] // 3, w_ref.shape[2]
    flip = w_ref[kk].astype(F32).T.astype(BF16)
    for i in range(size // chan_out):
        start = chan_in * (i - first)
        low, high = max(start, 0), min(start + 3 * chan_in, 256)
        if low < high:
            r = size * (kk % 3) + chan_out * i
            out[r : r + chan_out, low:high] = flip[:, low - start : high - start]


def _prep_kernel(w_ref, band_two, back_two):
    band_two[...] = jnp.zeros(band_two.shape, BF16)
    back_two[...] = jnp.zeros(back_two.shape, BF16)
    for kk in range(9):
        for j in range(2):
            r = 256 * kk + 64 * j
            band_two[r : r + 192, LANES * j : LANES * (j + 1)] = w_ref[kk]
        _back_bands(w_ref, kk, back_two.at[kk // 3], 768, 2)


def _first_kernel(x0_ref, x1_ref, w_ref, pre_ref, xs_ref, band_ref, buf):
    rows, groups = x0_ref.shape[0], pre_ref.shape[1]
    band_ref[...] = jnp.zeros(band_ref.shape, BF16)
    for kk in range(9):
        for j in range(4):
            r = 256 * kk + 32 * j
            band_ref[r : r + 96, 64 * j : 64 * j + 64] = w_ref[kk]
    _zero_edges(buf, rows)
    for p, ref in enumerate((x0_ref, x1_ref)):
        _spread(lambda t, ref=ref: ref[:, LANES * t : LANES * (t + 1)], groups, rows, 32, buf, xs_ref.at[p])
    step = 8

    def chunk(c, carry):
        g = c * step
        sides = [[_cols(xs_ref.at[p, kh], g, step) for kh in range(3)] for p in range(2)]
        lhs = jnp.concatenate(sides[0] + sides[1], axis=1)
        pre_ref[0, pl.ds(g, step)] = _dot(lhs, band_ref[768:2304, :]).reshape(step, rows, 256)
        pre_ref[1, pl.ds(g, step)] = _dot(lhs, band_ref[0:1536, :]).reshape(step, rows, 256)
        return carry

    lax.fori_loop(0, groups // step, chunk, 0)


def _second_kernel(left_ref, right_ref, pre_ref, band_ref, bias_ref, slope_ref, pool_ref, xs_ref, buf, low, high):
    rows, groups = left_ref.shape[0], pre_ref.shape[1]
    half = rows // 2
    bias = jnp.concatenate([bias_ref[...]] * 4, axis=1)
    _zero_edges(buf, rows)
    for s, ref in enumerate((left_ref, right_ref)):
        _spread(lambda t, ref=ref: ref[:, LANES * t : LANES * (t + 1)], groups, rows, 32, buf, xs_ref.at[s])
    step = 4
    lane = lax.broadcasted_iota(jnp.int32, (step * half, LANES), 1)

    def chunk(c, carry):
        g = c * step
        total = None
        for p in range(2):
            lhs = jnp.concatenate([_cols(xs_ref.at[p, kh], g, step) for kh in range(3)], axis=1)
            more = _dot(lhs, band_ref[1536 * p : 1536 * p + 768, :])
            pre = pre_ref[p, pl.ds(g, step)].reshape(step * rows, 256) + more + bias
            sig = _sigmoid(pre)
            slope_ref[p, pl.ds(g, step)] = (sig * (1.0 + pre * (1.0 - sig))).reshape(step, rows, 256)
            act = pre * sig
            total = act if total is None else total + act
        for part, lanes in ((low, 0), (high, LANES)):
            v = total[:, lanes : lanes + LANES]
            part[...] = v + pltpu.roll(v, 64, 1)
        a = low[pl.ds(0, step * half, stride=2), :] + low[pl.ds(1, step * half, stride=2), :]
        b = high[pl.ds(0, step * half, stride=2), :] + high[pl.ds(1, step * half, stride=2), :]
        mean = jnp.where(lane < 64, a, b) * 0.125
        pool_ref[pl.ds(g, step)] = mean.astype(BF16).reshape(step, half, LANES)
        return carry

    lax.fori_loop(0, groups // step, chunk, 0)


def _mid_kernel(own_ref, band_ref, bias_ref, ps_ref, pre_ref, buf):
    groups, rows = own_ref.shape[0], own_ref.shape[1]
    _zero_edges(buf, rows)
    _spread(lambda t: own_ref[t], groups, rows, 64, buf, ps_ref)
    lhs = jnp.concatenate([_cols(ps_ref.at[kh], 0, groups) for kh in range(3)], axis=1)
    bias = jnp.concatenate([bias_ref[...]] * 2, axis=1)
    pre_ref[...] = _dot(lhs, band_ref[768:1536, :]) + bias


def _third_kernel(
    left_ref, right_ref, pre_ref, band_ref, back_ref, cot_ref, delta_ref, ps_ref, ds_ref, gl_ref, gr_ref, buf
):
    groups, rows = left_ref.shape[0], left_ref.shape[1]
    _zero_edges(buf, rows)
    for s, ref in enumerate((left_ref, right_ref)):
        _spread(lambda t, ref=ref: ref[t], groups, rows, 64, buf, ps_ref.at[s])
    near = jnp.concatenate([_cols(ps_ref.at[0, kh], 0, groups) for kh in range(3)], axis=1)
    far = jnp.concatenate([_cols(ps_ref.at[1, kh], 0, groups) for kh in range(3)], axis=1)
    pre = pre_ref[...] + _dot(near, band_ref[0:768, :]) + _dot(far, band_ref[1536:2304, :])
    sig = _sigmoid(pre)
    cot = jnp.concatenate([cot_ref[:, 256 * g : 256 * (g + 1)] for g in range(groups)], axis=0)
    delta = (cot.astype(F32) * (sig * (1.0 + pre * (1.0 - sig)))).astype(BF16)
    delta_ref[...] = delta
    again = delta.astype(F32)
    cells = 2 * groups
    zero = jnp.zeros((rows, LANES), BF16)
    for kh in range(3):
        ds_ref[kh, 0] = zero
        ds_ref[kh, cells + 1] = zero
    for t in range(cells):
        g, j = t // 2, t % 2
        tile = again[g * rows : (g + 1) * rows, LANES * j : LANES * (j + 1)]
        spot = buf.at[t % buf.shape[0]]
        spot[8 : 8 + rows, :] = tile
        ds_ref[0, t + 1] = spot[9 : 9 + rows, :].astype(BF16)
        ds_ref[1, t + 1] = tile.astype(BF16)
        ds_ref[2, t + 1] = spot[7 : 7 + rows, :].astype(BF16)
    wide = cells // 4
    lhs = _window(ds_ref, 0, wide)
    for kd, ref in ((0, gl_ref), (2, gr_ref)):
        _put_cells(ref, _dot(lhs, back_ref[kd]), wide, rows)


def _put_cells(ref, out, wide, rows):
    for g in range(wide):
        for j in range(2):
            ref[2 * g + j] = out[g * rows : (g + 1) * rows, LANES * j : LANES * (j + 1)].astype(ref.dtype)


def _own_two_kernel(delta_ref, own_ref, halo_ref, ds_ref, back_ref, gm_ref, out_ref):
    groups, rows = own_ref.shape[1] - 1, own_ref.shape[2]
    out_ref[1728:, :] = jnp.zeros((out_ref.shape[0] - 1728, LANES), BF16)
    _put_cells(gm_ref, _dot(_window(ds_ref, 0, groups // 2), back_ref[1]), groups // 2, rows)
    delta = delta_ref[...]
    flip = delta.astype(F32).T.astype(BF16)
    planes = (halo_ref.at[0], own_ref, halo_ref.at[1])
    for kk in range(9):
        full = _dot(flip, _cols(planes[kk // 3].at[kk % 3], 0, groups))
        band = full[0:LANES, :] + pltpu.roll(full[LANES:256, :], 192, 1)
        out_ref[192 * kk : 192 * (kk + 1), :] = band.T[0:192, :].astype(BF16)
    total = jnp.sum(delta.astype(F32), axis=0, keepdims=True)
    line = total[:, 0:LANES] + total[:, LANES:256]
    out_ref[1728:1744, :] = jnp.broadcast_to(line, (16, LANES)).astype(BF16)


def _grad_one_kernel(
    gm_ref, fl_ref, fr_ref, slope_ref, own_ref, halo_ref, two_ref, delta_ref, out_ref, sums, up0, up1, flip, one
):
    groups, rows = slope_ref.shape[1], slope_ref.shape[2]
    half = rows // 2
    lane = lax.broadcasted_iota(jnp.int32, (half, LANES), 1)
    sums[...] = jnp.zeros(sums.shape, F32)
    for g in range(groups):
        v = (gm_ref[g] + fl_ref[g].astype(F32) + fr_ref[g].astype(F32)) * 0.125
        turned = pltpu.roll(v, 64, 1)
        a = jnp.where(lane < 64, v, turned)
        b = jnp.where(lane < 64, turned, v)
        for j, (ref, val) in enumerate(((up0, a), (up1, b))):
            spot = ref.at[g % 2]
            spot[pl.ds(0, half, stride=2), :] = val
            spot[pl.ds(1, half, stride=2), :] = val
            lanes = slice(LANES * j, LANES * (j + 1))
            both = []
            for p in range(2):
                low = (spot[...] * slope_ref[p, g, :, lanes]).astype(BF16)
                delta_ref[p, g, :, lanes] = low
                both.append(low.astype(F32))
            sums[:, lanes] += jnp.sum(both[0].reshape(rows // 8, 8, LANES) + both[1].reshape(rows // 8, 8, LANES), axis=0)
            turn = jnp.concatenate(both, axis=0).T.astype(BF16)
            flip[lanes, 2 * rows * g : 2 * rows * (g + 1)] = turn
    one[...] = jnp.zeros(one.shape, BF16)
    planes = (halo_ref.at[0], own_ref.at[0], own_ref.at[1], halo_ref.at[1])
    for kd in range(3):
        for kh in range(3):
            kk = 3 * kd + kh
            a = planes[kd].at[kh]
            b = planes[kd + 1].at[kh]
            left = jnp.concatenate([r[g] for g in range(groups) for r in (a, b)], axis=0)
            right = jnp.concatenate([r[g + 1] for g in range(groups) for r in (a, b)], axis=0)
            full = _dot(flip[...], jnp.concatenate([left, right], axis=1))
            band = full[0:64, 0:LANES]
            for j in range(1, 4):
                band = band + pltpu.roll(full[64 * j : 64 * j + 64, :], 256 - 32 * j, 1)[:, 0:LANES]
            tall = band.T[0:96, :].astype(BF16)
            for r in range(0, 96, 48):
                at = 96 * kk + r
                side = at // 432
                one[at - 432 * side : at - 432 * side + 48, 64 * side : 64 * side + 64] = tall[r : r + 48, :]
    total = jnp.sum(sums[...], axis=0, keepdims=True)
    line = total[:, 0:LANES] + total[:, LANES:256]
    line = line + pltpu.roll(line, 64, 1)
    one[432:448, :] = jnp.broadcast_to(line, (16, LANES)).astype(BF16)
    count = out_ref.shape[0]
    rows_two, rows_one = two_ref.shape[0] // count, one.shape[0] // count
    for i in range(count):
        out_ref[i, 0:rows_two, :] = two_ref[i * rows_two : (i + 1) * rows_two, :]
        out_ref[i, rows_two:, :] = one[i * rows_one : (i + 1) * rows_one, :]


def _input_kernel(delta_ref, w_ref, gl_ref, own_ref, gr_ref, ds, back, buf):
    groups, rows = delta_ref.shape[1], delta_ref.shape[2]
    cells = 2 * groups
    back[...] = jnp.zeros(back.shape, BF16)
    for kk in range(9):
        _back_bands(w_ref, kk, back.at[kk // 3], 768, 3)
    _zero_edges(buf, rows)
    zero = jnp.zeros((rows, LANES), BF16)
    for p in range(2):
        for kh in range(3):
            ds[p, kh, 0] = zero
            ds[p, kh, cells + 1] = zero

    def group(g, carry):
        for p in range(2):
            for j in range(2):
                low = delta_ref[p, g, :, LANES * j : LANES * (j + 1)]
                spot = buf.at[2 * p + j]
                spot[8 : 8 + rows, :] = low.astype(F32)
                t = 2 * g + j + 1
                ds[p, 0, t] = spot[9 : 9 + rows, :].astype(BF16)
                ds[p, 1, t] = low
                ds[p, 2, t] = spot[7 : 7 + rows, :].astype(BF16)
        return carry

    lax.fori_loop(0, groups, group, 0)
    step = 4

    def chunk(c, carry):
        g = c * step
        spot = pl.ds(g, step)
        near = _window(ds.at[0], g, step)
        far = _window(ds.at[1], g, step)
        gl_ref[spot] = _dot(near, back[0]).astype(BF16).reshape(step, rows, 256)
        gr_ref[spot] = _dot(far, back[2]).astype(BF16).reshape(step, rows, 256)
        for p in range(2):
            own = _dot(near, back[1 + p]) + _dot(far, back[p])
            own_ref[p, spot] = own.astype(BF16).reshape(step, rows, 256)
        return carry

    lax.fori_loop(0, groups // 2 // step, chunk, 0)


def _window(ref, first, count):
    parts = []
    for kh in range(3):
        for i in range(6):
            parts.append(jnp.concatenate([ref[kh, 4 * (first + g) + i] for g in range(count)], axis=0))
    return jnp.concatenate(parts, axis=1)


def _edges_kernel(own_ref, fl_ref, fr_ref, out_ref):
    for g in range(fl_ref.shape[0]):
        for p, ref in ((0, fl_ref), (1, fr_ref)):
            whole = own_ref[p, g].astype(F32) + ref[g].astype(F32)
            out_ref[p, :, 256 * g : 256 * (g + 1)] = whole.astype(BF16)


def _split_kernel(scale_two, scale_one, rows_two, in_ref, out_ref):
    whole = jnp.sum(in_ref[...].astype(F32), axis=0)
    a = (whole[0:rows_two] * scale_two).astype(BF16)
    b = (whole[rows_two:] * scale_one).astype(BF16)
    for i in range(out_ref.shape[0]):
        out_ref[i, 0:rows_two, :] = a
        out_ref[i, rows_two:, :] = b


def _join_kernel(in_ref, out_ref):
    whole = jnp.sum(in_ref[...].astype(F32), axis=0).astype(BF16)
    for i in range(out_ref.shape[0]):
        out_ref[i] = whole


def _unpack_kernel(rows_two, rows_one, in_ref, w_two_ref, b_two_ref, w_one_ref, b_one_ref):
    two, one = w_two_ref.shape[0], w_one_ref.shape[0] // 2
    for i in range(in_ref.shape[0]):
        at = i * rows_two
        take = min(rows_two, max(two - at, 0))
        if take:
            w_two_ref[at : at + take, :] = in_ref[i, 0:take, :].astype(F32)
        if at <= two < at + rows_two:
            b_two_ref[...] = in_ref[i, two - at : two - at + 8, :].astype(F32)[0:1]
        at = i * rows_one
        take = min(rows_one, max(one - at, 0))
        if take:
            block = in_ref[i, rows_two : rows_two + take, :].astype(F32)
            w_one_ref[at : at + take, :] = block[:, 0:64]
            w_one_ref[one + at : one + at + take, :] = block[:, 64:128]
        if at <= one < at + rows_one:
            spot = rows_two + one - at
            b_one_ref[...] = in_ref[i, spot : spot + 8, :].astype(F32)[0:1, 0:64]


def _shape(shape, dtype):
    return jax.ShapeDtypeStruct(shape, dtype)


def _call(kernel, out, scratch, flops, moved, mib, args):
    return pl.pallas_call(
        kernel, out_shape=out, scratch_shapes=scratch, compiler_params=_params(mib), cost_estimate=_cost(flops, moved)
    )(*args)


def _round_up(value, unit):
    return -(-value // unit) * unit


def local(act_in, weight_one, bias_one, weight_two, bias_two, cotangent):
    _, slab, side, merged = act_in.shape
    half = side // 2
    c0, c1 = weight_one.shape[3:]
    c2 = weight_two.shape[4]
    dp, space = lax.axis_size("dp"), lax.axis_size("space")
    depth_all = slab * space
    scale_one = 16.0 / math.sqrt(dp * depth_all * side * side)
    scale_two = 1.0 / math.sqrt(dp * (depth_all // 2) * half * half)
    up = [(i, i + 1) for i in range(space - 1)]
    down = [(i + 1, i) for i in range(space - 1)]

    x = act_in.reshape(slab, side, merged)
    x0, x1 = x[0], x[slab - 1]
    from_left = lax.ppermute(x1, "space", up)
    from_right = lax.ppermute(x0, "space", down)
    w_one = weight_one.reshape(9, 3 * c0, c1)
    w_two = weight_two.reshape(9, 3 * c1, c2)
    groups = merged // LANES
    xs_shape = (2, 3, groups + 1, side, LANES)
    work = 2 * side * groups * 256
    rows_mid = groups * half
    work_two = rows_mid * 256 * 768
    tile = _shape((groups, half, LANES), BF16)
    tall = pltpu.VMEM((groups + 1, side + 16, LANES), F32)
    short = pltpu.VMEM((groups + 1, half + 16, LANES), F32)
    pre, xs_own, band_one = _call(
        _first_kernel,
        (_shape((2, groups, side, 256), F32), _shape(xs_shape, BF16), _shape((2304, 256), BF16)),
        [tall],
        2 * work * 1536,
        8 * MIB,
        16,
        (x0, x1, w_one),
    )
    band_two, back_two = _call(
        _prep_kernel, (_shape((2304, 256), BF16), _shape((3, 2304, 256), BF16)), [], work * 768, 8 * MIB, 12, (w_two,)
    )
    slope, pooled, xs_halo = _call(
        _second_kernel,
        (_shape((2, groups, side, 256), F32), tile, _shape(xs_shape, BF16)),
        [tall] + [pltpu.VMEM((4 * side, LANES), F32)] * 2,
        2 * work * 768,
        8 * MIB,
        16,
        (from_left, from_right, pre, band_one, bias_one.reshape(1, c1)),
    )
    pool_left = lax.ppermute(pooled, "space", up)
    pool_right = lax.ppermute(pooled, "space", down)
    ps_own, pre_two = _call(
        _mid_kernel,
        (_shape((3, groups + 1, half, LANES), BF16), _shape((rows_mid, 256), F32)),
        [short],
        2 * work_two,
        2 * MIB,
        12,
        (pooled, band_two, bias_two.reshape(1, c2)),
    )
    delta_two, ps_halo, ds_two, gp_left, gp_right = _call(
        _third_kernel,
        (
            _shape((rows_mid, 256), BF16),
            _shape((2, 3, groups + 1, half, LANES), BF16),
            _shape((3, 2 * groups + 2, half, LANES), BF16),
            tile,
            tile,
        ),
        [short],
        8 * work_two,
        4 * MIB,
        16,
        (pool_left, pool_right, pre_two, band_two, back_two, cotangent.reshape(half, -1)),
    )
    gp_from_right = lax.ppermute(gp_left, "space", down)
    gp_from_left = lax.ppermute(gp_right, "space", up)
    runs = space // 2
    peers = 2 * dp
    planes = [[d * space + r * runs + z for d in range(dp) for r in range(2)] for z in range(runs)]
    lines = [[r * runs + z for z in range(runs)] for r in range(2)]
    rows_two = _round_up(1744, 8 * peers)
    rows_one = _round_up(448, 8 * peers)
    gp_own, part_two = _call(
        _own_two_kernel,
        (_shape((groups, half, LANES), F32), _shape((rows_two, LANES), BF16)),
        [],
        8 * work_two,
        2 * MIB,
        16,
        (delta_two, ps_own, ps_halo, ds_two, back_two),
    )
    rows_all = (rows_two + rows_one) // peers
    delta_one, parts = _call(
        _grad_one_kernel,
        (_shape((2, groups, side, 256), BF16), _shape((peers, rows_all, LANES), BF16)),
        [pltpu.VMEM((8, 256), F32)]
        + [pltpu.VMEM((2, side, LANES), F32)] * 2
        + [pltpu.VMEM((256, 2 * groups * side), BF16), pltpu.VMEM((rows_one, LANES), BF16)],
        2 * work * 2304,
        4 * MIB,
        16,
        (gp_own, gp_from_left, gp_from_right, slope, xs_own, xs_halo, part_two),
    )
    rows_two //= peers
    rows_one //= peers
    met = lax.all_to_all(parts, ("dp", "space"), 0, 0, axis_index_groups=planes)
    block = _shape((groups // 2, side, 256), BF16)
    gx_left, gx_own, gx_right = _call(
        _input_kernel,
        (block, _shape((2, groups // 2, side, 256), BF16), block),
        [
            pltpu.VMEM((2, 3, 2 * groups + 2, side, LANES), BF16),
            pltpu.VMEM((3, 2304, 256), BF16),
            pltpu.VMEM((4, side + 16, LANES), F32),
        ],
        2 * work * 2304 // 2,
        8 * MIB,
        20,
        (delta_one, w_one),
    )
    gx_from_right = lax.ppermute(gx_left, "space", down)
    gx_from_left = lax.ppermute(gx_right, "space", up)
    grad_x = _call(
        _edges_kernel,
        _shape((2, side, merged), BF16),
        [],
        2 * work * 128,
        4 * MIB,
        12,
        (gx_own, gx_from_left, gx_from_right),
    )
    mine = _call(
        functools.partial(_split_kernel, scale_two, scale_one, rows_two),
        _shape((runs, rows_all, LANES), BF16),
        [],
        0,
        MIB,
        8,
        (met,),
    )
    met = lax.all_to_all(mine, "space", 0, 0, axis_index_groups=lines)
    joined = _call(_join_kernel, _shape((peers, rows_all, LANES), BF16), [], 0, MIB, 8, (met,))
    done = lax.all_to_all(joined, ("dp", "space"), 0, 0, axis_index_groups=planes)
    gw_two, gb_two, gw_one, gb_one = _call(
        functools.partial(_unpack_kernel, rows_two, rows_one),
        (
            _shape((27 * c1, c2), F32),
            _shape((1, c2), F32),
            _shape((27 * c0, c1), F32),
            _shape((1, c1), F32),
        ),
        [],
        0,
        MIB,
        8,
        (done,),
    )
    return (
        grad_x.reshape(act_in.shape),
        gw_one.reshape(weight_one.shape),
        gb_one.reshape(bias_one.shape),
        gw_two.reshape(weight_two.shape),
        gb_two.reshape(bias_two.shape),
    )


def solution(mesh):
    placed = (P("dp", "space", None, None), P(), P(), P(), P(), P("dp", "space", None, None))
    return jax.shard_map(
        local,
        mesh=mesh,
        in_specs=placed,
        out_specs=(P("dp", "space", None, None), P(), P(), P(), P()),
        check_vma=False,
    )
```

```python
import functools
import math

import jax
import jax.numpy as jnp
from jax import lax
from jax.experimental import pallas as pl
from jax.experimental.pallas import tpu as pltpu
from jax.sharding import PartitionSpec as P


F32 = jnp.float32
BF16 = jnp.bfloat16
LANES = 128
MIB = 1024 * 1024


def _params(mib):
    return pltpu.CompilerParams(vmem_limit_bytes=mib * MIB)


def _cost(flops, moved):
    return pl.CostEstimate(flops=int(flops), bytes_accessed=int(moved), transcendentals=0)


def _dot(a, b):
    return lax.dot_general(a, b, (((1,), (0,)), ((), ())), preferred_element_type=F32)


def _sigmoid(v):
    return 0.5 * jnp.tanh(0.5 * v) + 0.5


def _zero_edges(buf, rows):
    tiles = buf.shape[0]
    buf[:, 0:8, :] = jnp.zeros((tiles, 8, LANES), F32)
    buf[:, 8 + rows : 16 + rows, :] = jnp.zeros((tiles, 8, LANES), F32)


def _spread(load, tiles, rows, shift, buf, out):
    lane = lax.broadcasted_iota(jnp.int32, (rows, LANES), 1)
    before = jnp.zeros((rows, LANES), F32)
    for t in range(tiles + 1):
        now = pltpu.roll(load(t).astype(F32), shift, 1) if t < tiles else jnp.zeros((rows, LANES), F32)
        tile = jnp.where(lane < shift, before, now)
        buf[t, 8 : 8 + rows, :] = tile
        out[1, t] = tile.astype(BF16)
        before = now
    for t in range(tiles + 1):
        out[0, t] = buf[t, 7 : 7 + rows, :].astype(BF16)
        out[2, t] = buf[t, 9 : 9 + rows, :].astype(BF16)


def _cols(ref, first, groups):
    rows = ref.shape[1]
    a = ref[pl.ds(first, groups)].reshape(groups * rows, LANES)
    b = ref[pl.ds(first + 1, groups)].reshape(groups * rows, LANES)
    return jnp.concatenate([a, b], axis=1)


def _back_bands(w_ref, kk, out, size, first):
    chan_in, chan_out = w_ref.shape[1] // 3, w_ref.shape[2]
    flip = w_ref[kk].astype(F32).T.astype(BF16)
    for i in range(size // chan_out):
        start = chan_in * (i - first)
        low, high = max(start, 0), min(start + 3 * chan_in, 256)
        if low < high:
            r = size * (kk % 3) + chan_out * i
            out[r : r + chan_out, low:high] = flip[:, low - start : high - start]


def _prep_kernel(w_ref, band_two, back_two):
    band_two[...] = jnp.zeros(band_two.shape, BF16)
    back_two[...] = jnp.zeros(back_two.shape, BF16)
    for kk in range(9):
        for j in range(2):
            r = 256 * kk + 64 * j
            band_two[r : r + 192, LANES * j : LANES * (j + 1)] = w_ref[kk]
        _back_bands(w_ref, kk, back_two.at[kk // 3], 768, 2)


def _first_kernel(x0_ref, x1_ref, w_ref, pre_ref, xs_ref, band_ref, buf):
    rows, groups = x0_ref.shape[0], pre_ref.shape[1]
    band_ref[...] = jnp.zeros(band_ref.shape, BF16)
    for kk in range(9):
        for j in range(4):
            r = 256 * kk + 32 * j
            band_ref[r : r + 96, 64 * j : 64 * j + 64] = w_ref[kk]
    _zero_edges(buf, rows)
    for p, ref in enumerate((x0_ref, x1_ref)):
        _spread(lambda t, ref=ref: ref[:, LANES * t : LANES * (t + 1)], groups, rows, 32, buf, xs_ref.at[p])
    step = 8

    def chunk(c, carry):
        g = c * step
        sides = [[_cols(xs_ref.at[p, kh], g, step) for kh in range(3)] for p in range(2)]
        lhs = jnp.concatenate(sides[0] + sides[1], axis=1)
        pre_ref[0, pl.ds(g, step)] = _dot(lhs, band_ref[768:2304, :]).reshape(step, rows, 256)
        pre_ref[1, pl.ds(g, step)] = _dot(lhs, band_ref[0:1536, :]).reshape(step, rows, 256)
        return carry

    lax.fori_loop(0, groups // step, chunk, 0)


def _second_kernel(keep_ref, left_ref, right_ref, pre_ref, band_ref, bias_ref, slope_ref, pool_ref, xs_ref, buf, low, high):
    rows, groups = left_ref.shape[0], pre_ref.shape[1]
    half = rows // 2
    bias = jnp.concatenate([bias_ref[...]] * 4, axis=1)
    _zero_edges(buf, rows)
    for s, ref in enumerate((left_ref, right_ref)):
        keep = keep_ref[0, s]
        _spread(
            lambda t, ref=ref, keep=keep: ref[:, LANES * t : LANES * (t + 1)].astype(F32) * keep,
            groups,
            rows,
            32,
            buf,
            xs_ref.at[s],
        )
    step = 4
    lane = lax.broadcasted_iota(jnp.int32, (step * half, LANES), 1)

    def chunk(c, carry):
        g = c * step
        total = None
        for p in range(2):
            lhs = jnp.concatenate([_cols(xs_ref.at[p, kh], g, step) for kh in range(3)], axis=1)
            more = _dot(lhs, band_ref[1536 * p : 1536 * p + 768, :])
            pre = pre_ref[p, pl.ds(g, step)].reshape(step * rows, 256) + more + bias
            sig = _sigmoid(pre)
            slope_ref[p, pl.ds(g, step)] = (sig * (1.0 + pre * (1.0 - sig))).reshape(step, rows, 256)
            act = pre * sig
            total = act if total is None else total + act
        for part, lanes in ((low, 0), (high, LANES)):
            v = total[:, lanes : lanes + LANES]
            part[...] = v + pltpu.roll(v, 64, 1)
        a = low[pl.ds(0, step * half, stride=2), :] + low[pl.ds(1, step * half, stride=2), :]
        b = high[pl.ds(0, step * half, stride=2), :] + high[pl.ds(1, step * half, stride=2), :]
        mean = jnp.where(lane < 64, a, b) * 0.125
        pool_ref[pl.ds(g, step)] = mean.astype(BF16).reshape(step, half, LANES)
        return carry

    lax.fori_loop(0, groups // step, chunk, 0)


def _mid_kernel(own_ref, band_ref, bias_ref, ps_ref, pre_ref, buf):
    groups, rows = own_ref.shape[0], own_ref.shape[1]
    _zero_edges(buf, rows)
    _spread(lambda t: own_ref[t], groups, rows, 64, buf, ps_ref)
    lhs = jnp.concatenate([_cols(ps_ref.at[kh], 0, groups) for kh in range(3)], axis=1)
    bias = jnp.concatenate([bias_ref[...]] * 2, axis=1)
    pre_ref[...] = _dot(lhs, band_ref[768:1536, :]) + bias


def _third_kernel(
    keep_ref, left_ref, right_ref, pre_ref, band_ref, back_ref, cot_ref, delta_ref, ps_ref, ds_ref, gl_ref, gr_ref, buf
):
    groups, rows = left_ref.shape[0], left_ref.shape[1]
    _zero_edges(buf, rows)
    for s, ref in enumerate((left_ref, right_ref)):
        keep = keep_ref[0, s]
        _spread(lambda t, ref=ref, keep=keep: ref[t].astype(F32) * keep, groups, rows, 64, buf, ps_ref.at[s])
    near = jnp.concatenate([_cols(ps_ref.at[0, kh], 0, groups) for kh in range(3)], axis=1)
    far = jnp.concatenate([_cols(ps_ref.at[1, kh], 0, groups) for kh in range(3)], axis=1)
    pre = pre_ref[...] + _dot(near, band_ref[0:768, :]) + _dot(far, band_ref[1536:2304, :])
    sig = _sigmoid(pre)
    cot = jnp.concatenate([cot_ref[:, 256 * g : 256 * (g + 1)] for g in range(groups)], axis=0)
    delta = (cot.astype(F32) * (sig * (1.0 + pre * (1.0 - sig)))).astype(BF16)
    delta_ref[...] = delta
    again = delta.astype(F32)
    cells = 2 * groups
    zero = jnp.zeros((rows, LANES), BF16)
    for kh in range(3):
        ds_ref[kh, 0] = zero
        ds_ref[kh, cells + 1] = zero
    for t in range(cells):
        g, j = t // 2, t % 2
        tile = again[g * rows : (g + 1) * rows, LANES * j : LANES * (j + 1)]
        spot = buf.at[t % buf.shape[0]]
        spot[8 : 8 + rows, :] = tile
        ds_ref[0, t + 1] = spot[9 : 9 + rows, :].astype(BF16)
        ds_ref[1, t + 1] = tile.astype(BF16)
        ds_ref[2, t + 1] = spot[7 : 7 + rows, :].astype(BF16)
    wide = cells // 4
    lhs = _window(ds_ref, 0, wide)
    for kd, ref in ((0, gl_ref), (2, gr_ref)):
        _put_cells(ref, _dot(lhs, back_ref[kd]), wide, rows)


def _put_cells(ref, out, wide, rows):
    for g in range(wide):
        for j in range(2):
            ref[2 * g + j] = out[g * rows : (g + 1) * rows, LANES * j : LANES * (j + 1)].astype(ref.dtype)


def _own_two_kernel(delta_ref, own_ref, halo_ref, ds_ref, back_ref, gm_ref, out_ref):
    groups, rows = own_ref.shape[1] - 1, own_ref.shape[2]
    out_ref[1728:, :] = jnp.zeros((out_ref.shape[0] - 1728, LANES), BF16)
    _put_cells(gm_ref, _dot(_window(ds_ref, 0, groups // 2), back_ref[1]), groups // 2, rows)
    delta = delta_ref[...]
    flip = delta.astype(F32).T.astype(BF16)
    planes = (halo_ref.at[0], own_ref, halo_ref.at[1])
    for kk in range(9):
        full = _dot(flip, _cols(planes[kk // 3].at[kk % 3], 0, groups))
        band = full[0:LANES, :] + pltpu.roll(full[LANES:256, :], 192, 1)
        out_ref[192 * kk : 192 * (kk + 1), :] = band.T[0:192, :].astype(BF16)
    total = jnp.sum(delta.astype(F32), axis=0, keepdims=True)
    line = total[:, 0:LANES] + total[:, LANES:256]
    out_ref[1728:1744, :] = jnp.broadcast_to(line, (16, LANES)).astype(BF16)


def _grad_one_kernel(
    keep_ref, gm_ref, fl_ref, fr_ref, slope_ref, own_ref, halo_ref, two_ref, delta_ref, out_ref, sums, up0, up1, flip, one
):
    groups, rows = slope_ref.shape[1], slope_ref.shape[2]
    half = rows // 2
    lane = lax.broadcasted_iota(jnp.int32, (half, LANES), 1)
    sums[...] = jnp.zeros(sums.shape, F32)
    keep_left, keep_right = keep_ref[0, 0], keep_ref[0, 1]
    for g in range(groups):
        v = (gm_ref[g] + fl_ref[g].astype(F32) * keep_left + fr_ref[g].astype(F32) * keep_right) * 0.125
        turned = pltpu.roll(v, 64, 1)
        a = jnp.where(lane < 64, v, turned)
        b = jnp.where(lane < 64, turned, v)
        for j, (ref, val) in enumerate(((up0, a), (up1, b))):
            spot = ref.at[g % 2]
            spot[pl.ds(0, half, stride=2), :] = val
            spot[pl.ds(1, half, stride=2), :] = val
            lanes = slice(LANES * j, LANES * (j + 1))
            both = []
            for p in range(2):
                low = (spot[...] * slope_ref[p, g, :, lanes]).astype(BF16)
                delta_ref[p, g, :, lanes] = low
                both.append(low.astype(F32))
            sums[:, lanes] += jnp.sum(both[0].reshape(rows // 8, 8, LANES) + both[1].reshape(rows // 8, 8, LANES), axis=0)
            turn = jnp.concatenate(both, axis=0).T.astype(BF16)
            flip[lanes, 2 * rows * g : 2 * rows * (g + 1)] = turn
    one[...] = jnp.zeros(one.shape, BF16)
    planes = (halo_ref.at[0], own_ref.at[0], own_ref.at[1], halo_ref.at[1])
    for kd in range(3):
        for kh in range(3):
            kk = 3 * kd + kh
            a = planes[kd].at[kh]
            b = planes[kd + 1].at[kh]
            left = jnp.concatenate([r[g] for g in range(groups) for r in (a, b)], axis=0)
            right = jnp.concatenate([r[g + 1] for g in range(groups) for r in (a, b)], axis=0)
            full = _dot(flip[...], jnp.concatenate([left, right], axis=1))
            band = full[0:64, 0:LANES]
            for j in range(1, 4):
                band = band + pltpu.roll(full[64 * j : 64 * j + 64, :], 256 - 32 * j, 1)[:, 0:LANES]
            tall = band.T[0:96, :].astype(BF16)
            for r in range(0, 96, 48):
                at = 96 * kk + r
                side = at // 432
                one[at - 432 * side : at - 432 * side + 48, 64 * side : 64 * side + 64] = tall[r : r + 48, :]
    total = jnp.sum(sums[...], axis=0, keepdims=True)
    line = total[:, 0:LANES] + total[:, LANES:256]
    line = line + pltpu.roll(line, 64, 1)
    one[432:448, :] = jnp.broadcast_to(line, (16, LANES)).astype(BF16)
    count = out_ref.shape[0]
    rows_two, rows_one = two_ref.shape[0] // count, one.shape[0] // count
    for i in range(count):
        out_ref[i, 0:rows_two, :] = two_ref[i * rows_two : (i + 1) * rows_two, :]
        out_ref[i, rows_two:, :] = one[i * rows_one : (i + 1) * rows_one, :]


def _input_kernel(delta_ref, w_ref, gl_ref, own_ref, gr_ref, ds, back, buf):
    groups, rows = delta_ref.shape[1], delta_ref.shape[2]
    cells = 2 * groups
    back[...] = jnp.zeros(back.shape, BF16)
    for kk in range(9):
        _back_bands(w_ref, kk, back.at[kk // 3], 768, 3)
    _zero_edges(buf, rows)
    zero = jnp.zeros((rows, LANES), BF16)
    for p in range(2):
        for kh in range(3):
            ds[p, kh, 0] = zero
            ds[p, kh, cells + 1] = zero

    def group(g, carry):
        for p in range(2):
            for j in range(2):
                low = delta_ref[p, g, :, LANES * j : LANES * (j + 1)]
                spot = buf.at[2 * p + j]
                spot[8 : 8 + rows, :] = low.astype(F32)
                t = 2 * g + j + 1
                ds[p, 0, t] = spot[9 : 9 + rows, :].astype(BF16)
                ds[p, 1, t] = low
                ds[p, 2, t] = spot[7 : 7 + rows, :].astype(BF16)
        return carry

    lax.fori_loop(0, groups, group, 0)
    step = 4

    def chunk(c, carry):
        g = c * step
        spot = pl.ds(g, step)
        near = _window(ds.at[0], g, step)
        far = _window(ds.at[1], g, step)
        gl_ref[spot] = _dot(near, back[0]).astype(BF16).reshape(step, rows, 256)
        gr_ref[spot] = _dot(far, back[2]).astype(BF16).reshape(step, rows, 256)
        for p in range(2):
            own = _dot(near, back[1 + p]) + _dot(far, back[p])
            own_ref[p, spot] = own.astype(BF16).reshape(step, rows, 256)
        return carry

    lax.fori_loop(0, groups // 2 // step, chunk, 0)


def _window(ref, first, count):
    parts = []
    for kh in range(3):
        for i in range(6):
            parts.append(jnp.concatenate([ref[kh, 4 * (first + g) + i] for g in range(count)], axis=0))
    return jnp.concatenate(parts, axis=1)


def _edges_kernel(keep_ref, own_ref, fl_ref, fr_ref, out_ref):
    for g in range(fl_ref.shape[0]):
        for p, ref in ((0, fl_ref), (1, fr_ref)):
            whole = own_ref[p, g].astype(F32) + ref[g].astype(F32) * keep_ref[0, p]
            out_ref[p, :, 256 * g : 256 * (g + 1)] = whole.astype(BF16)


def _split_kernel(scale_two, scale_one, rows_two, in_ref, out_ref):
    whole = jnp.sum(in_ref[...].astype(F32), axis=0)
    a = (whole[0:rows_two] * scale_two).astype(BF16)
    b = (whole[rows_two:] * scale_one).astype(BF16)
    for i in range(out_ref.shape[0]):
        out_ref[i, 0:rows_two, :] = a
        out_ref[i, rows_two:, :] = b


def _join_kernel(in_ref, out_ref):
    whole = jnp.sum(in_ref[...].astype(F32), axis=0).astype(BF16)
    for i in range(out_ref.shape[0]):
        out_ref[i] = whole


def _unpack_kernel(rows_two, rows_one, in_ref, w_two_ref, b_two_ref, w_one_ref, b_one_ref):
    two, one = w_two_ref.shape[0], w_one_ref.shape[0] // 2
    for i in range(in_ref.shape[0]):
        at = i * rows_two
        take = min(rows_two, max(two - at, 0))
        if take:
            w_two_ref[at : at + take, :] = in_ref[i, 0:take, :].astype(F32)
        if at <= two < at + rows_two:
            b_two_ref[...] = in_ref[i, two - at : two - at + 8, :].astype(F32)[0:1]
        at = i * rows_one
        take = min(rows_one, max(one - at, 0))
        if take:
            block = in_ref[i, rows_two : rows_two + take, :].astype(F32)
            w_one_ref[at : at + take, :] = block[:, 0:64]
            w_one_ref[one + at : one + at + take, :] = block[:, 64:128]
        if at <= one < at + rows_one:
            spot = rows_two + one - at
            b_one_ref[...] = in_ref[i, spot : spot + 8, :].astype(F32)[0:1, 0:64]


def _shape(shape, dtype):
    return jax.ShapeDtypeStruct(shape, dtype)


def _call(kernel, out, scratch, flops, moved, mib, args, masks=0):
    return pl.pallas_call(
        kernel,
        out_shape=out,
        in_specs=[pl.BlockSpec(memory_space=pltpu.SMEM)] * masks + [pl.BlockSpec()] * (len(args) - masks),
        scratch_shapes=scratch,
        compiler_params=_params(mib),
        cost_estimate=_cost(flops, moved),
    )(*args)


def _round_up(value, unit):
    return -(-value // unit) * unit


def local(act_in, weight_one, bias_one, weight_two, bias_two, cotangent):
    _, slab, side, merged = act_in.shape
    half = side // 2
    c0, c1 = weight_one.shape[3:]
    c2 = weight_two.shape[4]
    dp, space = lax.axis_size("dp"), lax.axis_size("space")
    depth_all = slab * space
    scale_one = 16.0 / math.sqrt(dp * depth_all * side * side)
    scale_two = 1.0 / math.sqrt(dp * (depth_all // 2) * half * half)
    up = [(i, (i + 1) % space) for i in range(space)]
    down = [((i + 1) % space, i) for i in range(space)]
    place = lax.axis_index("space")
    keep = jnp.stack([place > 0, place < space - 1]).astype(F32).reshape(1, 2)

    x = act_in.reshape(slab, side, merged)
    x0, x1 = x[0], x[slab - 1]
    from_left = lax.ppermute(x1, "space", up)
    from_right = lax.ppermute(x0, "space", down)
    w_one = weight_one.reshape(9, 3 * c0, c1)
    w_two = weight_two.reshape(9, 3 * c1, c2)
    groups = merged // LANES
    xs_shape = (2, 3, groups + 1, side, LANES)
    work = 2 * side * groups * 256
    rows_mid = groups * half
    work_two = rows_mid * 256 * 768
    tile = _shape((groups, half, LANES), BF16)
    tall = pltpu.VMEM((groups + 1, side + 16, LANES), F32)
    short = pltpu.VMEM((groups + 1, half + 16, LANES), F32)
    pre, xs_own, band_one = _call(
        _first_kernel,
        (_shape((2, groups, side, 256), F32), _shape(xs_shape, BF16), _shape((2304, 256), BF16)),
        [tall],
        2 * work * 1536,
        8 * MIB,
        16,
        (x0, x1, w_one),
    )
    band_two, back_two = _call(
        _prep_kernel, (_shape((2304, 256), BF16), _shape((3, 2304, 256), BF16)), [], work * 768, 8 * MIB, 12, (w_two,)
    )
    slope, pooled, xs_halo = _call(
        _second_kernel,
        (_shape((2, groups, side, 256), F32), tile, _shape(xs_shape, BF16)),
        [tall] + [pltpu.VMEM((4 * side, LANES), F32)] * 2,
        2 * work * 768,
        8 * MIB,
        16,
        (keep, from_left, from_right, pre, band_one, bias_one.reshape(1, c1)),
        1,
    )
    pool_left = lax.ppermute(pooled, "space", up)
    pool_right = lax.ppermute(pooled, "space", down)
    ps_own, pre_two = _call(
        _mid_kernel,
        (_shape((3, groups + 1, half, LANES), BF16), _shape((rows_mid, 256), F32)),
        [short],
        2 * work_two,
        2 * MIB,
        12,
        (pooled, band_two, bias_two.reshape(1, c2)),
    )
    delta_two, ps_halo, ds_two, gp_left, gp_right = _call(
        _third_kernel,
        (
            _shape((rows_mid, 256), BF16),
            _shape((2, 3, groups + 1, half, LANES), BF16),
            _shape((3, 2 * groups + 2, half, LANES), BF16),
            tile,
            tile,
        ),
        [short],
        8 * work_two,
        4 * MIB,
        16,
        (keep, pool_left, pool_right, pre_two, band_two, back_two, cotangent.reshape(half, -1)),
        1,
    )
    gp_from_right = lax.ppermute(gp_left, "space", down)
    gp_from_left = lax.ppermute(gp_right, "space", up)
    runs = space // 2
    peers = 2 * dp
    planes = [[d * space + r * runs + z for d in range(dp) for r in range(2)] for z in range(runs)]
    lines = [[r * runs + z for z in range(runs)] for r in range(2)]
    rows_two = _round_up(1744, 8 * peers)
    rows_one = _round_up(448, 8 * peers)
    gp_own, part_two = _call(
        _own_two_kernel,
        (_shape((groups, half, LANES), F32), _shape((rows_two, LANES), BF16)),
        [],
        8 * work_two,
        2 * MIB,
        16,
        (delta_two, ps_own, ps_halo, ds_two, back_two),
    )
    rows_all = (rows_two + rows_one) // peers
    delta_one, parts = _call(
        _grad_one_kernel,
        (_shape((2, groups, side, 256), BF16), _shape((peers, rows_all, LANES), BF16)),
        [pltpu.VMEM((8, 256), F32)]
        + [pltpu.VMEM((2, side, LANES), F32)] * 2
        + [pltpu.VMEM((256, 2 * groups * side), BF16), pltpu.VMEM((rows_one, LANES), BF16)],
        2 * work * 2304,
        4 * MIB,
        16,
        (keep, gp_own, gp_from_left, gp_from_right, slope, xs_own, xs_halo, part_two),
        1,
    )
    rows_two //= peers
    rows_one //= peers
    met = lax.all_to_all(parts, ("dp", "space"), 0, 0, axis_index_groups=planes)
    block = _shape((groups // 2, side, 256), BF16)
    gx_left, gx_own, gx_right = _call(
        _input_kernel,
        (block, _shape((2, groups // 2, side, 256), BF16), block),
        [
            pltpu.VMEM((2, 3, 2 * groups + 2, side, LANES), BF16),
            pltpu.VMEM((3, 2304, 256), BF16),
            pltpu.VMEM((4, side + 16, LANES), F32),
        ],
        2 * work * 2304 // 2,
        8 * MIB,
        20,
        (delta_one, w_one),
    )
    gx_from_right = lax.ppermute(gx_left, "space", down)
    gx_from_left = lax.ppermute(gx_right, "space", up)
    grad_x = _call(
        _edges_kernel,
        _shape((2, side, merged), BF16),
        [],
        2 * work * 128,
        4 * MIB,
        12,
        (keep, gx_own, gx_from_left, gx_from_right),
        1,
    )
    mine = _call(
        functools.partial(_split_kernel, scale_two, scale_one, rows_two),
        _shape((runs, rows_all, LANES), BF16),
        [],
        0,
        MIB,
        8,
        (met,),
    )
    met = lax.all_to_all(mine, "space", 0, 0, axis_index_groups=lines)
    joined = _call(_join_kernel, _shape((peers, rows_all, LANES), BF16), [], 0, MIB, 8, (met,))
    done = lax.all_to_all(joined, ("dp", "space"), 0, 0, axis_index_groups=planes)
    gw_two, gb_two, gw_one, gb_one = _call(
        functools.partial(_unpack_kernel, rows_two, rows_one),
        (
            _shape((27 * c1, c2), F32),
            _shape((1, c2), F32),
            _shape((27 * c0, c1), F32),
            _shape((1, c1), F32),
        ),
        [],
        0,
        MIB,
        8,
        (done,),
    )
    return (
        grad_x.reshape(act_in.shape),
        gw_one.reshape(weight_one.shape),
        gb_one.reshape(bias_one.shape),
        gw_two.reshape(weight_two.shape),
        gb_two.reshape(bias_two.shape),
    )


def solution(mesh):
    placed = (P("dp", "space", None, None), P(), P(), P(), P(), P("dp", "space", None, None))
    return jax.shard_map(
        local,
        mesh=mesh,
        in_specs=placed,
        out_specs=(P("dp", "space", None, None), P(), P(), P(), P()),
        check_vma=False,
    )
```

```python
import functools
import math

import jax
import jax.numpy as jnp
from jax import lax
from jax.experimental import pallas as pl
from jax.experimental.pallas import tpu as pltpu
from jax.sharding import PartitionSpec as P


F32 = jnp.float32
BF16 = jnp.bfloat16
LANES = 128
MIB = 1024 * 1024


def _params(mib):
    return pltpu.CompilerParams(vmem_limit_bytes=mib * MIB)


def _cost(flops, moved):
    return pl.CostEstimate(flops=int(flops), bytes_accessed=int(moved), transcendentals=0)


def _dot(a, b):
    return lax.dot_general(a, b, (((1,), (0,)), ((), ())), preferred_element_type=F32)


def _sigmoid(v):
    return 0.5 * jnp.tanh(0.5 * v) + 0.5


def _mask(keep_ref, side, rows):
    return jnp.concatenate([keep_ref[side]] * (rows // 8), axis=0)


def _zero_edges(buf, rows):
    tiles = buf.shape[0]
    buf[:, 0:8, :] = jnp.zeros((tiles, 8, LANES), F32)
    buf[:, 8 + rows : 16 + rows, :] = jnp.zeros((tiles, 8, LANES), F32)


def _spread(load, tiles, rows, shift, buf, out):
    lane = lax.broadcasted_iota(jnp.int32, (rows, LANES), 1)
    before = jnp.zeros((rows, LANES), F32)
    for t in range(tiles + 1):
        now = pltpu.roll(load(t).astype(F32), shift, 1) if t < tiles else jnp.zeros((rows, LANES), F32)
        tile = jnp.where(lane < shift, before, now)
        buf[t, 8 : 8 + rows, :] = tile
        out[1, t] = tile.astype(BF16)
        before = now
    for t in range(tiles + 1):
        out[0, t] = buf[t, 7 : 7 + rows, :].astype(BF16)
        out[2, t] = buf[t, 9 : 9 + rows, :].astype(BF16)


def _cols(ref, first, groups):
    rows = ref.shape[1]
    a = ref[pl.ds(first, groups)].reshape(groups * rows, LANES)
    b = ref[pl.ds(first + 1, groups)].reshape(groups * rows, LANES)
    return jnp.concatenate([a, b], axis=1)


def _back_bands(w_ref, kk, out, size, first):
    chan_in, chan_out = w_ref.shape[1] // 3, w_ref.shape[2]
    flip = w_ref[kk].astype(F32).T.astype(BF16)
    for i in range(size // chan_out):
        start = chan_in * (i - first)
        low, high = max(start, 0), min(start + 3 * chan_in, 256)
        if low < high:
            r = size * (kk % 3) + chan_out * i
            out[r : r + chan_out, low:high] = flip[:, low - start : high - start]


def _prep_kernel(w_ref, band_two, back_two):
    band_two[...] = jnp.zeros(band_two.shape, BF16)
    back_two[...] = jnp.zeros(back_two.shape, BF16)
    for kk in range(9):
        for j in range(2):
            r = 256 * kk + 64 * j
            band_two[r : r + 192, LANES * j : LANES * (j + 1)] = w_ref[kk]
        _back_bands(w_ref, kk, back_two.at[kk // 3], 768, 2)


def _first_kernel(x0_ref, x1_ref, w_ref, pre_ref, xs_ref, band_ref, buf):
    rows, groups = x0_ref.shape[0], pre_ref.shape[1]
    band_ref[...] = jnp.zeros(band_ref.shape, BF16)
    for kk in range(9):
        for j in range(4):
            r = 256 * kk + 32 * j
            band_ref[r : r + 96, 64 * j : 64 * j + 64] = w_ref[kk]
    _zero_edges(buf, rows)
    for p, ref in enumerate((x0_ref, x1_ref)):
        _spread(lambda t, ref=ref: ref[:, LANES * t : LANES * (t + 1)], groups, rows, 32, buf, xs_ref.at[p])
    step = 8
    for g in range(0, groups, step):
        sides = [[_cols(xs_ref.at[p, kh], g, step) for kh in range(3)] for p in range(2)]
        lhs = jnp.concatenate(sides[0] + sides[1], axis=1)
        pre_ref[0, pl.ds(g, step)] = _dot(lhs, band_ref[768:2304, :]).reshape(step, rows, 256)
        pre_ref[1, pl.ds(g, step)] = _dot(lhs, band_ref[0:1536, :]).reshape(step, rows, 256)


def _second_kernel(keep_ref, left_ref, right_ref, pre_ref, band_ref, bias_ref, slope_ref, pool_ref, xs_ref, buf, low, high):
    rows, groups = left_ref.shape[0], pre_ref.shape[1]
    half = rows // 2
    bias = jnp.concatenate([bias_ref[...]] * 4, axis=1)
    _zero_edges(buf, rows)
    for s, ref in enumerate((left_ref, right_ref)):
        keep = _mask(keep_ref, s, rows)
        _spread(
            lambda t, ref=ref, keep=keep: ref[:, LANES * t : LANES * (t + 1)].astype(F32) * keep,
            groups,
            rows,
            32,
            buf,
            xs_ref.at[s],
        )
    step = 4
    lane = lax.broadcasted_iota(jnp.int32, (step * half, LANES), 1)

    for g in range(0, groups, step):
        total = None
        for p in range(2):
            lhs = jnp.concatenate([_cols(xs_ref.at[p, kh], g, step) for kh in range(3)], axis=1)
            more = _dot(lhs, band_ref[1536 * p : 1536 * p + 768, :])
            pre = pre_ref[p, pl.ds(g, step)].reshape(step * rows, 256) + more + bias
            sig = _sigmoid(pre)
            slope_ref[p, pl.ds(g, step)] = (sig * (1.0 + pre * (1.0 - sig))).reshape(step, rows, 256)
            act = pre * sig
            total = act if total is None else total + act
        sums = []
        for ref, lanes in ((low, 0), (high, LANES)):
            part = ref.at[g // step]
            v = total[:, lanes : lanes + LANES]
            part[...] = v + pltpu.roll(v, 64, 1)
            sums.append(part[pl.ds(0, step * half, stride=2), :] + part[pl.ds(1, step * half, stride=2), :])
        mean = jnp.where(lane < 64, sums[0], sums[1]) * 0.125
        pool_ref[pl.ds(g, step)] = mean.astype(BF16).reshape(step, half, LANES)


def _mid_kernel(own_ref, band_ref, bias_ref, ps_ref, pre_ref, buf):
    groups, rows = own_ref.shape[0], own_ref.shape[1]
    _zero_edges(buf, rows)
    _spread(lambda t: own_ref[t], groups, rows, 64, buf, ps_ref)
    lhs = jnp.concatenate([_cols(ps_ref.at[kh], 0, groups) for kh in range(3)], axis=1)
    bias = jnp.concatenate([bias_ref[...]] * 2, axis=1)
    pre_ref[...] = _dot(lhs, band_ref[768:1536, :]) + bias


def _third_kernel(
    keep_ref, left_ref, right_ref, pre_ref, band_ref, back_ref, cot_ref, delta_ref, ps_ref, ds_ref, gl_ref, gr_ref, buf
):
    groups, rows = left_ref.shape[0], left_ref.shape[1]
    _zero_edges(buf, rows)
    for s, ref in enumerate((left_ref, right_ref)):
        keep = _mask(keep_ref, s, rows)
        _spread(lambda t, ref=ref, keep=keep: ref[t].astype(F32) * keep, groups, rows, 64, buf, ps_ref.at[s])
    near = jnp.concatenate([_cols(ps_ref.at[0, kh], 0, groups) for kh in range(3)], axis=1)
    far = jnp.concatenate([_cols(ps_ref.at[1, kh], 0, groups) for kh in range(3)], axis=1)
    pre = pre_ref[...] + _dot(near, band_ref[0:768, :]) + _dot(far, band_ref[1536:2304, :])
    sig = _sigmoid(pre)
    cot = jnp.concatenate([cot_ref[:, 256 * g : 256 * (g + 1)] for g in range(groups)], axis=0)
    delta = (cot.astype(F32) * (sig * (1.0 + pre * (1.0 - sig)))).astype(BF16)
    delta_ref[...] = delta
    again = delta.astype(F32)
    cells = 2 * groups
    zero = jnp.zeros((rows, LANES), BF16)
    for kh in range(3):
        ds_ref[kh, 0] = zero
        ds_ref[kh, cells + 1] = zero
    for t in range(cells):
        g, j = t // 2, t % 2
        tile = again[g * rows : (g + 1) * rows, LANES * j : LANES * (j + 1)]
        spot = buf.at[t % buf.shape[0]]
        spot[8 : 8 + rows, :] = tile
        ds_ref[0, t + 1] = spot[9 : 9 + rows, :].astype(BF16)
        ds_ref[1, t + 1] = tile.astype(BF16)
        ds_ref[2, t + 1] = spot[7 : 7 + rows, :].astype(BF16)
    wide = cells // 4
    lhs = _window(ds_ref, 0, wide)
    for kd, ref in ((0, gl_ref), (2, gr_ref)):
        _put_cells(ref, _dot(lhs, back_ref[kd]), wide, rows)


def _put_cells(ref, out, wide, rows):
    for g in range(wide):
        for j in range(2):
            ref[2 * g + j] = out[g * rows : (g + 1) * rows, LANES * j : LANES * (j + 1)].astype(ref.dtype)


def _own_two_kernel(delta_ref, own_ref, halo_ref, ds_ref, back_ref, gm_ref, out_ref):
    groups, rows = own_ref.shape[1] - 1, own_ref.shape[2]
    out_ref[1728:, :] = jnp.zeros((out_ref.shape[0] - 1728, LANES), BF16)
    _put_cells(gm_ref, _dot(_window(ds_ref, 0, groups // 2), back_ref[1]), groups // 2, rows)
    delta = delta_ref[...]
    flip = delta.astype(F32).T.astype(BF16)
    planes = (halo_ref.at[0], own_ref, halo_ref.at[1])
    for kk in range(9):
        full = _dot(flip, _cols(planes[kk // 3].at[kk % 3], 0, groups))
        band = full[0:LANES, :] + pltpu.roll(full[LANES:256, :], 192, 1)
        out_ref[192 * kk : 192 * (kk + 1), :] = band.T[0:192, :].astype(BF16)
    total = jnp.sum(delta.astype(F32), axis=0, keepdims=True)
    line = total[:, 0:LANES] + total[:, LANES:256]
    out_ref[1728:1744, :] = jnp.broadcast_to(line, (16, LANES)).astype(BF16)


def _grad_one_kernel(
    keep_ref, gm_ref, fl_ref, fr_ref, slope_ref, own_ref, halo_ref, two_ref, delta_ref, out_ref, sums, up0, up1, flip, one
):
    groups, rows = slope_ref.shape[1], slope_ref.shape[2]
    half = rows // 2
    lane = lax.broadcasted_iota(jnp.int32, (half, LANES), 1)
    sums[...] = jnp.zeros(sums.shape, F32)
    keep_left, keep_right = _mask(keep_ref, 0, half), _mask(keep_ref, 1, half)
    for g in range(groups):
        v = (gm_ref[g] + fl_ref[g].astype(F32) * keep_left + fr_ref[g].astype(F32) * keep_right) * 0.125
        turned = pltpu.roll(v, 64, 1)
        a = jnp.where(lane < 64, v, turned)
        b = jnp.where(lane < 64, turned, v)
        for j, (ref, val) in enumerate(((up0, a), (up1, b))):
            spot = ref.at[g % 2]
            spot[pl.ds(0, half, stride=2), :] = val
            spot[pl.ds(1, half, stride=2), :] = val
            lanes = slice(LANES * j, LANES * (j + 1))
            both = []
            for p in range(2):
                low = (spot[...] * slope_ref[p, g, :, lanes]).astype(BF16)
                delta_ref[p, g, :, lanes] = low
                both.append(low.astype(F32))
            sums[:, lanes] += jnp.sum(both[0].reshape(rows // 8, 8, LANES) + both[1].reshape(rows // 8, 8, LANES), axis=0)
            turn = jnp.concatenate(both, axis=0).T.astype(BF16)
            flip[lanes, 2 * rows * g : 2 * rows * (g + 1)] = turn
    one[...] = jnp.zeros(one.shape, BF16)
    planes = (halo_ref.at[0], own_ref.at[0], own_ref.at[1], halo_ref.at[1])
    for kd in range(3):
        for kh in range(3):
            kk = 3 * kd + kh
            a = planes[kd].at[kh]
            b = planes[kd + 1].at[kh]
            left = jnp.concatenate([r[g] for g in range(groups) for r in (a, b)], axis=0)
            right = jnp.concatenate([r[g + 1] for g in range(groups) for r in (a, b)], axis=0)
            full = _dot(flip[...], jnp.concatenate([left, right], axis=1))
            band = full[0:64, 0:LANES]
            for j in range(1, 4):
                band = band + pltpu.roll(full[64 * j : 64 * j + 64, :], 256 - 32 * j, 1)[:, 0:LANES]
            tall = band.T[0:96, :].astype(BF16)
            for r in range(0, 96, 48):
                at = 96 * kk + r
                side = at // 432
                one[at - 432 * side : at - 432 * side + 48, 64 * side : 64 * side + 64] = tall[r : r + 48, :]
    total = jnp.sum(sums[...], axis=0, keepdims=True)
    line = total[:, 0:LANES] + total[:, LANES:256]
    line = line + pltpu.roll(line, 64, 1)
    one[432:448, :] = jnp.broadcast_to(line, (16, LANES)).astype(BF16)
    count = out_ref.shape[0]
    rows_two, rows_one = two_ref.shape[0] // count, one.shape[0] // count
    for i in range(count):
        out_ref[i, 0:rows_two, :] = two_ref[i * rows_two : (i + 1) * rows_two, :]
        out_ref[i, rows_two:, :] = one[i * rows_one : (i + 1) * rows_one, :]


def _input_kernel(delta_ref, w_ref, gl_ref, own_ref, gr_ref, ds, back, buf):
    groups, rows = delta_ref.shape[1], delta_ref.shape[2]
    cells = 2 * groups
    back[...] = jnp.zeros(back.shape, BF16)
    for kk in range(9):
        _back_bands(w_ref, kk, back.at[kk // 3], 768, 3)
    _zero_edges(buf, rows)
    zero = jnp.zeros((rows, LANES), BF16)
    for p in range(2):
        for kh in range(3):
            ds[p, kh, 0] = zero
            ds[p, kh, cells + 1] = zero

    for g in range(groups):
        for p in range(2):
            for j in range(2):
                low = delta_ref[p, g, :, LANES * j : LANES * (j + 1)]
                spot = buf.at[(2 * p + j + 4 * g) % buf.shape[0]]
                spot[8 : 8 + rows, :] = low.astype(F32)
                t = 2 * g + j + 1
                ds[p, 0, t] = spot[9 : 9 + rows, :].astype(BF16)
                ds[p, 1, t] = low
                ds[p, 2, t] = spot[7 : 7 + rows, :].astype(BF16)
    step = 4
    for g in range(0, groups // 2, step):
        spot = pl.ds(g, step)
        near = _window(ds.at[0], g, step)
        far = _window(ds.at[1], g, step)
        gl_ref[spot] = _dot(near, back[0]).astype(BF16).reshape(step, rows, 256)
        gr_ref[spot] = _dot(far, back[2]).astype(BF16).reshape(step, rows, 256)
        for p in range(2):
            own = _dot(near, back[1 + p]) + _dot(far, back[p])
            own_ref[p, spot] = own.astype(BF16).reshape(step, rows, 256)


def _window(ref, first, count):
    parts = []
    for kh in range(3):
        for i in range(6):
            parts.append(jnp.concatenate([ref[kh, 4 * (first + g) + i] for g in range(count)], axis=0))
    return jnp.concatenate(parts, axis=1)


def _edges_kernel(keep_ref, own_ref, fl_ref, fr_ref, out_ref):
    rows = fl_ref.shape[1]
    masks = [jnp.concatenate([_mask(keep_ref, p, rows)] * 2, axis=1) for p in range(2)]
    for g in range(fl_ref.shape[0]):
        for p, ref in ((0, fl_ref), (1, fr_ref)):
            whole = own_ref[p, g].astype(F32) + ref[g].astype(F32) * masks[p]
            out_ref[p, :, 256 * g : 256 * (g + 1)] = whole.astype(BF16)


def _split_kernel(scale_two, scale_one, rows_two, in_ref, out_ref):
    whole = jnp.sum(in_ref[...].astype(F32), axis=0)
    a = (whole[0:rows_two] * scale_two).astype(BF16)
    b = (whole[rows_two:] * scale_one).astype(BF16)
    for i in range(out_ref.shape[0]):
        out_ref[i, 0:rows_two, :] = a
        out_ref[i, rows_two:, :] = b


def _join_kernel(in_ref, out_ref):
    whole = jnp.sum(in_ref[...].astype(F32), axis=0).astype(BF16)
    for i in range(out_ref.shape[0]):
        out_ref[i] = whole


def _unpack_kernel(rows_two, rows_one, in_ref, w_two_ref, b_two_ref, w_one_ref, b_one_ref):
    two, one = w_two_ref.shape[0], w_one_ref.shape[0] // 2
    for i in range(in_ref.shape[0]):
        at = i * rows_two
        take = min(rows_two, max(two - at, 0))
        if take:
            w_two_ref[at : at + take, :] = in_ref[i, 0:take, :].astype(F32)
        if at <= two < at + rows_two:
            b_two_ref[...] = in_ref[i, two - at : two - at + 8, :].astype(F32)[0:1]
        at = i * rows_one
        take = min(rows_one, max(one - at, 0))
        if take:
            block = in_ref[i, rows_two : rows_two + take, :].astype(F32)
            w_one_ref[at : at + take, :] = block[:, 0:64]
            w_one_ref[one + at : one + at + take, :] = block[:, 64:128]
        if at <= one < at + rows_one:
            spot = rows_two + one - at
            b_one_ref[...] = in_ref[i, spot : spot + 8, :].astype(F32)[0:1, 0:64]


def _shape(shape, dtype):
    return jax.ShapeDtypeStruct(shape, dtype)


def _call(kernel, out, scratch, flops, moved, mib, args):
    return pl.pallas_call(
        kernel, out_shape=out, scratch_shapes=scratch, compiler_params=_params(mib), cost_estimate=_cost(flops, moved)
    )(*args)


def _round_up(value, unit):
    return -(-value // unit) * unit


def local(act_in, weight_one, bias_one, weight_two, bias_two, cotangent):
    _, slab, side, merged = act_in.shape
    half = side // 2
    c0, c1 = weight_one.shape[3:]
    c2 = weight_two.shape[4]
    dp, space = lax.axis_size("dp"), lax.axis_size("space")
    depth_all = slab * space
    scale_one = 16.0 / math.sqrt(dp * depth_all * side * side)
    scale_two = 1.0 / math.sqrt(dp * (depth_all // 2) * half * half)
    up = [(i, (i + 1) % space) for i in range(space)]
    down = [((i + 1) % space, i) for i in range(space)]
    place = lax.axis_index("space")
    keep = jnp.stack([place > 0, place < space - 1]).astype(F32)
    keep = jnp.broadcast_to(keep[:, None, None], (2, 8, LANES))

    x = act_in.reshape(slab, side, merged)
    x0, x1 = x[0], x[slab - 1]
    from_left = lax.ppermute(x1, "space", up)
    from_right = lax.ppermute(x0, "space", down)
    w_one = weight_one.reshape(9, 3 * c0, c1)
    w_two = weight_two.reshape(9, 3 * c1, c2)
    groups = merged // LANES
    xs_shape = (2, 3, groups + 1, side, LANES)
    work = 2 * side * groups * 256
    rows_mid = groups * half
    work_two = rows_mid * 256 * 768
    tile = _shape((groups, half, LANES), BF16)
    tall = pltpu.VMEM((groups + 1, side + 16, LANES), F32)
    short = pltpu.VMEM((groups + 1, half + 16, LANES), F32)
    pre, xs_own, band_one = _call(
        _first_kernel,
        (_shape((2, groups, side, 256), F32), _shape(xs_shape, BF16), _shape((2304, 256), BF16)),
        [tall],
        2 * work * 1536,
        8 * MIB,
        16,
        (x0, x1, w_one),
    )
    band_two, back_two = _call(
        _prep_kernel, (_shape((2304, 256), BF16), _shape((3, 2304, 256), BF16)), [], work * 768, 8 * MIB, 12, (w_two,)
    )
    slope, pooled, xs_halo = _call(
        _second_kernel,
        (_shape((2, groups, side, 256), F32), tile, _shape(xs_shape, BF16)),
        [tall] + [pltpu.VMEM((groups // 4, 4 * side, LANES), F32)] * 2,
        2 * work * 768,
        8 * MIB,
        16,
        (keep, from_left, from_right, pre, band_one, bias_one.reshape(1, c1)),
    )
    pool_left = lax.ppermute(pooled, "space", up)
    pool_right = lax.ppermute(pooled, "space", down)
    ps_own, pre_two = _call(
        _mid_kernel,
        (_shape((3, groups + 1, half, LANES), BF16), _shape((rows_mid, 256), F32)),
        [short],
        2 * work_two,
        2 * MIB,
        12,
        (pooled, band_two, bias_two.reshape(1, c2)),
    )
    delta_two, ps_halo, ds_two, gp_left, gp_right = _call(
        _third_kernel,
        (
            _shape((rows_mid, 256), BF16),
            _shape((2, 3, groups + 1, half, LANES), BF16),
            _shape((3, 2 * groups + 2, half, LANES), BF16),
            tile,
            tile,
        ),
        [short],
        8 * work_two,
        4 * MIB,
        16,
        (keep, pool_left, pool_right, pre_two, band_two, back_two, cotangent.reshape(half, -1)),
    )
    gp_from_right = lax.ppermute(gp_left, "space", down)
    gp_from_left = lax.ppermute(gp_right, "space", up)
    runs = space // 2
    peers = 2 * dp
    planes = [[d * space + r * runs + z for d in range(dp) for r in range(2)] for z in range(runs)]
    lines = [[r * runs + z for z in range(runs)] for r in range(2)]
    rows_two = _round_up(1744, 8 * peers)
    rows_one = _round_up(448, 8 * peers)
    gp_own, part_two = _call(
        _own_two_kernel,
        (_shape((groups, half, LANES), F32), _shape((rows_two, LANES), BF16)),
        [],
        8 * work_two,
        2 * MIB,
        16,
        (delta_two, ps_own, ps_halo, ds_two, back_two),
    )
    rows_all = (rows_two + rows_one) // peers
    delta_one, parts = _call(
        _grad_one_kernel,
        (_shape((2, groups, side, 256), BF16), _shape((peers, rows_all, LANES), BF16)),
        [pltpu.VMEM((8, 256), F32)]
        + [pltpu.VMEM((2, side, LANES), F32)] * 2
        + [pltpu.VMEM((256, 2 * groups * side), BF16), pltpu.VMEM((rows_one, LANES), BF16)],
        2 * work * 2304,
        4 * MIB,
        16,
        (keep, gp_own, gp_from_left, gp_from_right, slope, xs_own, xs_halo, part_two),
    )
    rows_two //= peers
    rows_one //= peers
    met = lax.all_to_all(parts, ("dp", "space"), 0, 0, axis_index_groups=planes)
    block = _shape((groups // 2, side, 256), BF16)
    gx_left, gx_own, gx_right = _call(
        _input_kernel,
        (block, _shape((2, groups // 2, side, 256), BF16), block),
        [
            pltpu.VMEM((2, 3, 2 * groups + 2, side, LANES), BF16),
            pltpu.VMEM((3, 2304, 256), BF16),
            pltpu.VMEM((16, side + 16, LANES), F32),
        ],
        2 * work * 2304 // 2,
        8 * MIB,
        20,
        (delta_one, w_one),
    )
    gx_from_right = lax.ppermute(gx_left, "space", down)
    gx_from_left = lax.ppermute(gx_right, "space", up)
    grad_x = _call(
        _edges_kernel,
        _shape((2, side, merged), BF16),
        [],
        2 * work * 128,
        4 * MIB,
        12,
        (keep, gx_own, gx_from_left, gx_from_right),
    )
    mine = _call(
        functools.partial(_split_kernel, scale_two, scale_one, rows_two),
        _shape((runs, rows_all, LANES), BF16),
        [],
        0,
        MIB,
        8,
        (met,),
    )
    met = lax.all_to_all(mine, "space", 0, 0, axis_index_groups=lines)
    joined = _call(_join_kernel, _shape((peers, rows_all, LANES), BF16), [], 0, MIB, 8, (met,))
    done = lax.all_to_all(joined, ("dp", "space"), 0, 0, axis_index_groups=planes)
    gw_two, gb_two, gw_one, gb_one = _call(
        functools.partial(_unpack_kernel, rows_two, rows_one),
        (
            _shape((27 * c1, c2), F32),
            _shape((1, c2), F32),
            _shape((27 * c0, c1), F32),
            _shape((1, c1), F32),
        ),
        [],
        0,
        MIB,
        8,
        (done,),
    )
    return (
        grad_x.reshape(act_in.shape),
        gw_one.reshape(weight_one.shape),
        gb_one.reshape(bias_one.shape),
        gw_two.reshape(weight_two.shape),
        gb_two.reshape(bias_two.shape),
    )


def solution(mesh):
    placed = (P("dp", "space", None, None), P(), P(), P(), P(), P("dp", "space", None, None))
    return jax.shard_map(
        local,
        mesh=mesh,
        in_specs=placed,
        out_specs=(P("dp", "space", None, None), P(), P(), P(), P()),
        check_vma=False,
    )
```

```python
import functools
import math

import jax
import jax.numpy as jnp
from jax import lax
from jax.experimental import pallas as pl
from jax.experimental.pallas import tpu as pltpu
from jax.sharding import PartitionSpec as P


F32 = jnp.float32
BF16 = jnp.bfloat16
LANES = 128
MIB = 1024 * 1024


def _params(mib):
    return pltpu.CompilerParams(vmem_limit_bytes=mib * MIB)


def _cost(flops, moved):
    return pl.CostEstimate(flops=int(flops), bytes_accessed=int(moved), transcendentals=0)


def _dot(a, b):
    return lax.dot_general(a, b, (((1,), (0,)), ((), ())), preferred_element_type=F32)


def _sigmoid(v):
    return 0.5 * jnp.tanh(0.5 * v) + 0.5


def _mask(keep_ref, side, rows):
    return jnp.concatenate([keep_ref[side]] * (rows // 8), axis=0)


def _zero_edges(buf, rows):
    tiles = buf.shape[0]
    buf[:, 0:8, :] = jnp.zeros((tiles, 8, LANES), F32)
    buf[:, 8 + rows : 16 + rows, :] = jnp.zeros((tiles, 8, LANES), F32)


def _spread(load, tiles, rows, shift, buf, out):
    lane = lax.broadcasted_iota(jnp.int32, (rows, LANES), 1)
    before = jnp.zeros((rows, LANES), F32)
    for t in range(tiles + 1):
        now = pltpu.roll(load(t).astype(F32), shift, 1) if t < tiles else jnp.zeros((rows, LANES), F32)
        tile = jnp.where(lane < shift, before, now)
        buf[t, 8 : 8 + rows, :] = tile
        out[1, t] = tile.astype(BF16)
        before = now
    for t in range(tiles + 1):
        out[0, t] = buf[t, 7 : 7 + rows, :].astype(BF16)
        out[2, t] = buf[t, 9 : 9 + rows, :].astype(BF16)


def _cols(ref, first, groups):
    rows = ref.shape[1]
    a = ref[pl.ds(first, groups)].reshape(groups * rows, LANES)
    b = ref[pl.ds(first + 1, groups)].reshape(groups * rows, LANES)
    return jnp.concatenate([a, b], axis=1)


def _back_bands(w_ref, kk, out, size, first):
    chan_in, chan_out = w_ref.shape[1] // 3, w_ref.shape[2]
    flip = w_ref[kk].astype(F32).T.astype(BF16)
    for i in range(size // chan_out):
        start = chan_in * (i - first)
        low, high = max(start, 0), min(start + 3 * chan_in, 256)
        if low < high:
            r = size * (kk % 3) + chan_out * i
            out[r : r + chan_out, low:high] = flip[:, low - start : high - start]


def _prep_kernel(w_ref, band_two, back_two):
    band_two[...] = jnp.zeros(band_two.shape, BF16)
    back_two[...] = jnp.zeros(back_two.shape, BF16)
    for kk in range(9):
        for j in range(2):
            r = 256 * kk + 64 * j
            band_two[r : r + 192, LANES * j : LANES * (j + 1)] = w_ref[kk]
        _back_bands(w_ref, kk, back_two.at[kk // 3], 768, 2)


def _first_kernel(x0_ref, x1_ref, w_ref, pre_ref, xs_ref, band_ref, buf):
    rows, groups = x0_ref.shape[0], pre_ref.shape[1]
    band_ref[...] = jnp.zeros(band_ref.shape, BF16)
    for kk in range(9):
        for j in range(4):
            r = 256 * kk + 32 * j
            band_ref[r : r + 96, 64 * j : 64 * j + 64] = w_ref[kk]
    _zero_edges(buf, rows)
    for p, ref in enumerate((x0_ref, x1_ref)):
        _spread(lambda t, ref=ref: ref[:, LANES * t : LANES * (t + 1)], groups, rows, 32, buf, xs_ref.at[p])
    step = 8
    for g in range(0, groups, step):
        sides = [[_cols(xs_ref.at[p, kh], g, step) for kh in range(3)] for p in range(2)]
        lhs = jnp.concatenate(sides[0] + sides[1], axis=1)
        pre_ref[0, pl.ds(g, step)] = _dot(lhs, band_ref[768:2304, :]).reshape(step, rows, 256)
        pre_ref[1, pl.ds(g, step)] = _dot(lhs, band_ref[0:1536, :]).reshape(step, rows, 256)


def _second_kernel(keep_ref, left_ref, right_ref, pre_ref, band_ref, bias_ref, slope_ref, pool_ref, xs_ref, buf, low, high):
    rows, groups = left_ref.shape[0], pre_ref.shape[1]
    half = rows // 2
    bias = jnp.concatenate([bias_ref[...]] * 4, axis=1)
    _zero_edges(buf, rows)
    for s, ref in enumerate((left_ref, right_ref)):
        keep = _mask(keep_ref, s, rows)
        _spread(
            lambda t, ref=ref, keep=keep: ref[:, LANES * t : LANES * (t + 1)].astype(F32) * keep,
            groups,
            rows,
            32,
            buf,
            xs_ref.at[s],
        )
    step = 8
    lane = lax.broadcasted_iota(jnp.int32, (step * half, LANES), 1)

    for g in range(0, groups, step):
        total = None
        for p in range(2):
            lhs = jnp.concatenate([_cols(xs_ref.at[p, kh], g, step) for kh in range(3)], axis=1)
            more = _dot(lhs, band_ref[1536 * p : 1536 * p + 768, :])
            pre = pre_ref[p, pl.ds(g, step)].reshape(step * rows, 256) + more + bias
            sig = _sigmoid(pre)
            slope_ref[p, pl.ds(g, step)] = (sig * (1.0 + pre * (1.0 - sig))).reshape(step, rows, 256)
            act = pre * sig
            total = act if total is None else total + act
        sums = []
        for ref, lanes in ((low, 0), (high, LANES)):
            part = ref.at[g // step]
            v = total[:, lanes : lanes + LANES]
            part[...] = v + pltpu.roll(v, 64, 1)
            sums.append(part[pl.ds(0, step * half, stride=2), :] + part[pl.ds(1, step * half, stride=2), :])
        mean = jnp.where(lane < 64, sums[0], sums[1]) * 0.125
        pool_ref[pl.ds(g, step)] = mean.astype(BF16).reshape(step, half, LANES)


def _mid_kernel(own_ref, band_ref, bias_ref, ps_ref, pre_ref, buf):
    groups, rows = own_ref.shape[0], own_ref.shape[1]
    _zero_edges(buf, rows)
    _spread(lambda t: own_ref[t], groups, rows, 64, buf, ps_ref)
    lhs = jnp.concatenate([_cols(ps_ref.at[kh], 0, groups) for kh in range(3)], axis=1)
    bias = jnp.concatenate([bias_ref[...]] * 2, axis=1)
    pre_ref[...] = _dot(lhs, band_ref[768:1536, :]) + bias


def _third_kernel(
    keep_ref, left_ref, right_ref, pre_ref, band_ref, back_ref, cot_ref, delta_ref, ps_ref, ds_ref, gl_ref, gr_ref, buf
):
    groups, rows = left_ref.shape[0], left_ref.shape[1]
    _zero_edges(buf, rows)
    for s, ref in enumerate((left_ref, right_ref)):
        keep = _mask(keep_ref, s, rows)
        _spread(lambda t, ref=ref, keep=keep: ref[t].astype(F32) * keep, groups, rows, 64, buf, ps_ref.at[s])
    near = jnp.concatenate([_cols(ps_ref.at[0, kh], 0, groups) for kh in range(3)], axis=1)
    far = jnp.concatenate([_cols(ps_ref.at[1, kh], 0, groups) for kh in range(3)], axis=1)
    pre = pre_ref[...] + _dot(near, band_ref[0:768, :]) + _dot(far, band_ref[1536:2304, :])
    sig = _sigmoid(pre)
    cot = jnp.concatenate([cot_ref[:, 256 * g : 256 * (g + 1)] for g in range(groups)], axis=0)
    delta = (cot.astype(F32) * (sig * (1.0 + pre * (1.0 - sig)))).astype(BF16)
    delta_ref[...] = delta
    again = delta.astype(F32)
    cells = 2 * groups
    zero = jnp.zeros((rows, LANES), BF16)
    for kh in range(3):
        ds_ref[kh, 0] = zero
        ds_ref[kh, cells + 1] = zero
    for t in range(cells):
        g, j = t // 2, t % 2
        tile = again[g * rows : (g + 1) * rows, LANES * j : LANES * (j + 1)]
        spot = buf.at[t % buf.shape[0]]
        spot[8 : 8 + rows, :] = tile
        ds_ref[0, t + 1] = spot[9 : 9 + rows, :].astype(BF16)
        ds_ref[1, t + 1] = tile.astype(BF16)
        ds_ref[2, t + 1] = spot[7 : 7 + rows, :].astype(BF16)
    wide = cells // 4
    lhs = _window(ds_ref, 0, wide)
    for kd, ref in ((0, gl_ref), (2, gr_ref)):
        _put_cells(ref, _dot(lhs, back_ref[kd]), wide, rows)


def _put_cells(ref, out, wide, rows):
    for g in range(wide):
        for j in range(2):
            ref[2 * g + j] = out[g * rows : (g + 1) * rows, LANES * j : LANES * (j + 1)].astype(ref.dtype)


def _own_two_kernel(delta_ref, own_ref, halo_ref, ds_ref, back_ref, gm_ref, out_ref):
    groups, rows = own_ref.shape[1] - 1, own_ref.shape[2]
    out_ref[1728:, :] = jnp.zeros((out_ref.shape[0] - 1728, LANES), BF16)
    _put_cells(gm_ref, _dot(_window(ds_ref, 0, groups // 2), back_ref[1]), groups // 2, rows)
    delta = delta_ref[...]
    flip = delta.astype(F32).T.astype(BF16)
    planes = (halo_ref.at[0], own_ref, halo_ref.at[1])
    for kk in range(9):
        full = _dot(flip, _cols(planes[kk // 3].at[kk % 3], 0, groups))
        band = full[0:LANES, :] + pltpu.roll(full[LANES:256, :], 192, 1)
        out_ref[192 * kk : 192 * (kk + 1), :] = band.T[0:192, :].astype(BF16)
    total = jnp.sum(delta.astype(F32), axis=0, keepdims=True)
    line = total[:, 0:LANES] + total[:, LANES:256]
    out_ref[1728:1744, :] = jnp.broadcast_to(line, (16, LANES)).astype(BF16)


def _grad_one_kernel(
    keep_ref, gm_ref, fl_ref, fr_ref, slope_ref, own_ref, halo_ref, two_ref, delta_ref, out_ref, sums, up0, up1, flip, one
):
    groups, rows = slope_ref.shape[1], slope_ref.shape[2]
    half = rows // 2
    lane = lax.broadcasted_iota(jnp.int32, (half, LANES), 1)
    sums[...] = jnp.zeros(sums.shape, F32)
    keep_left, keep_right = _mask(keep_ref, 0, half), _mask(keep_ref, 1, half)
    for g in range(groups):
        v = (gm_ref[g] + fl_ref[g].astype(F32) * keep_left + fr_ref[g].astype(F32) * keep_right) * 0.125
        turned = pltpu.roll(v, 64, 1)
        a = jnp.where(lane < 64, v, turned)
        b = jnp.where(lane < 64, turned, v)
        for j, (ref, val) in enumerate(((up0, a), (up1, b))):
            spot = ref.at[g % 2]
            spot[pl.ds(0, half, stride=2), :] = val
            spot[pl.ds(1, half, stride=2), :] = val
            lanes = slice(LANES * j, LANES * (j + 1))
            both = []
            for p in range(2):
                low = (spot[...] * slope_ref[p, g, :, lanes]).astype(BF16)
                delta_ref[p, g, :, lanes] = low
                both.append(low.astype(F32))
            sums[:, lanes] += jnp.sum(both[0].reshape(rows // 8, 8, LANES) + both[1].reshape(rows // 8, 8, LANES), axis=0)
            turn = jnp.concatenate(both, axis=0).T.astype(BF16)
            flip[lanes, 2 * rows * g : 2 * rows * (g + 1)] = turn
    one[...] = jnp.zeros(one.shape, BF16)
    planes = (halo_ref.at[0], own_ref.at[0], own_ref.at[1], halo_ref.at[1])
    for kd in range(3):
        for kh in range(3):
            kk = 3 * kd + kh
            a = planes[kd].at[kh]
            b = planes[kd + 1].at[kh]
            left = jnp.concatenate([r[g] for g in range(groups) for r in (a, b)], axis=0)
            right = jnp.concatenate([r[g + 1] for g in range(groups) for r in (a, b)], axis=0)
            full = _dot(flip[...], jnp.concatenate([left, right], axis=1))
            band = full[0:64, 0:LANES]
            for j in range(1, 4):
                band = band + pltpu.roll(full[64 * j : 64 * j + 64, :], 256 - 32 * j, 1)[:, 0:LANES]
            tall = band.T[0:96, :].astype(BF16)
            for r in range(0, 96, 48):
                at = 96 * kk + r
                side = at // 432
                one[at - 432 * side : at - 432 * side + 48, 64 * side : 64 * side + 64] = tall[r : r + 48, :]
    total = jnp.sum(sums[...], axis=0, keepdims=True)
    line = total[:, 0:LANES] + total[:, LANES:256]
    line = line + pltpu.roll(line, 64, 1)
    one[432:448, :] = jnp.broadcast_to(line, (16, LANES)).astype(BF16)
    count = out_ref.shape[0]
    rows_two, rows_one = two_ref.shape[0] // count, one.shape[0] // count
    for i in range(count):
        out_ref[i, 0:rows_two, :] = two_ref[i * rows_two : (i + 1) * rows_two, :]
        out_ref[i, rows_two:, :] = one[i * rows_one : (i + 1) * rows_one, :]


def _input_kernel(delta_ref, w_ref, gl_ref, own_ref, gr_ref, ds, back, buf):
    groups, rows = delta_ref.shape[1], delta_ref.shape[2]
    cells = 2 * groups
    back[...] = jnp.zeros(back.shape, BF16)
    for kk in range(9):
        _back_bands(w_ref, kk, back.at[kk // 3], 768, 3)
    _zero_edges(buf, rows)
    zero = jnp.zeros((rows, LANES), BF16)
    for p in range(2):
        for kh in range(3):
            ds[p, kh, 0] = zero
            ds[p, kh, cells + 1] = zero

    for g in range(groups):
        for p in range(2):
            for j in range(2):
                low = delta_ref[p, g, :, LANES * j : LANES * (j + 1)]
                spot = buf.at[(2 * p + j + 4 * g) % buf.shape[0]]
                spot[8 : 8 + rows, :] = low.astype(F32)
                t = 2 * g + j + 1
                ds[p, 0, t] = spot[9 : 9 + rows, :].astype(BF16)
                ds[p, 1, t] = low
                ds[p, 2, t] = spot[7 : 7 + rows, :].astype(BF16)
    step = 8
    for g in range(0, groups // 2, step):
        spot = pl.ds(g, step)
        near = _window(ds.at[0], g, step)
        far = _window(ds.at[1], g, step)
        gl_ref[spot] = _dot(near, back[0]).astype(BF16).reshape(step, rows, 256)
        gr_ref[spot] = _dot(far, back[2]).astype(BF16).reshape(step, rows, 256)
        for p in range(2):
            own = _dot(near, back[1 + p]) + _dot(far, back[p])
            own_ref[p, spot] = own.astype(BF16).reshape(step, rows, 256)


def _window(ref, first, count):
    parts = []
    for kh in range(3):
        for i in range(6):
            parts.append(jnp.concatenate([ref[kh, 4 * (first + g) + i] for g in range(count)], axis=0))
    return jnp.concatenate(parts, axis=1)


def _edges_kernel(keep_ref, own_ref, fl_ref, fr_ref, out_ref):
    rows = fl_ref.shape[1]
    masks = [jnp.concatenate([_mask(keep_ref, p, rows)] * 2, axis=1) for p in range(2)]
    for g in range(fl_ref.shape[0]):
        for p, ref in ((0, fl_ref), (1, fr_ref)):
            whole = own_ref[p, g].astype(F32) + ref[g].astype(F32) * masks[p]
            out_ref[p, :, 256 * g : 256 * (g + 1)] = whole.astype(BF16)


def _split_kernel(scale_two, scale_one, rows_two, in_ref, out_ref):
    whole = jnp.sum(in_ref[...].astype(F32), axis=0)
    a = (whole[0:rows_two] * scale_two).astype(BF16)
    b = (whole[rows_two:] * scale_one).astype(BF16)
    for i in range(out_ref.shape[0]):
        out_ref[i, 0:rows_two, :] = a
        out_ref[i, rows_two:, :] = b


def _join_kernel(in_ref, out_ref):
    whole = jnp.sum(in_ref[...].astype(F32), axis=0).astype(BF16)
    for i in range(out_ref.shape[0]):
        out_ref[i] = whole


def _unpack_kernel(rows_two, rows_one, in_ref, w_two_ref, b_two_ref, w_one_ref, b_one_ref):
    two, one = w_two_ref.shape[0], w_one_ref.shape[0] // 2
    for i in range(in_ref.shape[0]):
        at = i * rows_two
        take = min(rows_two, max(two - at, 0))
        if take:
            w_two_ref[at : at + take, :] = in_ref[i, 0:take, :].astype(F32)
        if at <= two < at + rows_two:
            b_two_ref[...] = in_ref[i, two - at : two - at + 8, :].astype(F32)[0:1]
        at = i * rows_one
        take = min(rows_one, max(one - at, 0))
        if take:
            block = in_ref[i, rows_two : rows_two + take, :].astype(F32)
            w_one_ref[at : at + take, :] = block[:, 0:64]
            w_one_ref[one + at : one + at + take, :] = block[:, 64:128]
        if at <= one < at + rows_one:
            spot = rows_two + one - at
            b_one_ref[...] = in_ref[i, spot : spot + 8, :].astype(F32)[0:1, 0:64]


def _shape(shape, dtype):
    return jax.ShapeDtypeStruct(shape, dtype)


def _call(kernel, out, scratch, flops, moved, mib, args):
    return pl.pallas_call(
        kernel, out_shape=out, scratch_shapes=scratch, compiler_params=_params(mib), cost_estimate=_cost(flops, moved)
    )(*args)


def _round_up(value, unit):
    return -(-value // unit) * unit


def local(act_in, weight_one, bias_one, weight_two, bias_two, cotangent):
    _, slab, side, merged = act_in.shape
    half = side // 2
    c0, c1 = weight_one.shape[3:]
    c2 = weight_two.shape[4]
    dp, space = lax.axis_size("dp"), lax.axis_size("space")
    depth_all = slab * space
    scale_one = 16.0 / math.sqrt(dp * depth_all * side * side)
    scale_two = 1.0 / math.sqrt(dp * (depth_all // 2) * half * half)
    up = [(i, (i + 1) % space) for i in range(space)]
    down = [((i + 1) % space, i) for i in range(space)]
    place = lax.axis_index("space")
    keep = jnp.stack([place > 0, place < space - 1]).astype(F32)
    keep = jnp.broadcast_to(keep[:, None, None], (2, 8, LANES))

    x = act_in.reshape(slab, side, merged)
    x0, x1 = x[0], x[slab - 1]
    from_left = lax.ppermute(x1, "space", up)
    from_right = lax.ppermute(x0, "space", down)
    w_one = weight_one.reshape(9, 3 * c0, c1)
    w_two = weight_two.reshape(9, 3 * c1, c2)
    groups = merged // LANES
    xs_shape = (2, 3, groups + 1, side, LANES)
    work = 2 * side * groups * 256
    rows_mid = groups * half
    work_two = rows_mid * 256 * 768
    tile = _shape((groups, half, LANES), BF16)
    tall = pltpu.VMEM((groups + 1, side + 16, LANES), F32)
    short = pltpu.VMEM((groups + 1, half + 16, LANES), F32)
    pre, xs_own, band_one = _call(
        _first_kernel,
        (_shape((2, groups, side, 256), F32), _shape(xs_shape, BF16), _shape((2304, 256), BF16)),
        [tall],
        2 * work * 1536,
        8 * MIB,
        16,
        (x0, x1, w_one),
    )
    band_two, back_two = _call(
        _prep_kernel, (_shape((2304, 256), BF16), _shape((3, 2304, 256), BF16)), [], work * 768, 8 * MIB, 12, (w_two,)
    )
    slope, pooled, xs_halo = _call(
        _second_kernel,
        (_shape((2, groups, side, 256), F32), tile, _shape(xs_shape, BF16)),
        [tall] + [pltpu.VMEM((groups // 8, 8 * side, LANES), F32)] * 2,
        2 * work * 768,
        8 * MIB,
        16,
        (keep, from_left, from_right, pre, band_one, bias_one.reshape(1, c1)),
    )
    pool_left = lax.ppermute(pooled, "space", up)
    pool_right = lax.ppermute(pooled, "space", down)
    ps_own, pre_two = _call(
        _mid_kernel,
        (_shape((3, groups + 1, half, LANES), BF16), _shape((rows_mid, 256), F32)),
        [short],
        2 * work_two,
        2 * MIB,
        12,
        (pooled, band_two, bias_two.reshape(1, c2)),
    )
    delta_two, ps_halo, ds_two, gp_left, gp_right = _call(
        _third_kernel,
        (
            _shape((rows_mid, 256), BF16),
            _shape((2, 3, groups + 1, half, LANES), BF16),
            _shape((3, 2 * groups + 2, half, LANES), BF16),
            tile,
            tile,
        ),
        [short],
        8 * work_two,
        4 * MIB,
        16,
        (keep, pool_left, pool_right, pre_two, band_two, back_two, cotangent.reshape(half, -1)),
    )
    gp_from_right = lax.ppermute(gp_left, "space", down)
    gp_from_left = lax.ppermute(gp_right, "space", up)
    runs = space // 2
    peers = 2 * dp
    planes = [[d * space + r * runs + z for d in range(dp) for r in range(2)] for z in range(runs)]
    lines = [[r * runs + z for z in range(runs)] for r in range(2)]
    rows_two = _round_up(1744, 8 * peers)
    rows_one = _round_up(448, 8 * peers)
    gp_own, part_two = _call(
        _own_two_kernel,
        (_shape((groups, half, LANES), F32), _shape((rows_two, LANES), BF16)),
        [],
        8 * work_two,
        2 * MIB,
        16,
        (delta_two, ps_own, ps_halo, ds_two, back_two),
    )
    rows_all = (rows_two + rows_one) // peers
    delta_one, parts = _call(
        _grad_one_kernel,
        (_shape((2, groups, side, 256), BF16), _shape((peers, rows_all, LANES), BF16)),
        [pltpu.VMEM((8, 256), F32)]
        + [pltpu.VMEM((2, side, LANES), F32)] * 2
        + [pltpu.VMEM((256, 2 * groups * side), BF16), pltpu.VMEM((rows_one, LANES), BF16)],
        2 * work * 2304,
        4 * MIB,
        16,
        (keep, gp_own, gp_from_left, gp_from_right, slope, xs_own, xs_halo, part_two),
    )
    rows_two //= peers
    rows_one //= peers
    met = lax.all_to_all(parts, ("dp", "space"), 0, 0, axis_index_groups=planes)
    block = _shape((groups // 2, side, 256), BF16)
    gx_left, gx_own, gx_right = _call(
        _input_kernel,
        (block, _shape((2, groups // 2, side, 256), BF16), block),
        [
            pltpu.VMEM((2, 3, 2 * groups + 2, side, LANES), BF16),
            pltpu.VMEM((3, 2304, 256), BF16),
            pltpu.VMEM((16, side + 16, LANES), F32),
        ],
        2 * work * 2304 // 2,
        8 * MIB,
        20,
        (delta_one, w_one),
    )
    gx_from_right = lax.ppermute(gx_left, "space", down)
    gx_from_left = lax.ppermute(gx_right, "space", up)
    grad_x = _call(
        _edges_kernel,
        _shape((2, side, merged), BF16),
        [],
        2 * work * 128,
        4 * MIB,
        12,
        (keep, gx_own, gx_from_left, gx_from_right),
    )
    mine = _call(
        functools.partial(_split_kernel, scale_two, scale_one, rows_two),
        _shape((runs, rows_all, LANES), BF16),
        [],
        0,
        MIB,
        8,
        (met,),
    )
    met = lax.all_to_all(mine, "space", 0, 0, axis_index_groups=lines)
    joined = _call(_join_kernel, _shape((peers, rows_all, LANES), BF16), [], 0, MIB, 8, (met,))
    done = lax.all_to_all(joined, ("dp", "space"), 0, 0, axis_index_groups=planes)
    gw_two, gb_two, gw_one, gb_one = _call(
        functools.partial(_unpack_kernel, rows_two, rows_one),
        (
            _shape((27 * c1, c2), F32),
            _shape((1, c2), F32),
            _shape((27 * c0, c1), F32),
            _shape((1, c1), F32),
        ),
        [],
        0,
        MIB,
        8,
        (done,),
    )
    return (
        grad_x.reshape(act_in.shape),
        gw_one.reshape(weight_one.shape),
        gb_one.reshape(bias_one.shape),
        gw_two.reshape(weight_two.shape),
        gb_two.reshape(bias_two.shape),
    )


def solution(mesh):
    placed = (P("dp", "space", None, None), P(), P(), P(), P(), P("dp", "space", None, None))
    return jax.shard_map(
        local,
        mesh=mesh,
        in_specs=placed,
        out_specs=(P("dp", "space", None, None), P(), P(), P(), P()),
        check_vma=False,
    )
```
